256 devices in a mesh: tp: 8 (over z), dp: 4 (over y), pp: 8 (over x, core).
Axes of the slice: x: 4, y: 4, z: 8, core: 2. Of those that a mesh axis runs over, the one named last changes fastest.
Arguments:
- master: float32 [50304, 1024], P('tp')
- exp_avg: float32 [50304, 1024], P('tp')
- exp_avg_sq: float32 [50304, 1024], P('tp')
- stage_ids: int32 [8, 24, 256], P('pp', 'dp')
- stage_acts: bfloat16 [8, 24, 256, 1024], P('pp', 'dp')
Outputs:
- output 1: float32 [50304, 1024], P('tp')
- output 2: float32 [50304, 1024], P('tp')
- output 3: float32 [50304, 1024], P('tp')
- output 4: bfloat16 [50304, 1024], P('tp')
All inputs are finite; a program needn't handle non-finite values.
Results may differ from the reference program's by a relative error of at most 0.001.
Values sent between devices are 32-bit elements.
A program may use at most 768 MiB of HBM per device.

```python
import math
import jax
import jax.numpy as jnp
from jax import lax

VOCAB_SIZE = 50304
MODEL_DIM = 1024
SEQ_LEN = 256
BATCH_DEV = 6
DATA_REPL = 4
PIPE_STAGES = 8
OPT_STEP = 10
TOKEN_BLOCK = 128

BATCH_ALL = BATCH_DEV * DATA_REPL
TOKENS_REPL = BATCH_DEV * SEQ_LEN
LOG_SPAN = math.ceil(math.log2(VOCAB_SIZE))
LEARN_RATE = 0.003
BETA_ONE = 0.9
BETA_TWO = 0.95
ADAM_EPS = 1e-8
WEIGHT_DECAY = 0.1
CLIP_NORM = 1.0


def draw_ids(key, perm):
    key_exp, key_rank = jax.random.split(key)
    ids_shape = (PIPE_STAGES, BATCH_ALL, SEQ_LEN)
    exponents = jax.random.randint(key_exp, ids_shape, 0, LOG_SPAN + 1)
    upper_bound = jnp.minimum(jnp.left_shift(jnp.int32(1), exponents), VOCAB_SIZE)
    ranks = jax.random.randint(key_rank, ids_shape, 0, upper_bound)
    tokens = perm[ranks]
    tokens = tokens.at[:, 0, 0].set(0)
    tokens = tokens.at[:, BATCH_ALL - 1, SEQ_LEN - 1].set(VOCAB_SIZE - 1)
    return tokens.astype(jnp.int32)


def setup_inputs(seed: int = 0) -> dict:
    key = jax.random.key(seed)
    k_tab, k_avg, k_sq, k_perm, k_ids, k_act, k_hid = jax.random.split(key, 7)
    table_shape = (VOCAB_SIZE, MODEL_DIM)
    elem_scale = (VOCAB_SIZE * MODEL_DIM) ** -0.5
    master = jax.random.normal(k_tab, table_shape, jnp.float32) * MODEL_DIM ** -0.5
    exp_avg = jax.random.normal(k_avg, table_shape, jnp.float32) * (0.3 * elem_scale)
    exp_avg_sq = jnp.exp(0.5 * jax.random.normal(k_sq, table_shape, jnp.float32)) * (0.09 * elem_scale * elem_scale)
    perm = jax.random.permutation(k_perm, VOCAB_SIZE)
    stage_ids = draw_ids(k_ids, perm)
    grad_scale = 0.08 * math.sqrt(DATA_REPL / TOKENS_REPL)
    stage_acts = jax.random.normal(k_act, (PIPE_STAGES, BATCH_ALL, SEQ_LEN, MODEL_DIM), jnp.float32) * grad_scale
    label_pull = math.log(VOCAB_SIZE) / math.sqrt(MODEL_DIM)
    noise = jax.random.normal(k_hid, (BATCH_ALL, SEQ_LEN, MODEL_DIM), jnp.float32)
    hidden = math.sqrt(1.0 - label_pull * label_pull) * noise + (label_pull * math.sqrt(MODEL_DIM)) * master[stage_ids[PIPE_STAGES - 1]]
    stage_acts = stage_acts.at[PIPE_STAGES - 1].set(hidden)
    return {"master": master, "exp_avg": exp_avg, "exp_avg_sq": exp_avg_sq, "stage_ids": stage_ids, "stage_acts": stage_acts.astype(jnp.bfloat16)}


def head_block(table_bf, hid_block, lab_block):
    logits = jnp.dot(hid_block, table_bf.T, preferred_element_type=jnp.float32)
    prob_mat = jax.nn.softmax(logits, axis=-1)
    is_label = lab_block[:, None] == jnp.arange(VOCAB_SIZE, dtype=jnp.int32)[None, :]
    dlogits = (jnp.where(is_label, prob_mat - 1.0, prob_mat) / TOKENS_REPL).astype(jnp.bfloat16)
    return jnp.dot(dlogits.T, hid_block, preferred_element_type=jnp.float32)


def replica_grad(table_bf, ids_in, dx_in, hidden, labels):
    grad_embed = jax.ops.segment_sum(dx_in.astype(jnp.float32), ids_in, num_segments=VOCAB_SIZE)

    def add_block(acc_grad, block_in):
        return acc_grad + head_block(table_bf, block_in[0], block_in[1]), None

    hid_blocks = hidden.reshape(-1, TOKEN_BLOCK, MODEL_DIM)
    lab_blocks = labels.reshape(-1, TOKEN_BLOCK)
    return lax.scan(add_block, grad_embed, (hid_blocks, lab_blocks))[0]


def reference(master, exp_avg, exp_avg_sq, stage_ids, stage_acts):
    table_bf = master.astype(jnp.bfloat16)
    ids_in = stage_ids[0].reshape(DATA_REPL, TOKENS_REPL)
    labels = stage_ids[PIPE_STAGES - 1].reshape(DATA_REPL, TOKENS_REPL)
    dx_in = stage_acts[0].reshape(DATA_REPL, TOKENS_REPL, MODEL_DIM)
    hidden = stage_acts[PIPE_STAGES - 1].reshape(DATA_REPL, TOKENS_REPL, MODEL_DIM)

    def add_replica(acc_grad, block_in):
        return acc_grad + replica_grad(table_bf, block_in[0], block_in[1], block_in[2], block_in[3]), None

    zero_grad = jnp.zeros((VOCAB_SIZE, MODEL_DIM), jnp.float32)
    grad_sum = lax.scan(add_replica, zero_grad, (ids_in, dx_in, hidden, labels))[0]
    gradient = grad_sum / DATA_REPL
    norm_val = jnp.sqrt(jnp.sum(gradient * gradient))
    gradient = gradient * (CLIP_NORM / jnp.maximum(norm_val, CLIP_NORM))
    new_avg = BETA_ONE * exp_avg + (1.0 - BETA_ONE) * gradient
    new_avg_sq = BETA_TWO * exp_avg_sq + (1.0 - BETA_TWO) * gradient * gradient
    corr_one = 1.0 - BETA_ONE ** OPT_STEP
    corr_two = 1.0 - BETA_TWO ** OPT_STEP
    step_dir = (new_avg / corr_one) / (jnp.sqrt(new_avg_sq / corr_two) + ADAM_EPS)
    new_master = master - LEARN_RATE * (step_dir + WEIGHT_DECAY * master)
    return new_master, new_avg, new_avg_sq, new_master.astype(jnp.bfloat16)
```

```python
import functools

import jax
import jax.numpy as jnp
from jax import lax
from jax.experimental import pallas as pl
from jax.experimental.pallas import tpu as pltpu
from jax.sharding import PartitionSpec as P

LEARN_RATE = 0.003
BETA_ONE = 0.9
BETA_TWO = 0.95
ADAM_EPS = 1e-8
WEIGHT_DECAY = 0.1
CLIP_NORM = 1.0
OPT_STEP = 10

MESH_ID = pl.DeviceIdType.MESH
LOW = -1e30


def stats_kernel(n_pp, n_tp, loc_ref, out_ref, buf_p, buf_z, mid, send_p, recv_p, send_z, recv_z):
    p = lax.axis_index("pp")
    z = lax.axis_index("tp")
    barrier = pltpu.get_barrier_semaphore()
    for o in range(1, n_pp):
        pl.semaphore_signal(barrier, inc=1, device_id={"pp": lax.rem(p + o, n_pp)}, device_id_type=MESH_ID)
    for o in range(1, n_tp):
        pl.semaphore_signal(barrier, inc=1, device_id={"tp": lax.rem(z + o, n_tp)}, device_id_type=MESH_ID)
    pl.semaphore_wait(barrier, n_pp + n_tp - 2)

    def exchange(src, buf, send, recv, axis, me, n):
        copies = []
        for o in range(1, n):
            copies.append(pltpu.make_async_remote_copy(
                src_ref=src, dst_ref=buf.at[o - 1], send_sem=send.at[o - 1], recv_sem=recv.at[o - 1],
                device_id={axis: lax.rem(me + o, n)}, device_id_type=MESH_ID))
        for c in copies:
            c.start()
        for c in copies:
            c.wait()
        top = src[0:1, :]
        for o in range(1, n):
            top = jnp.maximum(top, buf[o - 1, 0:1, :])
        tot = src[1:2, :] * jnp.exp(src[0:1, :] - top)
        for o in range(1, n):
            tot = tot + buf[o - 1, 1:2, :] * jnp.exp(buf[o - 1, 0:1, :] - top)
        return top, tot

    top, tot = exchange(loc_ref, buf_p, send_p, recv_p, "pp", p, n_pp)
    mid[0:1, :] = top
    mid[1:2, :] = tot
    top, tot = exchange(mid, buf_z, send_z, recv_z, "tp", z, n_tp)
    out_ref[0:1, :] = top
    out_ref[1:2, :] = tot


def merge_stats(stats, n_pp, n_tp):
    shape = stats.shape
    return pl.pallas_call(
        functools.partial(stats_kernel, n_pp, n_tp),
        out_shape=jax.ShapeDtypeStruct(shape, jnp.float32),
        in_specs=[pl.BlockSpec(memory_space=pltpu.VMEM)],
        out_specs=pl.BlockSpec(memory_space=pltpu.VMEM),
        scratch_shapes=[
            pltpu.VMEM((n_pp - 1, *shape), jnp.float32), pltpu.VMEM((n_tp - 1, *shape), jnp.float32),
            pltpu.VMEM(shape, jnp.float32),
            pltpu.SemaphoreType.DMA((n_pp - 1,)), pltpu.SemaphoreType.DMA((n_pp - 1,)),
            pltpu.SemaphoreType.DMA((n_tp - 1,)), pltpu.SemaphoreType.DMA((n_tp - 1,)),
        ],
        compiler_params=pltpu.CompilerParams(collective_id=0, has_side_effects=True),
        name="merge_stats",
    )(stats)


def cast_kernel(src_ref, out_ref):
    out_ref[...] = src_ref[...].astype(out_ref.dtype)


def to_bf16(arr):
    rows, dim = arr.shape
    spec = pl.BlockSpec((256, dim), lambda i: (i, 0))
    return pl.pallas_call(
        cast_kernel, out_shape=jax.ShapeDtypeStruct(arr.shape, jnp.bfloat16), grid=(rows // 256,),
        in_specs=[spec], out_specs=spec, name="to_bf16")(arr)


def adamw_kernel(scale_ref, e_ref, m_ref, v_ref, g_ref, *refs):
    ne_ref, nm_ref, nv_ref, nb_ref = refs[-4:]
    g = g_ref[...] * scale_ref[0, 0]
    e = e_ref[...]
    m = BETA_ONE * m_ref[...] + (1.0 - BETA_ONE) * g
    v = BETA_TWO * v_ref[...] + (1.0 - BETA_TWO) * g * g
    step = (m / (1.0 - BETA_ONE ** OPT_STEP)) / (jnp.sqrt(v / (1.0 - BETA_TWO ** OPT_STEP)) + ADAM_EPS)
    ne = e - LEARN_RATE * (step + WEIGHT_DECAY * e)
    ne_ref[...] = ne
    nm_ref[...] = m
    nv_ref[...] = v
    nb_ref[...] = ne.astype(jnp.bfloat16)


def adamw_chunk(scale, master, exp_avg, exp_avg_sq, grad, col, prev):
    rows, dim = master.shape
    width = grad.shape[1]
    tile = 256
    at = col // width
    wide = pl.BlockSpec((tile, width), lambda i: (i, at))
    narrow = pl.BlockSpec((tile, width), lambda i: (i, 0))
    f32 = jax.ShapeDtypeStruct((rows, dim), jnp.float32)
    bf16 = jax.ShapeDtypeStruct((rows, dim), jnp.bfloat16)
    extra = list(prev) if prev is not None else []
    count = rows * width
    return pl.pallas_call(
        adamw_kernel,
        out_shape=(f32, f32, f32, bf16),
        grid=(pl.cdiv(rows, tile),),
        in_specs=[pl.BlockSpec(memory_space=pltpu.SMEM), wide, wide, wide, narrow]
        + [pl.BlockSpec(memory_space=pl.ANY)] * len(extra),
        out_specs=(wide, wide, wide, wide),
        input_output_aliases={5 + i: i for i in range(len(extra))},
        cost_estimate=pl.CostEstimate(flops=20 * count, bytes_accessed=30 * count, transcendentals=2 * count),
        compiler_params=pltpu.CompilerParams(vmem_limit_bytes=58 << 20),
        name="adamw",
    )(scale, master, exp_avg, exp_avg_sq, grad, *extra)


def solution(mesh):
    n_pp, n_dp, n_tp = mesh.shape["pp"], mesh.shape["dp"], mesh.shape["tp"]
    table_spec = P("tp", None)

    def device_step(master, exp_avg, exp_avg_sq, stage_ids, stage_acts):
        vocab, dim = master.shape
        p, z = lax.axis_index("pp"), lax.axis_index("tp")
        tok = stage_ids.shape[1] * stage_ids.shape[2]
        n_blk = n_pp * n_dp
        rows = -(-vocab // n_blk)
        rows = -(-rows // 8) * 8
        part = tok // (n_tp * n_pp)

        acts = stage_acts.reshape(n_tp, n_pp, part, dim)
        mine = lax.dynamic_index_in_dim(acts, z, 0, keepdims=False).astype(jnp.float32)
        got = lax.all_to_all(mine, "pp", 0, 0, tiled=False)
        hid = lax.all_gather(got[n_pp - 1], ("tp", "pp"), tiled=True)
        dx = lax.all_gather(got[0], ("tp", "pp"), tiled=True)
        hid, dx = to_bf16(hid), to_bf16(dx)
        ids = stage_ids.reshape(1, 1, tok)
        ids = lax.all_gather(ids, "pp", axis=0, tiled=True)
        labels, lookup = ids[n_pp - 1], ids[0]

        blocks, index = [], []
        for d in range(n_dp):
            first = (d * n_pp + p) * rows
            short = max(0, ((d + 1) * n_pp) * rows - vocab)
            start = jnp.minimum(first, vocab - rows)
            blk = lax.dynamic_slice_in_dim(master, start, rows, 0).astype(jnp.bfloat16)
            if short:
                blk = jnp.concatenate([blk, jnp.zeros((short, dim), jnp.bfloat16)], 0)
                blk = lax.dynamic_slice_in_dim(blk, first - start, rows, 0)
            blocks.append(blk)
            index.append(first + lax.broadcasted_iota(jnp.int32, (rows, 1), 0))
        table = jnp.concatenate(blocks, 0)
        row_loc = jnp.concatenate(index, 0)
        valid = row_loc < vocab
        row_id = jnp.where(valid, row_loc + z * vocab, -1)

        logits = jnp.einsum("vd,td->vt", table, hid, preferred_element_type=jnp.float32)
        logits = jnp.where(valid, logits, LOW)
        top = jnp.max(logits, axis=0, keepdims=True)
        tot = jnp.sum(jnp.exp(logits - top), axis=0, keepdims=True)
        stats = merge_stats(jnp.concatenate([top, tot], 0), n_pp, n_tp)
        prob = jnp.exp(logits - stats[0:1]) / stats[1:2]
        hit = labels == row_id
        dlog = (jnp.where(hit, prob - 1.0, prob) / tok).astype(jnp.bfloat16)
        part_grad = jnp.einsum("vt,td->vd", dlog, hid, preferred_element_type=jnp.float32)
        look = (lookup == row_id).astype(jnp.bfloat16)
        part_grad = part_grad + jnp.einsum("vt,td->vd", look, dx, preferred_element_type=jnp.float32)

        grad = lax.psum_scatter(part_grad, "dp", scatter_dimension=0, tiled=True) / n_dp
        sq_total = lax.psum(jnp.sum(grad * grad), ("tp", "dp", "pp"))
        scale = (CLIP_NORM / jnp.maximum(jnp.sqrt(sq_total), CLIP_NORM)).reshape(1, 1)
        outs = None
        n_chunk = 2
        width = dim // n_chunk
        for k in range(n_chunk):
            full = lax.all_gather(grad[:, k * width:(k + 1) * width], ("dp", "pp"), tiled=True)
            outs = adamw_chunk(scale, master, exp_avg, exp_avg_sq, full, k * width, outs)
        return tuple(outs)

    return jax.shard_map(device_step, mesh=mesh, in_specs=(table_spec, table_spec, table_spec, P("pp", "dp", None), P("pp", "dp", None, None)), out_specs=(table_spec, table_spec, table_spec, table_spec), check_vma=False)
```

```python
import functools

import jax
import jax.numpy as jnp
from jax import lax
from jax.experimental import pallas as pl
from jax.experimental.pallas import tpu as pltpu
from jax.sharding import PartitionSpec as P

LEARN_RATE = 0.003
BETA_ONE = 0.9
BETA_TWO = 0.95
ADAM_EPS = 1e-8
WEIGHT_DECAY = 0.1
CLIP_NORM = 1.0
OPT_STEP = 10

MESH_ID = pl.DeviceIdType.MESH
LOW = -1e30
VMEM = pltpu.VMEM
DMA = pltpu.SemaphoreType.DMA
F32, BF16 = jnp.float32, jnp.bfloat16


def remote(src, dst, send, recv, where):
    return pltpu.make_async_remote_copy(src_ref=src, dst_ref=dst, send_sem=send, recv_sem=recv, device_id=where, device_id_type=MESH_ID)


def in_vmem(arr):
    return pltpu.with_memory_space_constraint(arr, VMEM)


def enter(groups):
    barrier = pltpu.get_barrier_semaphore()
    for axis, peer in groups:
        pl.semaphore_signal(barrier, inc=1, device_id={axis: peer}, device_id_type=MESH_ID)
    pl.semaphore_wait(barrier, len(groups))


def spread_kernel(n_tp, n_pp, n_chunk, acts_ref, ids_ref, hid_ref, dx_ref, lab_ref, look_ref, hid_buf, dx_buf, feed_sem, send_x, send_z, send_d, send_e, recv_x, recv_z, recv_d, recv_e, id_send, id_recv):
    p, z = lax.axis_index("pp"), lax.axis_index("tp")
    n_x = n_pp // 2
    x, c, par = p // 2, lax.rem(p, 2), lax.rem(z, 2)
    step = 1 - 2 * c
    next_p = 2 * lax.rem(x + step + n_x, n_x) + c
    next_z = lax.rem(z + step + n_tp, n_tp)
    mate = 2 * x + 1 - c
    tok = hid_buf.shape[0]
    quarter = tok // 4
    size = quarter // n_chunk
    lag = 2

    enter([("pp", lax.rem(p + o, n_pp)) for o in range(1, n_pp)] + [("tp", lax.rem(z + 1, n_tp)), ("tp", lax.rem(z + n_tp - 1, n_tp))])

    def rows(core, parity, k):
        return pl.ds(pl.multiple_of((2 * parity + core) * quarter + k * size, 8), size)

    for a, source in enumerate((n_pp - 1, 0)):
        dst = (lab_ref, look_ref)[a]

        @pl.when(p == source)
        def _(a=a, dst=dst):
            dst[...] = ids_ref[...]
            for o in range(1, n_pp):
                remote(ids_ref, dst, id_send.at[a, o - 1], id_recv.at[a], {"pp": lax.rem(p + o, n_pp)}).start()

    for a, (source, buf, out) in enumerate(((n_pp - 1, hid_buf, hid_ref), (0, dx_buf, dx_ref))):
        s_x, s_c = source // 2, source % 2
        ahead = jnp.where(c == 0, x - s_x, s_x - x)
        dist = lax.rem(ahead + n_x, n_x)
        is_src = p == source

        def feed(k):
            there = rows(1 - c, par, k)
            return remote(acts_ref.at[there], buf.at[there], feed_sem.at[a, k], recv_x.at[a, k], {"pp": mate})

        def ring(k, src=buf):
            here = rows(c, par, k)
            return remote(src.at[here], buf.at[here], send_x.at[a, k], recv_x.at[a, k], {"pp": next_p})

        def plane(k, src=buf):
            here = rows(c, par, k)
            return remote(src.at[here], buf.at[here], send_z.at[a, k], recv_z.at[a, k], {"tp": next_z})

        def plane_in(k):
            here = rows(c, 1 - par, k)
            return remote(buf.at[here], buf.at[here], send_z.at[a, k], recv_z.at[a, k], {"tp": next_z})

        def across(k, src=buf):
            here = rows(c, par, k)
            return remote(src.at[here], buf.at[here], send_d.at[a, k], recv_d.at[a, k], {"pp": mate})

        def across_in(k):
            here = rows(1 - c, par, k)
            return remote(buf.at[here], buf.at[here], send_d.at[a, k], recv_d.at[a, k], {"pp": mate})

        def again(k):
            here = rows(c, 1 - par, k)
            return remote(buf.at[here], buf.at[here], send_e.at[a, k], recv_e.at[a, k], {"pp": mate})

        def again_in(k):
            here = rows(1 - c, 1 - par, k)
            return remote(buf.at[here], buf.at[here], send_e.at[a, k], recv_e.at[a, k], {"pp": mate})

        @pl.when(is_src)
        def _():
            @pl.loop(0, n_chunk)
            def _(k):
                feed(k).start()

        @pl.loop(0, n_chunk + lag)
        def _(k):
            @pl.when(k < n_chunk)
            def _():
                def onward(src):
                    if n_x > 1:
                        @pl.when(dist < n_x - 1)
                        def _():
                            ring(k, src).start()

                    plane(k, src).start()
                    across(k, src).start()

                @pl.when(is_src)
                def _():
                    onward(acts_ref)
                    here = rows(c, par, k)
                    buf[here, :] = acts_ref[here, :]

                @pl.when(jnp.logical_not(is_src))
                def _():
                    ring(k).wait_recv()
                    onward(buf)

            @pl.when(k >= lag)
            def _():
                plane_in(k - lag).wait_recv()
                again(k - lag).start()

        @pl.loop(0, n_chunk)
        def _(k):
            across_in(k).wait_recv()
            again_in(k).wait_recv()

        @pl.loop(0, tok // 128)
        def _(k):
            here = pl.ds(pl.multiple_of(k * 128, 128), 128)
            out[here, :] = buf[here, :].astype(BF16)

        @pl.loop(0, n_chunk)
        def _(k):
            @pl.when(is_src)
            def _():
                feed(k).wait_send()

            if n_x > 1:
                @pl.when(dist < n_x - 1)
                def _():
                    ring(k).wait_send()

            plane(k).wait_send()
            across(k).wait_send()
            again(k).wait_send()

    for a, source in enumerate((n_pp - 1, 0)):
        dst = (lab_ref, look_ref)[a]

        @pl.when(p == source)
        def _(a=a, dst=dst):
            for o in range(1, n_pp):
                remote(ids_ref, dst, id_send.at[a, o - 1], id_recv.at[a], {"pp": lax.rem(p + o, n_pp)}).wait_send()

        @pl.when(p != source)
        def _(a=a, dst=dst):
            remote(ids_ref, dst, id_send.at[a, 0], id_recv.at[a], {"pp": mate}).wait_recv()


def spread(acts, ids, n_tp, n_pp):
    tok, dim = acts.shape
    n_chunk = 12 if tok % (4 * 12 * 8) == 0 else 2
    sem = DMA((2, n_chunk))
    full = pl.BlockSpec(memory_space=VMEM)
    return pl.pallas_call(
        functools.partial(spread_kernel, n_tp, n_pp, n_chunk),
        out_shape=(VMEM((tok, dim), BF16), VMEM((tok, dim), BF16), jax.ShapeDtypeStruct(ids.shape, jnp.int32), jax.ShapeDtypeStruct(ids.shape, jnp.int32)),
        in_specs=[full, full],
        out_specs=(full, full, full, full),
        scratch_shapes=[VMEM((tok, dim), F32), VMEM((tok, dim), F32)] + [sem] * 9 + [DMA((2, n_pp - 1)), DMA((2,))],
        compiler_params=pltpu.CompilerParams(collective_id=0, has_side_effects=True, vmem_limit_bytes=32 << 20),
        name="spread",
    )(in_vmem(acts), ids)


def ring_plan(n_one, n_two):
    items = [(1, s, 0) for s in range(n_one - 1)] + [(2, s, t) for s in range(n_one) for t in range(n_two - 1)]
    return sorted(items, key=lambda i: (i[1] + i[2], i[0], i[2]))


def grad_kernel(n_tp, n_dp, n_pp, vocab, tab_ref, hid_ref, dx_ref, lab_ref, look_ref, g_ref, scale_ref, exp_ref, dl_ref, part_ref, stat_ref, mid_ref, buf_p, buf_z, rel_ref, one_ref, com_ref, nb_p, nb_y, nb_z, sp_s, sp_r, sz_s, sz_r, rs_s, rs_r, np_s, np_r, ny_s, ny_r, nz_s, nz_r, ag_s, ag_r, d_s, d_r):
    p, z, y = lax.axis_index("pp"), lax.axis_index("tp"), lax.axis_index("dp")
    n_x = n_pp // 2
    x, c = p // 2, lax.rem(p, 2)
    mate = 2 * x + 1 - c
    rows, tok = exp_ref.shape[1:]
    dq = g_ref.shape[3]
    up_y, down_y = lax.rem(y + 1, n_dp), lax.rem(y + n_dp - 1, n_dp)

    enter([("pp", lax.rem(p + o, n_pp)) for o in range(1, n_pp)] + [("tp", lax.rem(z + o, n_tp)) for o in range(1, n_tp)] + [("dp", lax.rem(y + o, n_dp)) for o in range(1, n_dp)])

    def first_row(d):
        return (d * n_pp + p) * rows

    wide = min(256, tok)

    @pl.loop(0, tok // wide)
    def _(j):
        cols = pl.ds(pl.multiple_of(j * wide, wide), wide)
        h = hid_ref[cols, :]
        top = jnp.full((1, wide), LOW, F32)
        for d in range(n_dp):
            lg = lax.dot_general(tab_ref[d], h, (((1,), (1,)), ((), ())), preferred_element_type=F32)
            if (d + 1) * n_pp * rows > vocab:
                ok = first_row(d) + lax.broadcasted_iota(jnp.int32, (rows, wide), 0) < vocab
                lg = jnp.where(ok, lg, LOW)
            exp_ref[d, :, cols] = lg
            top = jnp.maximum(top, jnp.max(lg, axis=0, keepdims=True))
        tot = jnp.zeros((1, wide), F32)
        for d in range(n_dp):
            e = jnp.exp(exp_ref[d, :, cols] - top)
            exp_ref[d, :, cols] = e
            tot = tot + jnp.sum(e, axis=0, keepdims=True)
        stat_ref[0:1, cols] = top
        stat_ref[1:2, cols] = tot

    def swap(src, buf, send, recv, axis, me, n):
        return [remote(src, buf.at[o - 1], send.at[o - 1], recv.at[o - 1], {axis: lax.rem(me + o, n)}) for o in range(1, n)]

    def merge(src, buf, n):
        top = src[0:1, :]
        for o in range(1, n):
            top = jnp.maximum(top, buf[o - 1, 0:1, :])
        tot = src[1:2, :] * jnp.exp(src[0:1, :] - top)
        for o in range(1, n):
            tot = tot + buf[o - 1, 1:2, :] * jnp.exp(buf[o - 1, 0:1, :] - top)
        return top, tot

    def local_ids(ref):
        ids = ref[...] - z * vocab
        return jnp.where(ids < vocab, ids, -1)

    def row_ids(d):
        return first_row(d) + lax.broadcasted_iota(jnp.int32, (rows, tok), 0)

    def lookup(d):
        dl_ref[...] = (local_ids(look_ref) == row_ids(d)).astype(BF16)
        for q in range(4):
            part_ref[d, q] = jnp.dot(dl_ref[...], dx_ref[:, q * dq:(q + 1) * dq], preferred_element_type=F32)

    stage = swap(stat_ref, buf_p, sp_s, sp_r, "pp", p, n_pp)
    for cp in stage:
        cp.start()
    pl.loop(0, n_dp // 2)(lookup)
    for cp in stage:
        cp.wait()
    top, tot = merge(stat_ref, buf_p, n_pp)
    mid_ref[0:1, :] = top
    mid_ref[1:2, :] = tot
    stage = swap(mid_ref, buf_z, sz_s, sz_r, "tp", z, n_tp)
    for cp in stage:
        cp.start()
    pl.loop(n_dp // 2, n_dp)(lookup)
    for cp in stage:
        cp.wait()
    top, tot = merge(mid_ref, buf_z, n_tp)
    mid_ref[0:1, :] = jnp.exp(stat_ref[0:1, :] - top) / (tot * tok)

    def head(d):
        prob = exp_ref[d] * mid_ref[0:1, :]
        hit = local_ids(lab_ref) == row_ids(d)
        dl_ref[...] = jnp.where(hit, prob - 1.0 / tok, prob).astype(BF16)
        for q in range(4):
            part_ref[d, q] += jnp.dot(dl_ref[...], hid_ref[:, q * dq:(q + 1) * dq], preferred_element_type=F32)

    lo, hi = pl.ds(0, 2), pl.ds(2, 2)
    far = lax.rem(y + 2, n_dp)
    rel_a = remote(part_ref.at[far, lo], rel_ref.at[0], rs_s.at[0], rs_r.at[0], {"dp": up_y})
    rel_b = remote(part_ref.at[far, hi], rel_ref.at[1], rs_s.at[1], rs_r.at[1], {"dp": down_y})
    one_b = remote(part_ref.at[up_y, hi], one_ref.at[1], rs_s.at[2], rs_r.at[2], {"dp": up_y})
    one_a = remote(part_ref.at[down_y, lo], one_ref.at[0], rs_s.at[3], rs_r.at[3], {"dp": down_y})
    com_a = remote(part_ref.at[up_y, lo], com_ref.at[0], rs_s.at[4], rs_r.at[4], {"dp": up_y})
    com_b = remote(part_ref.at[down_y, hi], com_ref.at[1], rs_s.at[5], rs_r.at[5], {"dp": down_y})
    head(far)
    rel_a.start()
    rel_b.start()
    head(up_y)
    one_b.start()
    head(down_y)
    one_a.start()
    head(y)
    rel_a.wait_recv()
    part_ref[up_y, lo] += rel_ref[0]
    com_a.start()
    rel_b.wait_recv()
    part_ref[down_y, hi] += rel_ref[1]
    com_b.start()
    own = y * n_pp + p
    square = jnp.zeros((8, 128), F32)
    one_a.wait_recv()
    one_b.wait_recv()
    for half, cp in ((0, com_a), (1, com_b)):
        cp.wait_recv()
        for q in range(2):
            total = (part_ref[y, 2 * half + q] + com_ref[half, q] + one_ref[half, q]) * (1.0 / n_dp)
            g_ref[own, 2 * half + q] = total
            lanes = jnp.sum((total * total).reshape(rows // 8, 8, dq), axis=0)
            for i in range(0, dq, 128):
                square = square + lanes[:, i:i + 128]

    def block(xx, yy):
        return lax.rem(yy + 2 * n_dp, n_dp) * n_pp + 2 * lax.rem(xx + 2 * n_x, n_x) + c

    colours = []
    for q, (axes, sign) in enumerate((("xy", 1), ("xy", -1), ("yx", 1), ("yx", -1))):
        sizes = (n_x, n_dp) if axes == "xy" else (n_dp, n_x)
        to_x = {"pp": 2 * lax.rem(x + sign + n_x, n_x) + c}
        to_y = {"dp": lax.rem(y + sign + n_dp, n_dp)}
        dest = (to_x, to_y) if axes == "xy" else (to_y, to_x)
        colours.append((q, axes, sign, sizes, dest, ring_plan(*sizes)))

    def holder(axes, sign, s, t):
        return block(x - sign * s, y - sign * t) if axes == "xy" else block(x - sign * t, y - sign * s)

    def message(colour, item, coming):
        q, axes, sign, _, dest, plan = colour
        phase, s, t = item
        at = plan.index(item)
        s_at, t_at = (s + coming, t) if phase == 1 else (s, t + coming)
        b = holder(axes, sign, s_at, t_at)
        return remote(g_ref.at[b, q], g_ref.at[b, q], ag_s.at[q, at], ag_r.at[q, at], dest[phase - 1])

    def mate_copy(q, slot, b):
        return remote(g_ref.at[b, q], g_ref.at[b, q], d_s.at[q, slot], d_r.at[q, slot], {"pp": mate})

    sends = []

    def push(cp):
        cp.start()
        sends.append(cp)

    for colour in colours:
        if colour[3][0] > 1:
            push(message(colour, (1, 0, 0), 0))
    for colour in colours:
        if colour[3][1] > 1:
            push(message(colour, (2, 0, 0), 0))

    def norm_swap(value, buf, send, recv, axis, me, n):
        buf[me] = value
        return [remote(buf.at[me], buf.at[me], send.at[o - 1], recv.at[o - 1], {axis: lax.rem(me + o, n)}) for o in range(1, n)], [
            remote(buf.at[lax.rem(me + n - o, n)], buf.at[lax.rem(me + n - o, n)], send.at[o - 1], recv.at[o - 1], {axis: lax.rem(me + o, n)}) for o in range(1, n)]

    norm_out, norm_in = norm_swap(square, nb_p, np_s, np_r, "pp", p, n_pp)
    for cp in norm_out:
        push(cp)
    for q in range(4):
        push(mate_copy(q, 0, own))

    steps = n_x * n_dp - 1
    for i in range(steps):
        for colour in colours:
            q, axes, sign, sizes, dest, plan = colour
            phase, s, t = plan[i]
            message(colour, plan[i], 1).wait_recv()
            if phase == 1:
                if s + 1 < sizes[0] - 1:
                    push(message(colour, (1, s + 1, 0), 0))
                if sizes[1] > 1:
                    push(message(colour, (2, s + 1, 0), 0))
                push(mate_copy(q, i + 1, holder(axes, sign, s + 1, 0)))
            else:
                if t + 1 < sizes[1] - 1:
                    push(message(colour, (2, s, t + 1), 0))
                push(mate_copy(q, i + 1, holder(axes, sign, s, t + 1)))
        if i == 0:
            for cp in norm_in:
                cp.wait_recv()
            total = nb_p[0]
            for o in range(1, n_pp):
                total = total + nb_p[o]
            norm_out, norm_in = norm_swap(total, nb_y, ny_s, ny_r, "dp", y, n_dp)
            for cp in norm_out:
                push(cp)
        if i == 1:
            for cp in norm_in:
                cp.wait_recv()
            total = nb_y[0]
            for o in range(1, n_dp):
                total = total + nb_y[o]
            norm_out, norm_in = norm_swap(total, nb_z, nz_s, nz_r, "tp", z, n_tp)
            for cp in norm_out:
                push(cp)
        if i == 2:
            for cp in norm_in:
                cp.wait_recv()
            total = nb_z[0]
            for o in range(1, n_tp):
                total = total + nb_z[o]
            norm = jnp.sqrt(jnp.sum(total, axis=(0, 1), keepdims=True))
            scale_ref[...] = jnp.broadcast_to(CLIP_NORM / jnp.maximum(norm, CLIP_NORM), (8, 128))

    for q, axes, sign, sizes, dest, plan in colours:
        for i in range(steps + 1):
            if i == 0:
                b = own
            else:
                phase, s, t = plan[i - 1]
                b = holder(axes, sign, s + 1, 0) if phase == 1 else holder(axes, sign, s, t + 1)
            mate_copy(q, i, b + 1 - 2 * c).wait_recv()
    for cp in (rel_a, rel_b, one_a, one_b, com_a, com_b, *sends):
        cp.wait_send()


def plane_gradient(table, hid, dx, labels, lookup, n_tp, n_dp, n_pp, vocab):
    _, rows, dim = table.shape
    tok = hid.shape[0]
    dq = dim // 4
    steps = (n_pp // 2) * n_dp
    full = pl.BlockSpec(memory_space=VMEM)
    half = VMEM((2, 2, rows, dq), F32)
    return pl.pallas_call(
        functools.partial(grad_kernel, n_tp, n_dp, n_pp, vocab),
        out_shape=(VMEM((n_dp * n_pp, 4, rows, dq), F32), jax.ShapeDtypeStruct((8, 128), F32)),
        in_specs=[full] * 5,
        out_specs=(full, full),
        scratch_shapes=[
            VMEM((n_dp, rows, tok), F32), VMEM((rows, tok), BF16), VMEM((n_dp, 4, rows, dq), F32),
            VMEM((2, tok), F32), VMEM((2, tok), F32), VMEM((n_pp - 1, 2, tok), F32), VMEM((n_tp - 1, 2, tok), F32),
            half, half, half,
            VMEM((n_pp, 8, 128), F32), VMEM((n_dp, 8, 128), F32), VMEM((n_tp, 8, 128), F32),
            DMA((n_pp - 1,)), DMA((n_pp - 1,)), DMA((n_tp - 1,)), DMA((n_tp - 1,)), DMA((6,)), DMA((6,)),
            DMA((n_pp - 1,)), DMA((n_pp - 1,)), DMA((n_dp - 1,)), DMA((n_dp - 1,)), DMA((n_tp - 1,)), DMA((n_tp - 1,)),
            DMA((4, steps)), DMA((4, steps)), DMA((4, steps)), DMA((4, steps)),
        ],
        compiler_params=pltpu.CompilerParams(collective_id=1, has_side_effects=True, vmem_limit_bytes=22 << 20),
        name="plane_gradient",
    )(in_vmem(table), in_vmem(hid), in_vmem(dx), labels, lookup)


def adamw_kernel(scale_ref, g_ref, e_ref, m_ref, v_ref, ne_ref, nm_ref, nv_ref, nb_ref):
    i = pl.program_id(0)
    dq = g_ref.shape[3]
    scale = scale_ref[0:1, 0:1]
    for q in range(4):
        cols = pl.ds(q * dq, dq)
        g = g_ref[i, q] * scale
        e = e_ref[:, cols]
        m = BETA_ONE * m_ref[:, cols] + (1.0 - BETA_ONE) * g
        v = BETA_TWO * v_ref[:, cols] + (1.0 - BETA_TWO) * g * g
        step = (m * (1.0 / (1.0 - BETA_ONE ** OPT_STEP))) / (jnp.sqrt(v * (1.0 / (1.0 - BETA_TWO ** OPT_STEP))) + ADAM_EPS)
        ne = e - LEARN_RATE * (step + WEIGHT_DECAY * e)
        ne_ref[:, cols] = ne
        nm_ref[:, cols] = m
        nv_ref[:, cols] = v
        nb_ref[:, cols] = ne.astype(BF16)


def adamw(scale, grad, master, exp_avg, exp_avg_sq):
    vocab, dim = master.shape
    tile = grad.shape[2]
    spec = pl.BlockSpec((tile, dim), lambda i: (i, 0))
    full = pl.BlockSpec(memory_space=VMEM)
    f32 = jax.ShapeDtypeStruct((vocab, dim), F32)
    count = vocab * dim
    return pl.pallas_call(
        adamw_kernel,
        out_shape=(f32, f32, f32, jax.ShapeDtypeStruct((vocab, dim), BF16)),
        grid=(grad.shape[0],),
        in_specs=[full, full, spec, spec, spec],
        out_specs=(spec,) * 4,
        cost_estimate=pl.CostEstimate(flops=20 * count, bytes_accessed=30 * count, transcendentals=2 * count),
        compiler_params=pltpu.CompilerParams(vmem_limit_bytes=32 << 20),
        name="adamw",
    )(scale, in_vmem(grad), master, exp_avg, exp_avg_sq)


def own_rows(master, n_dp, n_pp, rows):
    vocab, dim = master.shape
    p = lax.axis_index("pp")
    blocks = []
    for d in range(n_dp):
        first = (d * n_pp + p) * rows
        short = max(0, (d + 1) * n_pp * rows - vocab)
        start = jnp.minimum(first, vocab - rows)
        blk = lax.dynamic_slice_in_dim(master, start, rows, 0).astype(BF16)
        if short:
            blk = jnp.concatenate([blk, jnp.zeros((short, dim), BF16)], 0)
            blk = lax.dynamic_slice_in_dim(blk, first - start, rows, 0)
        blocks.append(blk)
    return jnp.stack(blocks)


def solution(mesh):
    n_pp, n_dp, n_tp = mesh.shape["pp"], mesh.shape["dp"], mesh.shape["tp"]
    table_spec = P("tp", None)

    def device_step(master, exp_avg, exp_avg_sq, stage_ids, stage_acts):
        vocab, dim = master.shape
        tok = stage_ids.shape[1] * stage_ids.shape[2]
        rows = -(-vocab // (n_pp * n_dp))
        rows = -(-rows // 8) * 8
        acts = stage_acts.reshape(tok, dim).astype(F32)
        hid, dx, labels, lookup = spread(acts, stage_ids.reshape(1, tok), n_tp, n_pp)
        table = own_rows(master, n_dp, n_pp, rows)
        grad, scale = plane_gradient(table, hid, dx, labels, lookup, n_tp, n_dp, n_pp, vocab)
        return adamw(scale, grad, master, exp_avg, exp_avg_sq)

    return jax.shard_map(device_step, mesh=mesh, in_specs=(table_spec, table_spec, table_spec, P("pp", "dp", None), P("pp", "dp", None, None)), out_specs=(table_spec, table_spec, table_spec, table_spec), check_vma=False)
```

```python
import functools

import jax
import jax.numpy as jnp
from jax import lax
from jax.experimental import pallas as pl
from jax.experimental.pallas import tpu as pltpu
from jax.sharding import PartitionSpec as P

LEARN_RATE = 0.003
BETA_ONE = 0.9
BETA_TWO = 0.95
ADAM_EPS = 1e-8
WEIGHT_DECAY = 0.1
CLIP_NORM = 1.0
OPT_STEP = 10

MESH_ID = pl.DeviceIdType.MESH
LOW = -1e30
VMEM = pltpu.VMEM
DMA = pltpu.SemaphoreType.DMA
F32, BF16 = jnp.float32, jnp.bfloat16


def remote(src, dst, send, recv, where):
    return pltpu.make_async_remote_copy(src_ref=src, dst_ref=dst, send_sem=send, recv_sem=recv, device_id=where, device_id_type=MESH_ID)


def in_vmem(arr):
    return pltpu.with_memory_space_constraint(arr, VMEM)


def enter(groups):
    barrier = pltpu.get_barrier_semaphore()
    for axis, peer in groups:
        pl.semaphore_signal(barrier, inc=1, device_id={axis: peer}, device_id_type=MESH_ID)
    pl.semaphore_wait(barrier, len(groups))


def ring_plan(n_one, n_two):
    items = [(1, s, 0) for s in range(n_one - 1)] + [(2, s, t) for s in range(n_one) for t in range(n_two - 1)]
    return sorted(items, key=lambda i: (i[1] + i[2], i[0], i[2]))


def grad_kernel(n_tp, n_dp, n_pp, n_chunk, table_ref, acts_ref, ids_ref, g_ref, scale_ref, hid_buf, dx_buf, hid_ref, dx_ref, lab_ref, look_ref, tab_ref, exp_ref, dl_ref, part_ref, stat_ref, mid_ref, buf_p, buf_z, rel_ref, one_ref, com_ref, nb_p, nb_y, nb_z, load_s, feed_s, send_x, send_z, send_d, send_e, recv_x, recv_z, recv_d, recv_e, id_s, id_r, sp_s, sp_r, sz_s, sz_r, rs_s, rs_r, np_s, np_r, ny_s, ny_r, nz_s, nz_r, ag_s, ag_r, d_s, d_r):
    p, z, y = lax.axis_index("pp"), lax.axis_index("tp"), lax.axis_index("dp")
    n_x = n_pp // 2
    x, c, par = p // 2, lax.rem(p, 2), lax.rem(z, 2)
    mate = 2 * x + 1 - c
    vocab = table_ref.shape[0]
    rows, tok = exp_ref.shape[1:]
    dq = g_ref.shape[3]
    up_y, down_y = lax.rem(y + 1, n_dp), lax.rem(y + n_dp - 1, n_dp)

    def first_row(d):
        return (d * n_pp + p) * rows

    short = vocab - (n_dp * n_pp - 1) * rows

    def table_copies(count, blocks):
        return [pltpu.make_async_copy(table_ref.at[pl.ds(pl.multiple_of(first_row(d), 8), count), pl.ds(q * dq, dq)], part_ref.at[d, q, pl.ds(0, count)], load_s.at[1 + 4 * d + q]) for d in blocks for q in range(4)]

    def each_table_copy(act):
        for cp in table_copies(rows, range(n_dp - 1)):
            act(cp)
        for cond, count in ((p < n_pp - 1, rows), (p == n_pp - 1, short)):
            @pl.when(cond)
            def _(count=count):
                for cp in table_copies(count, (n_dp - 1,)):
                    act(cp)

    each_table_copy(lambda cp: cp.start())
    sources = ((n_pp - 1, hid_buf, hid_ref, lab_ref), (0, dx_buf, dx_ref, look_ref))
    for source, _, low, _ in sources:
        @pl.when(p == source)
        def _(low=low):
            pltpu.make_async_copy(acts_ref, low, load_s.at[0]).start()

    enter([("pp", lax.rem(p + o, n_pp)) for o in range(1, n_pp)] + [("tp", lax.rem(z + o, n_tp)) for o in range(1, n_tp)] + [("dp", lax.rem(y + o, n_dp)) for o in range(1, n_dp)])

    step_x = 1 - 2 * c
    next_p = 2 * lax.rem(x + step_x + n_x, n_x) + c
    next_z = lax.rem(z + step_x + n_tp, n_tp)
    size = tok // (4 * n_chunk)
    lag = 2

    def span(core, parity, k):
        return pl.ds(pl.multiple_of(((2 * parity + core) * n_chunk + k) * size, 8), size)

    class Stream:
        def __init__(self, a):
            self.a = a
            self.source, self.buf, self.low, self.ids = sources[a]
            self.is_src = p == self.source
            s_x = self.source // 2
            self.dist = lax.rem(jnp.where(c == 0, x - s_x, s_x - x) + n_x, n_x)

        def hop(self, part, send, recv, where):
            return remote(self.buf.at[part], self.buf.at[part], send, recv, where)

        def feed(self, k):
            return self.hop(span(1 - c, par, k), feed_s.at[self.a, k], recv_x.at[self.a, k], {"pp": mate})

        def ring(self, k):
            return self.hop(span(c, par, k), send_x.at[self.a, k], recv_x.at[self.a, k], {"pp": next_p})

        def plane(self, k, parity):
            return self.hop(span(c, parity, k), send_z.at[self.a, k], recv_z.at[self.a, k], {"tp": next_z})

        def across(self, k, core):
            return self.hop(span(core, par, k), send_d.at[self.a, k], recv_d.at[self.a, k], {"pp": mate})

        def again(self, k, core):
            return self.hop(span(core, 1 - par, k), send_e.at[self.a, k], recv_e.at[self.a, k], {"pp": mate})

        def id_copy(self, o):
            return remote(ids_ref, self.ids, id_s.at[self.a, o - 1], id_r.at[self.a], {"pp": lax.rem(p + o, n_pp)})

        def begin(self):
            @pl.when(self.is_src)
            def _():
                pltpu.make_async_copy(acts_ref, self.low, load_s.at[0]).wait()
                self.ids[...] = ids_ref[...]

                @pl.loop(0, n_chunk)
                def _(k):
                    def widen(part):
                        self.buf[part, :] = self.low[part, :].astype(F32)

                    widen(span(1 - c, par, k))
                    self.feed(k).start()
                    widen(span(c, par, k))
                    if n_x > 1:
                        self.ring(k).start()
                    self.across(k, c).start()
                    widen(span(c, 1 - par, k))
                    self.again(k, c).start()

                for o in range(1, n_pp):
                    self.id_copy(o).start()

        def steps(self, lo, hi):
            @pl.when(jnp.logical_not(self.is_src))
            def _():
                @pl.loop(lo, hi)
                def _(k):
                    @pl.when(k < n_chunk)
                    def _():
                        self.ring(k).wait_recv()
                        if n_x > 1:
                            @pl.when(self.dist < n_x - 1)
                            def _():
                                self.ring(k).start()

                        self.plane(k, par).start()

                        @pl.when(mate != self.source)
                        def _():
                            self.across(k, c).start()

                    @pl.when(k >= lag)
                    def _():
                        self.plane(k - lag, 1 - par).wait_recv()

                        @pl.when(mate != self.source)
                        def _():
                            self.again(k - lag, c).start()

        def collect(self):
            @pl.when(jnp.logical_not(self.is_src))
            def _():
                self.id_copy(1).wait_recv()

                @pl.loop(0, n_chunk)
                def _(k):
                    self.across(k, 1 - c).wait_recv()
                    self.again(k, 1 - c).wait_recv()

                tile = min(128, tok)

                @pl.loop(0, tok // tile)
                def _(k):
                    here = pl.ds(pl.multiple_of(k * tile, tile), tile)
                    self.low[here, :] = self.buf[here, :].astype(BF16)

        def settle(self):
            @pl.when(self.is_src)
            def _():
                for o in range(1, n_pp):
                    self.id_copy(o).wait_send()

            @pl.loop(0, n_chunk)
            def _(k):
                @pl.when(self.is_src)
                def _():
                    self.feed(k).wait_send()

                @pl.when(jnp.logical_not(self.is_src))
                def _():
                    self.plane(k, par).wait_send()

                if n_x > 1:
                    @pl.when(self.dist < n_x - 1)
                    def _():
                        self.ring(k).wait_send()

                @pl.when(mate != self.source)
                def _():
                    self.across(k, c).wait_send()
                    self.again(k, c).wait_send()

    hid_in, dx_in = Stream(0), Stream(1)
    hid_in.begin()
    each_table_copy(lambda cp: cp.wait())
    for d in range(n_dp):
        for q in range(4):
            tab_ref[d, :, q * dq:(q + 1) * dq] = part_ref[d, q].astype(BF16)
    hid_in.steps(0, n_chunk + lag)
    dx_in.begin()
    hid_in.collect()

    wide = min(256, tok)

    @pl.loop(0, tok // wide)
    def _(j):
        cols = pl.ds(pl.multiple_of(j * wide, wide), wide)
        h = hid_ref[cols, :]
        top = jnp.full((1, wide), LOW, F32)
        for d in range(n_dp):
            lg = lax.dot_general(tab_ref[d], h, (((1,), (1,)), ((), ())), preferred_element_type=F32)
            if d == n_dp - 1 and short < rows:
                ok = first_row(d) + lax.broadcasted_iota(jnp.int32, (rows, wide), 0) < vocab
                lg = jnp.where(ok, lg, LOW)
            exp_ref[d, :, cols] = lg
            top = jnp.maximum(top, jnp.max(lg, axis=0, keepdims=True))
        tot = jnp.zeros((1, wide), F32)
        for d in range(n_dp):
            e = jnp.exp(exp_ref[d, :, cols] - top)
            exp_ref[d, :, cols] = e
            tot = tot + jnp.sum(e, axis=0, keepdims=True)
        stat_ref[0:1, cols] = top
        stat_ref[1:2, cols] = tot

    def swap(src, buf, send, recv, axis, me, n):
        return [remote(src, buf.at[o - 1], send.at[o - 1], recv.at[o - 1], {axis: lax.rem(me + o, n)}) for o in range(1, n)]

    def merge(src, buf, n):
        top = src[0:1, :]
        for o in range(1, n):
            top = jnp.maximum(top, buf[o - 1, 0:1, :])
        tot = src[1:2, :] * jnp.exp(src[0:1, :] - top)
        for o in range(1, n):
            tot = tot + buf[o - 1, 1:2, :] * jnp.exp(buf[o - 1, 0:1, :] - top)
        return top, tot

    def local_ids(ref):
        ids = ref[...] - z * vocab
        return jnp.where(ids < vocab, ids, -1)

    def row_ids(d):
        return first_row(d) + lax.broadcasted_iota(jnp.int32, (rows, tok), 0)

    third = (n_chunk + lag) // 3
    stage = swap(stat_ref, buf_p, sp_s, sp_r, "pp", p, n_pp)
    for cp in stage:
        cp.start()
    dx_in.steps(0, third)
    for cp in stage:
        cp.wait()
    top, tot = merge(stat_ref, buf_p, n_pp)
    mid_ref[0:1, :] = top
    mid_ref[1:2, :] = tot
    stage = swap(mid_ref, buf_z, sz_s, sz_r, "tp", z, n_tp)
    for cp in stage:
        cp.start()
    dx_in.steps(third, 2 * third)
    for cp in stage:
        cp.wait()
    top, tot = merge(mid_ref, buf_z, n_tp)
    mid_ref[0:1, :] = jnp.exp(stat_ref[0:1, :] - top) / (tot * tok)

    def head(d):
        prob = exp_ref[d] * mid_ref[0:1, :]
        hit = local_ids(lab_ref) == row_ids(d)
        dl_ref[...] = jnp.where(hit, prob - 1.0 / tok, prob).astype(BF16)
        for q in range(4):
            part_ref[d, q] = jnp.dot(dl_ref[...], hid_ref[:, q * dq:(q + 1) * dq], preferred_element_type=F32)

    def lookup(d):
        dl_ref[...] = (local_ids(look_ref) == row_ids(d)).astype(BF16)
        for q in range(4):
            part_ref[d, q] += jnp.dot(dl_ref[...], dx_ref[:, q * dq:(q + 1) * dq], preferred_element_type=F32)

    pl.loop(0, n_dp)(head)
    dx_in.steps(2 * third, n_chunk + lag)
    dx_in.collect()

    lo, hi = pl.ds(0, 2), pl.ds(2, 2)
    far = lax.rem(y + 2, n_dp)
    rel_a = remote(part_ref.at[far, lo], rel_ref.at[0], rs_s.at[0], rs_r.at[0], {"dp": up_y})
    rel_b = remote(part_ref.at[far, hi], rel_ref.at[1], rs_s.at[1], rs_r.at[1], {"dp": down_y})
    one_b = remote(part_ref.at[up_y, hi], one_ref.at[1], rs_s.at[2], rs_r.at[2], {"dp": up_y})
    one_a = remote(part_ref.at[down_y, lo], one_ref.at[0], rs_s.at[3], rs_r.at[3], {"dp": down_y})
    com_a = remote(part_ref.at[up_y, lo], com_ref.at[0], rs_s.at[4], rs_r.at[4], {"dp": up_y})
    com_b = remote(part_ref.at[down_y, hi], com_ref.at[1], rs_s.at[5], rs_r.at[5], {"dp": down_y})
    lookup(far)
    rel_a.start()
    rel_b.start()
    lookup(up_y)
    one_b.start()
    lookup(down_y)
    one_a.start()
    lookup(y)
    rel_a.wait_recv()
    part_ref[up_y, lo] += rel_ref[0]
    com_a.start()
    rel_b.wait_recv()
    part_ref[down_y, hi] += rel_ref[1]
    com_b.start()
    own = y * n_pp + p
    square = jnp.zeros((8, 128), F32)
    one_a.wait_recv()
    one_b.wait_recv()
    for half, cp in ((0, com_a), (1, com_b)):
        cp.wait_recv()
        for q in range(2):
            total = (part_ref[y, 2 * half + q] + com_ref[half, q] + one_ref[half, q]) * (1.0 / n_dp)
            g_ref[own, 2 * half + q] = total
            lanes = jnp.sum((total * total).reshape(rows // 8, 8, dq), axis=0)
            for i in range(0, dq, 128):
                square = square + lanes[:, i:i + 128]

    def block(xx, yy):
        return lax.rem(yy + 2 * n_dp, n_dp) * n_pp + 2 * lax.rem(xx + 2 * n_x, n_x) + c

    colours = []
    for q, (axes, sign) in enumerate((("xy", 1), ("xy", -1), ("yx", 1), ("yx", -1))):
        sizes = (n_x, n_dp) if axes == "xy" else (n_dp, n_x)
        to_x = {"pp": 2 * lax.rem(x + sign + n_x, n_x) + c}
        to_y = {"dp": lax.rem(y + sign + n_dp, n_dp)}
        dest = (to_x, to_y) if axes == "xy" else (to_y, to_x)
        colours.append((q, axes, sign, sizes, dest, ring_plan(*sizes)))

    def holder(axes, sign, s, t):
        return block(x - sign * s, y - sign * t) if axes == "xy" else block(x - sign * t, y - sign * s)

    def message(colour, item, coming):
        q, axes, sign, _, dest, plan = colour
        phase, s, t = item
        at = plan.index(item)
        s_at, t_at = (s + coming, t) if phase == 1 else (s, t + coming)
        b = holder(axes, sign, s_at, t_at)
        return remote(g_ref.at[b, q], g_ref.at[b, q], ag_s.at[q, at], ag_r.at[q, at], dest[phase - 1])

    def mate_copy(q, slot, b):
        return remote(g_ref.at[b, q], g_ref.at[b, q], d_s.at[q, slot], d_r.at[q, slot], {"pp": mate})

    sends = []

    def push(cp):
        cp.start()
        sends.append(cp)

    for colour in colours:
        if colour[3][0] > 1:
            push(message(colour, (1, 0, 0), 0))
    for colour in colours:
        if colour[3][1] > 1:
            push(message(colour, (2, 0, 0), 0))

    def norm_swap(value, buf, send, recv, axis, me, n):
        buf[me] = value
        return [remote(buf.at[me], buf.at[me], send.at[o - 1], recv.at[o - 1], {axis: lax.rem(me + o, n)}) for o in range(1, n)], [
            remote(buf.at[lax.rem(me + n - o, n)], buf.at[lax.rem(me + n - o, n)], send.at[o - 1], recv.at[o - 1], {axis: lax.rem(me + o, n)}) for o in range(1, n)]

    norm_out, norm_in = norm_swap(square, nb_p, np_s, np_r, "pp", p, n_pp)
    for cp in norm_out:
        push(cp)
    for q in range(4):
        push(mate_copy(q, 0, own))

    steps = n_x * n_dp - 1
    for i in range(steps):
        for colour in colours:
            q, axes, sign, sizes, dest, plan = colour
            phase, s, t = plan[i]
            message(colour, plan[i], 1).wait_recv()
            if phase == 1:
                if s + 1 < sizes[0] - 1:
                    push(message(colour, (1, s + 1, 0), 0))
                if sizes[1] > 1:
                    push(message(colour, (2, s + 1, 0), 0))
                push(mate_copy(q, i + 1, holder(axes, sign, s + 1, 0)))
            else:
                if t + 1 < sizes[1] - 1:
                    push(message(colour, (2, s, t + 1), 0))
                push(mate_copy(q, i + 1, holder(axes, sign, s, t + 1)))
        if i == 0:
            for cp in norm_in:
                cp.wait_recv()
            total = nb_p[0]
            for o in range(1, n_pp):
                total = total + nb_p[o]
            norm_out, norm_in = norm_swap(total, nb_y, ny_s, ny_r, "dp", y, n_dp)
            for cp in norm_out:
                push(cp)
        if i == 1:
            for cp in norm_in:
                cp.wait_recv()
            total = nb_y[0]
            for o in range(1, n_dp):
                total = total + nb_y[o]
            norm_out, norm_in = norm_swap(total, nb_z, nz_s, nz_r, "tp", z, n_tp)
            for cp in norm_out:
                push(cp)
        if i == 2:
            for cp in norm_in:
                cp.wait_recv()
            total = nb_z[0]
            for o in range(1, n_tp):
                total = total + nb_z[o]
            norm = jnp.sqrt(jnp.sum(total, axis=(0, 1), keepdims=True))
            scale_ref[...] = jnp.broadcast_to(CLIP_NORM / jnp.maximum(norm, CLIP_NORM), (8, 128))

    for q, axes, sign, sizes, dest, plan in colours:
        for i in range(steps + 1):
            if i == 0:
                b = own
            else:
                phase, s, t = plan[i - 1]
                b = holder(axes, sign, s + 1, 0) if phase == 1 else holder(axes, sign, s, t + 1)
            mate_copy(q, i, b + 1 - 2 * c).wait_recv()
    for cp in (rel_a, rel_b, one_a, one_b, com_a, com_b, *sends):
        cp.wait_send()
    hid_in.settle()
    dx_in.settle()


def plane_gradient(master, acts, ids, n_tp, n_dp, n_pp):
    vocab, dim = master.shape
    tok = acts.shape[0]
    rows = -(-vocab // (n_pp * n_dp))
    rows = -(-rows // 8) * 8
    dq = dim // 4
    n_chunk = 12 if tok % (4 * 12 * 8) == 0 else 2
    steps = (n_pp // 2) * n_dp
    full = pl.BlockSpec(memory_space=VMEM)
    any_space = pl.BlockSpec(memory_space=pl.ANY)
    half = VMEM((2, 2, rows, dq), F32)
    chunk = DMA((2, n_chunk))
    return pl.pallas_call(
        functools.partial(grad_kernel, n_tp, n_dp, n_pp, n_chunk),
        out_shape=(VMEM((n_dp * n_pp, 4, rows, dq), F32), jax.ShapeDtypeStruct((8, 128), F32)),
        in_specs=[any_space, any_space, full],
        out_specs=(full, full),
        scratch_shapes=[
            VMEM((tok, dim), F32), VMEM((tok, dim), F32), VMEM((tok, dim), BF16), VMEM((tok, dim), BF16),
            VMEM((1, tok), jnp.int32), VMEM((1, tok), jnp.int32), VMEM((n_dp, rows, dim), BF16),
            VMEM((n_dp, rows, tok), F32), VMEM((rows, tok), BF16), VMEM((n_dp, 4, rows, dq), F32),
            VMEM((2, tok), F32), VMEM((2, tok), F32), VMEM((n_pp - 1, 2, tok), F32), VMEM((n_tp - 1, 2, tok), F32),
            half, half, half,
            VMEM((n_pp, 8, 128), F32), VMEM((n_dp, 8, 128), F32), VMEM((n_tp, 8, 128), F32),
            DMA((1 + 4 * n_dp,)), *[chunk] * 9, DMA((2, n_pp - 1)), DMA((2,)),
            DMA((n_pp - 1,)), DMA((n_pp - 1,)), DMA((n_tp - 1,)), DMA((n_tp - 1,)), DMA((6,)), DMA((6,)),
            DMA((n_pp - 1,)), DMA((n_pp - 1,)), DMA((n_dp - 1,)), DMA((n_dp - 1,)), DMA((n_tp - 1,)), DMA((n_tp - 1,)),
            DMA((4, steps)), DMA((4, steps)), DMA((4, steps)), DMA((4, steps)),
        ],
        compiler_params=pltpu.CompilerParams(collective_id=0, has_side_effects=True, vmem_limit_bytes=34 << 20),
        name="plane_gradient",
    )(master, acts, ids)


def adamw_kernel(n_slot, ahead, scale_ref, g_ref, e_hbm, m_hbm, v_hbm, ne_hbm, nm_hbm, nv_hbm, nb_hbm, e_buf, m_buf, v_buf, b_buf, in_s, out_s):
    n_blk, _, rows, dq = g_ref.shape
    vocab = e_hbm.shape[0]
    last = vocab - (n_blk - 1) * rows
    scale = scale_ref[0:1, 0:1]

    def loads(i, count):
        slot = lax.rem(i, n_slot)
        here = pl.ds(pl.multiple_of(i * rows, 8), count)
        return [pltpu.make_async_copy(hbm.at[here], buf.at[slot, pl.ds(0, count)], in_s.at[a, slot]) for a, (hbm, buf) in enumerate(((e_hbm, e_buf), (m_hbm, m_buf), (v_hbm, v_buf)))]

    def stores(i, count):
        slot = lax.rem(i, n_slot)
        here = pl.ds(pl.multiple_of(i * rows, 8), count)
        return [pltpu.make_async_copy(buf.at[slot, pl.ds(0, count)], hbm.at[here], out_s.at[a, slot]) for a, (buf, hbm) in enumerate(((e_buf, ne_hbm), (m_buf, nm_hbm), (v_buf, nv_hbm), (b_buf, nb_hbm)))]

    def each(copies, i, act):
        if last == rows:
            for cp in copies(i, rows):
                act(cp)
            return
        for cond, count in ((i < n_blk - 1, rows), (i == n_blk - 1, last)):
            @pl.when(cond)
            def _(count=count):
                for cp in copies(i, count):
                    act(cp)

    for i in range(min(ahead, n_blk)):
        each(loads, i, lambda cp: cp.start())

    @pl.loop(0, n_blk)
    def _(i):
        slot = lax.rem(i, n_slot)

        @pl.when(i + ahead < n_blk)
        def _():
            @pl.when(i + ahead >= n_slot)
            def _():
                each(stores, i + ahead - n_slot, lambda cp: cp.wait())

            each(loads, i + ahead, lambda cp: cp.start())

        each(loads, i, lambda cp: cp.wait())

        @pl.loop(0, rows // 8, unroll=5 if rows % 40 == 0 else 1)
        def _(r):
            at = pl.ds(pl.multiple_of(r * 8, 8), 8)
            for q in range(4):
                cols = pl.ds(q * dq, dq)
                g = g_ref[i, q, at, :] * scale
                e = e_buf[slot, at, cols]
                m = BETA_ONE * m_buf[slot, at, cols] + (1.0 - BETA_ONE) * g
                v = BETA_TWO * v_buf[slot, at, cols] + (1.0 - BETA_TWO) * g * g
                step = (m * (1.0 / (1.0 - BETA_ONE ** OPT_STEP))) / (jnp.sqrt(v * (1.0 / (1.0 - BETA_TWO ** OPT_STEP))) + ADAM_EPS)
                ne = e - LEARN_RATE * (step + WEIGHT_DECAY * e)
                e_buf[slot, at, cols] = ne
                m_buf[slot, at, cols] = m
                v_buf[slot, at, cols] = v
                b_buf[slot, at, cols] = ne.astype(BF16)

        each(stores, i, lambda cp: cp.start())

    for i in range(max(0, n_blk - n_slot), n_blk):
        each(stores, i, lambda cp: cp.wait())


def adamw(scale, grad, master, exp_avg, exp_avg_sq):
    vocab, dim = master.shape
    rows = grad.shape[2]
    n_slot = 6
    full = pl.BlockSpec(memory_space=VMEM)
    any_space = pl.BlockSpec(memory_space=pl.ANY)
    f32 = jax.ShapeDtypeStruct((vocab, dim), F32)
    count = vocab * dim
    ring = VMEM((n_slot, rows, dim), F32)
    return pl.pallas_call(
        functools.partial(adamw_kernel, n_slot, 3),
        out_shape=(f32, f32, f32, jax.ShapeDtypeStruct((vocab, dim), BF16)),
        in_specs=[full, full, any_space, any_space, any_space],
        out_specs=(any_space,) * 4,
        scratch_shapes=[ring, ring, ring, VMEM((n_slot, rows, dim), BF16), DMA((3, n_slot)), DMA((4, n_slot))],
        cost_estimate=pl.CostEstimate(flops=20 * count, bytes_accessed=30 * count, transcendentals=2 * count),
        compiler_params=pltpu.CompilerParams(vmem_limit_bytes=32 << 20),
        name="adamw",
    )(scale, in_vmem(grad), master, exp_avg, exp_avg_sq)


def solution(mesh):
    n_pp, n_dp, n_tp = mesh.shape["pp"], mesh.shape["dp"], mesh.shape["tp"]
    table_spec = P("tp", None)

    def device_step(master, exp_avg, exp_avg_sq, stage_ids, stage_acts):
        vocab, dim = master.shape
        tok = stage_ids.shape[1] * stage_ids.shape[2]
        acts = stage_acts.reshape(tok, dim)
        grad, scale = plane_gradient(master, acts, stage_ids.reshape(1, tok), n_tp, n_dp, n_pp)
        return adamw(scale, grad, master, exp_avg, exp_avg_sq)

    return jax.shard_map(device_step, mesh=mesh, in_specs=(table_spec, table_spec, table_spec, P("pp", "dp", None), P("pp", "dp", None, None)), out_specs=(table_spec, table_spec, table_spec, table_spec), check_vma=False)
```

```python
import functools

import jax
import jax.numpy as jnp
from jax import lax
from jax.experimental import pallas as pl
from jax.experimental.pallas import tpu as pltpu
from jax.sharding import PartitionSpec as P

LEARN_RATE = 0.003
BETA_ONE = 0.9
BETA_TWO = 0.95
ADAM_EPS = 1e-8
WEIGHT_DECAY = 0.1
CLIP_NORM = 1.0
OPT_STEP = 10

MESH_ID = pl.DeviceIdType.MESH
LOW = -1e30
VMEM = pltpu.VMEM
DMA = pltpu.SemaphoreType.DMA
F32, BF16 = jnp.float32, jnp.bfloat16
PRE_BLOCKS = 6
scope = jax.named_scope


def remote(src, dst, send, recv, where):
    return pltpu.make_async_remote_copy(src_ref=src, dst_ref=dst, send_sem=send, recv_sem=recv, device_id=where, device_id_type=MESH_ID)


def in_vmem(arr):
    return pltpu.with_memory_space_constraint(arr, VMEM)


def enter(groups):
    barrier = pltpu.get_barrier_semaphore()
    for axis, peer in groups:
        pl.semaphore_signal(barrier, inc=1, device_id={axis: peer}, device_id_type=MESH_ID)
    pl.semaphore_wait(barrier, len(groups))


def ring_plan(n_one, n_two):
    items = [(1, s, 0) for s in range(n_one - 1)] + [(2, s, t) for s in range(n_one) for t in range(n_two - 1)]
    return sorted(items, key=lambda i: (i[1] + i[2], i[0], i[2]))


def grad_kernel(n_tp, n_dp, n_pp, n_chunk, lag, table_ref, acts_ref, ids_ref, avg_ref, sq_ref, g_ref, scale_ref, pre_ref, hid_ref, dx_ref, lab_ref, look_ref, tab_ref, exp_ref, dl_ref, part_ref, stat_ref, mid_ref, buf_p, buf_z, rel_ref, one_ref, com_ref, nb_p, nb_y, nb_z, load_s, feed_s, send_x, send_z, send_d, send_e, recv_x, recv_z, recv_d, recv_e, id_s, id_r, sp_s, sp_r, sz_s, sz_r, rs_s, rs_r, np_s, np_r, ny_s, ny_r, nz_s, nz_r, ag_s, ag_r, d_s, d_r, pre_s):
    p, z, y = lax.axis_index("pp"), lax.axis_index("tp"), lax.axis_index("dp")
    n_x = n_pp // 2
    x, c, par = p // 2, lax.rem(p, 2), lax.rem(z, 2)
    mate = 2 * x + 1 - c
    vocab = table_ref.shape[0]
    rows, tok = exp_ref.shape[1:]
    dq = g_ref.shape[3]
    up_y, down_y = lax.rem(y + 1, n_dp), lax.rem(y + n_dp - 1, n_dp)

    def first_row(d):
        return (d * n_pp + p) * rows

    short = vocab - (n_dp * n_pp - 1) * rows

    def table_copies(count, blocks):
        return [pltpu.make_async_copy(table_ref.at[pl.ds(pl.multiple_of(first_row(d), 8), count), pl.ds(q * dq, dq)], part_ref.at[d, q, pl.ds(0, count)], load_s.at[1 + 4 * d + q]) for d in blocks for q in range(4)]

    def each_table_copy(act):
        for cp in table_copies(rows, range(n_dp - 1)):
            act(cp)
        for cond, count in ((p < n_pp - 1, rows), (p == n_pp - 1, short)):
            @pl.when(cond)
            def _(count=count):
                for cp in table_copies(count, (n_dp - 1,)):
                    act(cp)

    each_table_copy(lambda cp: cp.start())
    hid_buf, dx_buf = pre_ref.at[pl.ds(0, tok)], pre_ref.at[pl.ds(tok, tok)]
    sources = ((n_pp - 1, hid_buf, hid_ref, lab_ref), (0, dx_buf, dx_ref, look_ref))
    for source, _, low, _ in sources:
        @pl.when(p == source)
        def _(low=low):
            pltpu.make_async_copy(acts_ref, low, load_s.at[0]).start()

    enter([("pp", lax.rem(p + o, n_pp)) for o in range(1, n_pp)] + [("tp", lax.rem(z + o, n_tp)) for o in range(1, n_tp)] + [("dp", lax.rem(y + o, n_dp)) for o in range(1, n_dp)])

    step_x = 1 - 2 * c
    next_p = 2 * lax.rem(x + step_x + n_x, n_x) + c
    next_z = lax.rem(z + step_x + n_tp, n_tp)
    size = tok // (4 * n_chunk)
    last = n_chunk + lag
    n_group = 3
    per_group = n_chunk // n_group
    group = tok // n_group

    def span(core, parity, k):
        return pl.ds(pl.multiple_of((4 * k + 2 * parity + core) * size, 8), size)

    class Stream:
        def __init__(self, a):
            self.a = a
            self.source, self.buf, self.low, self.ids = sources[a]
            self.is_src = p == self.source
            s_x = self.source // 2
            self.dist = lax.rem(jnp.where(c == 0, x - s_x, s_x - x) + n_x, n_x)

        def hop(self, part, send, recv, where):
            return remote(self.buf.at[part], self.buf.at[part], send, recv, where)

        def feed(self, k):
            return self.hop(span(1 - c, par, k), feed_s.at[self.a, k], recv_x.at[self.a, k], {"pp": mate})

        def ring(self, k):
            return self.hop(span(c, par, k), send_x.at[self.a, k], recv_x.at[self.a, k], {"pp": next_p})

        def plane(self, k, parity):
            return self.hop(span(c, parity, k), send_z.at[self.a, k], recv_z.at[self.a, k], {"tp": next_z})

        def across(self, k, core):
            return self.hop(span(core, par, k), send_d.at[self.a, k], recv_d.at[self.a, k], {"pp": mate})

        def again(self, k, core):
            return self.hop(span(core, 1 - par, k), send_e.at[self.a, k], recv_e.at[self.a, k], {"pp": mate})

        def id_copy(self, o):
            return remote(ids_ref, self.ids, id_s.at[self.a, o - 1], id_r.at[self.a], {"pp": lax.rem(p + o, n_pp)})

        def begin(self, with_ring):
            @pl.when(self.is_src)
            def _():
                pltpu.make_async_copy(acts_ref, self.low, load_s.at[0]).wait()
                self.ids[...] = ids_ref[...]

                @pl.loop(0, n_chunk)
                def _(k):
                    def widen(part):
                        self.buf[part, :] = self.low[part, :].astype(F32)

                    widen(span(1 - c, par, k))
                    self.feed(k).start()
                    widen(span(c, par, k))
                    if n_x > 1 and with_ring:
                        self.ring(k).start()
                    self.across(k, c).start()
                    widen(span(c, 1 - par, k))
                    self.again(k, c).start()

                for o in range(1, n_pp):
                    self.id_copy(o).start()

        def early_ring(self):
            @pl.when(mate == self.source)
            def _():
                @pl.loop(0, n_chunk)
                def _(k):
                    self.ring(k).wait_recv()
                    if n_x > 1:
                        self.ring(k).start()

        def late_sends(self):
            if n_x > 1:
                @pl.when(self.is_src)
                def _():
                    @pl.loop(0, n_chunk)
                    def _(k):
                        self.ring(k).start()

            @pl.when(mate == self.source)
            def _():
                @pl.loop(0, n_chunk)
                def _(k):
                    self.plane(k, par).start()

        def steps(self, lo, hi, early=False):
            @pl.when(jnp.logical_not(self.is_src))
            def _():
                @pl.loop(lo, hi)
                def _(k):
                    @pl.when(jnp.logical_and(k < n_chunk, jnp.logical_or(mate != self.source, not early)))
                    def _():
                        self.ring(k).wait_recv()
                        if n_x > 1:
                            @pl.when(self.dist < n_x - 1)
                            def _():
                                self.ring(k).start()

                        self.plane(k, par).start()

                        @pl.when(mate != self.source)
                        def _():
                            self.across(k, c).start()

                    @pl.when(k >= lag)
                    def _():
                        self.plane(k - lag, 1 - par).wait_recv()

                        @pl.when(mate != self.source)
                        def _():
                            self.again(k - lag, c).start()

        def collect(self, g):
            @pl.when(jnp.logical_not(self.is_src))
            def _():
                if g == 0:
                    self.id_copy(1).wait_recv()

                @pl.loop(g * per_group, (g + 1) * per_group)
                def _(k):
                    self.across(k, 1 - c).wait_recv()
                    self.again(k, 1 - c).wait_recv()

                tile = min(128, group)

                @pl.loop(0, group // tile)
                def _(k):
                    here = pl.ds(pl.multiple_of(g * group + k * tile, tile), tile)
                    self.low[here, :] = self.buf[here, :].astype(BF16)

        def settle(self):
            @pl.when(self.is_src)
            def _():
                for o in range(1, n_pp):
                    self.id_copy(o).wait_send()

            @pl.loop(0, n_chunk)
            def _(k):
                @pl.when(self.is_src)
                def _():
                    self.feed(k).wait_send()

                @pl.when(jnp.logical_not(self.is_src))
                def _():
                    self.plane(k, par).wait_send()

                if n_x > 1:
                    @pl.when(self.dist < n_x - 1)
                    def _():
                        self.ring(k).wait_send()

                @pl.when(mate != self.source)
                def _():
                    self.across(k, c).wait_send()
                    self.again(k, c).wait_send()

    hid_in, dx_in = Stream(0), Stream(1)
    wide = min(256, group)

    def logits(g):
        @pl.loop(0, group // wide)
        def _(j):
            cols = pl.ds(pl.multiple_of(g * group + j * wide, wide), wide)
            h = hid_ref[cols, :]
            top = jnp.full((1, wide), LOW, F32)
            for d in range(n_dp):
                lg = lax.dot_general(tab_ref[d], h, (((1,), (1,)), ((), ())), preferred_element_type=F32)
                if d == n_dp - 1 and short < rows:
                    ok = first_row(d) + lax.broadcasted_iota(jnp.int32, (rows, wide), 0) < vocab
                    lg = jnp.where(ok, lg, LOW)
                exp_ref[d, :, cols] = lg
                top = jnp.maximum(top, jnp.max(lg, axis=0, keepdims=True))
            tot = jnp.zeros((1, wide), F32)
            for d in range(n_dp):
                e = jnp.exp(exp_ref[d, :, cols] - top)
                exp_ref[d, :, cols] = e
                tot = tot + jnp.sum(e, axis=0, keepdims=True)
            stat_ref[0:1, cols] = top
            stat_ref[1:2, cols] = tot

    with scope("begin"):
        hid_in.begin(True)
        dx_in.begin(False)
        each_table_copy(lambda cp: cp.wait())
        for d in range(n_dp):
            for q in range(4):
                tab_ref[d, :, q * dq:(q + 1) * dq] = part_ref[d, q].astype(BF16)
    with scope("early"):
        dx_in.early_ring()
    lo = 0
    for g, hi in enumerate((per_group + lag + 2, 2 * per_group + lag + 2, last)):
        hi = min(hi, last)
        with scope(f"hid{g}"):
            if lo < n_chunk <= hi:
                hid_in.steps(lo, n_chunk)
                dx_in.late_sends()
                hid_in.steps(n_chunk, hi)
            else:
                hid_in.steps(lo, hi)
        lo = hi
        with scope(f"hid_collect{g}"):
            hid_in.collect(g)
        with scope(f"logits{g}"):
            logits(g)

    def swap(src, buf, send, recv, axis, me, n):
        return [remote(src, buf.at[o - 1], send.at[o - 1], recv.at[o - 1], {axis: lax.rem(me + o, n)}) for o in range(1, n)]

    def merge(src, buf, n):
        top = src[0:1, :]
        for o in range(1, n):
            top = jnp.maximum(top, buf[o - 1, 0:1, :])
        tot = src[1:2, :] * jnp.exp(src[0:1, :] - top)
        for o in range(1, n):
            tot = tot + buf[o - 1, 1:2, :] * jnp.exp(buf[o - 1, 0:1, :] - top)
        return top, tot

    def local_ids(ref, start, count):
        ids = ref[:, start:start + count] - z * vocab
        return jnp.where(ids < vocab, ids, -1)

    def row_ids(d, count):
        return first_row(d) + lax.broadcasted_iota(jnp.int32, (rows, count), 0)

    took = jnp.where(c == 0, 17 - 4 * dx_in.dist, 27 - 4 * dx_in.dist)
    took = jnp.where(p == n_pp - 1, last, jnp.where(p == 1, 0, took))
    at_one, at_two = jnp.clip(took, 0, last), jnp.clip(jnp.where(p == 1, 0, took + 5), 0, last)
    at_three = jnp.clip(took + 10, per_group + lag, last)
    at_four = min(last, max(n_chunk, 2 * per_group + lag))

    stage = swap(stat_ref, buf_p, sp_s, sp_r, "pp", p, n_pp)
    for cp in stage:
        cp.start()
    with scope("dx1"):
        dx_in.steps(0, at_one, True)
    with scope("stat1"):
        for cp in stage:
            cp.wait()
    top, tot = merge(stat_ref, buf_p, n_pp)
    mid_ref[0:1, :] = top
    mid_ref[1:2, :] = tot
    stage = swap(mid_ref, buf_z, sz_s, sz_r, "tp", z, n_tp)
    for cp in stage:
        cp.start()
    with scope("dx2"):
        dx_in.steps(at_one, at_two, True)
    with scope("stat2"):
        for cp in stage:
            cp.wait()
    top, tot = merge(mid_ref, buf_z, n_tp)
    mid_ref[0:1, :] = jnp.exp(stat_ref[0:1, :] - top) / (tot * tok)

    def head(d):
        prob = exp_ref[d] * mid_ref[0:1, :]
        hit = local_ids(lab_ref, 0, tok) == row_ids(d, tok)
        dl_ref[...] = jnp.where(hit, prob - 1.0 / tok, prob).astype(BF16)
        for q in range(4):
            part_ref[d, q] = jnp.dot(dl_ref[...], hid_ref[:, q * dq:(q + 1) * dq], preferred_element_type=F32)

    def lookup(g):
        def add(d):
            hot = (local_ids(look_ref, g * group, group) == row_ids(d, group)).astype(BF16)
            dl_ref[:, 0:group] = hot
            for q in range(4):
                part_ref[d, q] += jnp.dot(dl_ref[:, 0:group], dx_ref[g * group:(g + 1) * group, q * dq:(q + 1) * dq], preferred_element_type=F32)
        return add

    with scope("dx3"):
        dx_in.steps(at_two, at_three, True)
    with scope("head"):
        pl.loop(0, n_dp)(head)
    with scope("dx_group0"):
        dx_in.collect(0)
        pl.loop(0, n_dp)(lookup(0))
    with scope("dx4"):
        dx_in.steps(at_three, at_four, True)
    with scope("dx_group1"):
        dx_in.collect(1)
        pl.loop(0, n_dp)(lookup(1))
    with scope("dx5"):
        dx_in.steps(jnp.maximum(at_three, at_four), last, True)
    with scope("dx_group2"):
        dx_in.collect(2)

    lo, hi = pl.ds(0, 2), pl.ds(2, 2)
    far = lax.rem(y + 2, n_dp)
    rel_a = remote(part_ref.at[far, lo], rel_ref.at[0], rs_s.at[0], rs_r.at[0], {"dp": up_y})
    rel_b = remote(part_ref.at[far, hi], rel_ref.at[1], rs_s.at[1], rs_r.at[1], {"dp": down_y})
    one_b = remote(part_ref.at[up_y, hi], one_ref.at[1], rs_s.at[2], rs_r.at[2], {"dp": up_y})
    one_a = remote(part_ref.at[down_y, lo], one_ref.at[0], rs_s.at[3], rs_r.at[3], {"dp": down_y})
    com_a = remote(part_ref.at[up_y, lo], com_ref.at[0], rs_s.at[4], rs_r.at[4], {"dp": up_y})
    com_b = remote(part_ref.at[down_y, hi], com_ref.at[1], rs_s.at[5], rs_r.at[5], {"dp": down_y})
    add = lookup(n_group - 1)
    add(far)
    rel_a.start()
    rel_b.start()
    add(up_y)
    one_b.start()
    add(down_y)
    one_a.start()
    add(y)
    hid_in.settle()
    dx_in.settle()
    n_pre = pre_ref.shape[0] // (3 * rows)
    loads = [pltpu.make_async_copy(ref.at[pl.ds(i * rows, rows)], pre_ref.at[pl.ds((3 * i + a) * rows, rows)], pre_s.at[3 * i + a]) for i in range(n_pre) for a, ref in enumerate((table_ref, avg_ref, sq_ref))]
    for cp in loads:
        cp.start()
    with scope("relay"):
        rel_a.wait_recv()
    part_ref[up_y, lo] += rel_ref[0]
    com_a.start()
    rel_b.wait_recv()
    part_ref[down_y, hi] += rel_ref[1]
    com_b.start()
    own = y * n_pp + p
    square = jnp.zeros((8, 128), F32)
    with scope("one"):
        one_a.wait_recv()
        one_b.wait_recv()
    for half, cp in ((0, com_a), (1, com_b)):
        with scope("com"):
            cp.wait_recv()
        for q in range(2):
            total = (part_ref[y, 2 * half + q] + com_ref[half, q] + one_ref[half, q]) * (1.0 / n_dp)
            g_ref[own, 2 * half + q] = total
            lanes = jnp.sum((total * total).reshape(rows // 8, 8, dq), axis=0)
            for i in range(0, dq, 128):
                square = square + lanes[:, i:i + 128]

    def block(xx, yy):
        return lax.rem(yy + 2 * n_dp, n_dp) * n_pp + 2 * lax.rem(xx + 2 * n_x, n_x) + c

    colours = []
    for q, (axes, sign) in enumerate((("xy", 1), ("xy", -1), ("yx", 1), ("yx", -1))):
        sizes = (n_x, n_dp) if axes == "xy" else (n_dp, n_x)
        to_x = {"pp": 2 * lax.rem(x + sign + n_x, n_x) + c}
        to_y = {"dp": lax.rem(y + sign + n_dp, n_dp)}
        dest = (to_x, to_y) if axes == "xy" else (to_y, to_x)
        colours.append((q, axes, sign, sizes, dest, ring_plan(*sizes)))

    def holder(axes, sign, s, t):
        return block(x - sign * s, y - sign * t) if axes == "xy" else block(x - sign * t, y - sign * s)

    def message(colour, item, coming):
        q, axes, sign, _, dest, plan = colour
        phase, s, t = item
        at = plan.index(item)
        s_at, t_at = (s + coming, t) if phase == 1 else (s, t + coming)
        b = holder(axes, sign, s_at, t_at)
        return remote(g_ref.at[b, q], g_ref.at[b, q], ag_s.at[q, at], ag_r.at[q, at], dest[phase - 1])

    def mate_copy(q, slot, b):
        return remote(g_ref.at[b, q], g_ref.at[b, q], d_s.at[q, slot], d_r.at[q, slot], {"pp": mate})

    sends = []

    def push(cp):
        cp.start()
        sends.append(cp)

    for colour in colours:
        if colour[3][0] > 1:
            push(message(colour, (1, 0, 0), 0))
    for colour in colours:
        if colour[3][1] > 1:
            push(message(colour, (2, 0, 0), 0))

    def norm_swap(value, buf, send, recv, axis, me, n):
        buf[me] = value
        return [remote(buf.at[me], buf.at[me], send.at[o - 1], recv.at[o - 1], {axis: lax.rem(me + o, n)}) for o in range(1, n)], [
            remote(buf.at[lax.rem(me + n - o, n)], buf.at[lax.rem(me + n - o, n)], send.at[o - 1], recv.at[o - 1], {axis: lax.rem(me + o, n)}) for o in range(1, n)]

    norm_out, norm_in = norm_swap(square, nb_p, np_s, np_r, "pp", p, n_pp)
    for cp in norm_out:
        push(cp)
    for q in range(4):
        push(mate_copy(q, 0, own))

    steps = n_x * n_dp - 1
    for i in range(steps):
        for colour in colours:
            q, axes, sign, sizes, dest, plan = colour
            phase, s, t = plan[i]
            message(colour, plan[i], 1).wait_recv()
            if phase == 1:
                if s + 1 < sizes[0] - 1:
                    push(message(colour, (1, s + 1, 0), 0))
                if sizes[1] > 1:
                    push(message(colour, (2, s + 1, 0), 0))
                push(mate_copy(q, i + 1, holder(axes, sign, s + 1, 0)))
            else:
                if t + 1 < sizes[1] - 1:
                    push(message(colour, (2, s, t + 1), 0))
                push(mate_copy(q, i + 1, holder(axes, sign, s, t + 1)))
        if i == 0:
            for cp in norm_in:
                cp.wait_recv()
            total = nb_p[0]
            for o in range(1, n_pp):
                total = total + nb_p[o]
            norm_out, norm_in = norm_swap(total, nb_y, ny_s, ny_r, "dp", y, n_dp)
            for cp in norm_out:
                push(cp)
        if i == 1:
            for cp in norm_in:
                cp.wait_recv()
            total = nb_y[0]
            for o in range(1, n_dp):
                total = total + nb_y[o]
            norm_out, norm_in = norm_swap(total, nb_z, nz_s, nz_r, "tp", z, n_tp)
            for cp in norm_out:
                push(cp)
        if i == 2:
            for cp in norm_in:
                cp.wait_recv()
            total = nb_z[0]
            for o in range(1, n_tp):
                total = total + nb_z[o]
            norm = jnp.sqrt(jnp.sum(total, axis=(0, 1), keepdims=True))
            scale_ref[...] = jnp.broadcast_to(CLIP_NORM / jnp.maximum(norm, CLIP_NORM), (8, 128))

    for q, axes, sign, sizes, dest, plan in colours:
        for i in range(steps + 1):
            if i == 0:
                b = own
            else:
                phase, s, t = plan[i - 1]
                b = holder(axes, sign, s + 1, 0) if phase == 1 else holder(axes, sign, s, t + 1)
            mate_copy(q, i, b + 1 - 2 * c).wait_recv()
    for cp in (rel_a, rel_b, one_a, one_b, com_a, com_b, *sends):
        cp.wait_send()
    for cp in loads:
        cp.wait()


def plane_gradient(master, acts, ids, exp_avg, exp_avg_sq, n_tp, n_dp, n_pp):
    vocab, dim = master.shape
    tok = acts.shape[0]
    rows = -(-vocab // (n_pp * n_dp))
    rows = -(-rows // 8) * 8
    dq = dim // 4
    n_chunk = 24 if tok % (4 * 24 * 8) == 0 else 6
    lag = 4
    steps = (n_pp // 2) * n_dp
    n_pre = max(PRE_BLOCKS, -(-2 * tok // (3 * rows)))
    full = pl.BlockSpec(memory_space=VMEM)
    any_space = pl.BlockSpec(memory_space=pl.ANY)
    half = VMEM((2, 2, rows, dq), F32)
    chunk = DMA((2, n_chunk))
    return pl.pallas_call(
        functools.partial(grad_kernel, n_tp, n_dp, n_pp, n_chunk, lag),
        out_shape=(VMEM((n_dp * n_pp, 4, rows, dq), F32), jax.ShapeDtypeStruct((8, 128), F32), VMEM((3 * n_pre * rows, dim), F32)),
        in_specs=[any_space, any_space, full, any_space, any_space],
        out_specs=(full, full, full),
        scratch_shapes=[
            VMEM((tok, dim), BF16), VMEM((tok, dim), BF16),
            VMEM((1, tok), jnp.int32), VMEM((1, tok), jnp.int32), VMEM((n_dp, rows, dim), BF16),
            VMEM((n_dp, rows, tok), F32), VMEM((rows, tok), BF16), VMEM((n_dp, 4, rows, dq), F32),
            VMEM((2, tok), F32), VMEM((2, tok), F32), VMEM((n_pp - 1, 2, tok), F32), VMEM((n_tp - 1, 2, tok), F32),
            half, half, half,
            VMEM((n_pp, 8, 128), F32), VMEM((n_dp, 8, 128), F32), VMEM((n_tp, 8, 128), F32),
            DMA((1 + 4 * n_dp,)), *[chunk] * 9, DMA((2, n_pp - 1)), DMA((2,)),
            DMA((n_pp - 1,)), DMA((n_pp - 1,)), DMA((n_tp - 1,)), DMA((n_tp - 1,)), DMA((6,)), DMA((6,)),
            DMA((n_pp - 1,)), DMA((n_pp - 1,)), DMA((n_dp - 1,)), DMA((n_dp - 1,)), DMA((n_tp - 1,)), DMA((n_tp - 1,)),
            DMA((4, steps)), DMA((4, steps)), DMA((4, steps)), DMA((4, steps)), DMA((3 * n_pre,)),
        ],
        compiler_params=pltpu.CompilerParams(collective_id=0, has_side_effects=True, vmem_limit_bytes=21 << 20),
        name="plane_gradient",
    )(master, acts, ids, exp_avg, exp_avg_sq)


def adamw_kernel(n_slot, ahead, scale_ref, g_ref, pre_ref, e_hbm, m_hbm, v_hbm, ne_hbm, nm_hbm, nv_hbm, nb_hbm, e_buf, m_buf, v_buf, b_buf, in_s, out_s):
    n_blk, _, rows, dq = g_ref.shape
    vocab = e_hbm.shape[0]
    last = vocab - (n_blk - 1) * rows
    scale = scale_ref[0:1, 0:1]

    def loads(i, count):
        slot = lax.rem(i, n_slot)
        here = pl.ds(pl.multiple_of(i * rows, 8), count)
        return [pltpu.make_async_copy(hbm.at[here], buf.at[slot, pl.ds(0, count)], in_s.at[a, slot]) for a, (hbm, buf) in enumerate(((e_hbm, e_buf), (m_hbm, m_buf), (v_hbm, v_buf)))]

    def stores(i, count):
        slot = lax.rem(i, n_slot)
        here = pl.ds(pl.multiple_of(i * rows, 8), count)
        return [pltpu.make_async_copy(buf.at[slot, pl.ds(0, count)], hbm.at[here], out_s.at[a, slot]) for a, (buf, hbm) in enumerate(((e_buf, ne_hbm), (m_buf, nm_hbm), (v_buf, nv_hbm), (b_buf, nb_hbm)))]

    def each(copies, i, act):
        if last == rows:
            for cp in copies(i, rows):
                act(cp)
            return
        for cond, count in ((i < n_blk - 1, rows), (i == n_blk - 1, last)):
            @pl.when(cond)
            def _(count=count):
                for cp in copies(i, count):
                    act(cp)

    n_pre = pre_ref.shape[0] // (3 * rows)

    for i in range(n_pre, min(ahead, n_blk)):
        each(loads, i, lambda cp: cp.start())

    @pl.loop(0, n_blk)
    def _(i):
        slot = lax.rem(i, n_slot)

        @pl.when(i + ahead < n_blk)
        def _():
            @pl.when(i + ahead >= n_slot)
            def _():
                each(stores, i + ahead - n_slot, lambda cp: cp.wait())

            @pl.when(i + ahead >= n_pre)
            def _():
                each(loads, i + ahead, lambda cp: cp.start())

        def update(read):
            @pl.loop(0, rows // 8, unroll=5 if rows % 40 == 0 else 1)
            def _(r):
                at = pl.ds(pl.multiple_of(r * 8, 8), 8)
                for q in range(4):
                    cols = pl.ds(q * dq, dq)
                    g = g_ref[i, q, at, :] * scale
                    e, m, v = read(r, at, cols)
                    m = BETA_ONE * m + (1.0 - BETA_ONE) * g
                    v = BETA_TWO * v + (1.0 - BETA_TWO) * g * g
                    step = (m * (1.0 / (1.0 - BETA_ONE ** OPT_STEP))) / (jnp.sqrt(v * (1.0 / (1.0 - BETA_TWO ** OPT_STEP))) + ADAM_EPS)
                    ne = e - LEARN_RATE * (step + WEIGHT_DECAY * e)
                    e_buf[slot, at, cols] = ne
                    m_buf[slot, at, cols] = m
                    v_buf[slot, at, cols] = v
                    b_buf[slot, at, cols] = ne.astype(BF16)

        @pl.when(i < n_pre)
        def _():
            def read(r, at, cols):
                return [pre_ref[pl.ds(pl.multiple_of((3 * i + a) * rows + r * 8, 8), 8), cols] for a in range(3)]

            update(read)

        @pl.when(i >= n_pre)
        def _():
            each(loads, i, lambda cp: cp.wait())
            update(lambda r, at, cols: [buf[slot, at, cols] for buf in (e_buf, m_buf, v_buf)])

        each(stores, i, lambda cp: cp.start())

    for i in range(max(0, n_blk - n_slot), n_blk):
        each(stores, i, lambda cp: cp.wait())


def adamw(scale, grad, pre, master, exp_avg, exp_avg_sq):
    vocab, dim = master.shape
    rows = grad.shape[2]
    n_slot = 6
    full = pl.BlockSpec(memory_space=VMEM)
    any_space = pl.BlockSpec(memory_space=pl.ANY)
    f32 = jax.ShapeDtypeStruct((vocab, dim), F32)
    count = vocab * dim
    ring = VMEM((n_slot, rows, dim), F32)
    return pl.pallas_call(
        functools.partial(adamw_kernel, n_slot, 3),
        out_shape=(f32, f32, f32, jax.ShapeDtypeStruct((vocab, dim), BF16)),
        in_specs=[full, full, full, any_space, any_space, any_space],
        out_specs=(any_space,) * 4,
        scratch_shapes=[ring, ring, ring, VMEM((n_slot, rows, dim), BF16), DMA((3, n_slot)), DMA((4, n_slot))],
        cost_estimate=pl.CostEstimate(flops=20 * count, bytes_accessed=30 * count, transcendentals=2 * count),
        compiler_params=pltpu.CompilerParams(vmem_limit_bytes=21 << 20),
        name="adamw",
    )(scale, in_vmem(grad), in_vmem(pre), master, exp_avg, exp_avg_sq)


def solution(mesh):
    n_pp, n_dp, n_tp = mesh.shape["pp"], mesh.shape["dp"], mesh.shape["tp"]
    table_spec = P("tp", None)

    def device_step(master, exp_avg, exp_avg_sq, stage_ids, stage_acts):
        vocab, dim = master.shape
        tok = stage_ids.shape[1] * stage_ids.shape[2]
        acts = stage_acts.reshape(tok, dim)
        grad, scale, pre = plane_gradient(master, acts, stage_ids.reshape(1, tok), exp_avg, exp_avg_sq, n_tp, n_dp, n_pp)
        return adamw(scale, grad, pre, master, exp_avg, exp_avg_sq)

    return jax.shard_map(device_step, mesh=mesh, in_specs=(table_spec, table_spec, table_spec, P("pp", "dp", None), P("pp", "dp", None, None)), out_specs=(table_spec, table_spec, table_spec, table_spec), check_vma=False)
```

```python
import functools

import jax
import jax.numpy as jnp
from jax import lax
from jax.experimental import pallas as pl
from jax.experimental.pallas import tpu as pltpu
from jax.sharding import PartitionSpec as P

LEARN_RATE = 0.003
BETA_ONE = 0.9
BETA_TWO = 0.95
ADAM_EPS = 1e-8
WEIGHT_DECAY = 0.1
CLIP_NORM = 1.0
OPT_STEP = 10

MESH_ID = pl.DeviceIdType.MESH
LOW = -1e30
VMEM = pltpu.VMEM
DMA = pltpu.SemaphoreType.DMA
F32, BF16 = jnp.float32, jnp.bfloat16
PRE_BLOCKS = 6
scope = jax.named_scope


def remote(src, dst, send, recv, where):
    return pltpu.make_async_remote_copy(src_ref=src, dst_ref=dst, send_sem=send, recv_sem=recv, device_id=where, device_id_type=MESH_ID)


def in_vmem(arr):
    return pltpu.with_memory_space_constraint(arr, VMEM)


def enter(groups):
    barrier = pltpu.get_barrier_semaphore()
    for axis, peer in groups:
        pl.semaphore_signal(barrier, inc=1, device_id={axis: peer}, device_id_type=MESH_ID)
    pl.semaphore_wait(barrier, len(groups))


def ring_plan(n_one, n_two):
    items = [(1, s, 0) for s in range(n_one - 1)] + [(2, s, t) for s in range(n_one) for t in range(n_two - 1)]
    return sorted(items, key=lambda i: (i[1] + i[2], i[0], i[2]))


def grad_kernel(n_tp, n_dp, n_pp, n_chunk, lag, table_ref, acts_ref, ids_ref, avg_ref, sq_ref, g_ref, scale_ref, pre_ref, hid_ref, dx_ref, lab_ref, look_ref, tab_ref, exp_ref, dl_ref, part_ref, stat_ref, mid_ref, buf_p, buf_z, rel_ref, one_ref, com_ref, nb_p, nb_y, nb_z, load_s, feed_s, send_x, send_z, send_d, send_e, recv_x, recv_z, recv_d, recv_e, id_s, id_r, sp_s, sp_r, sz_s, sz_r, rs_s, rs_r, np_s, np_r, ny_s, ny_r, nz_s, nz_r, ag_s, ag_r, d_s, d_r, pre_s):
    p, z, y = lax.axis_index("pp"), lax.axis_index("tp"), lax.axis_index("dp")
    n_x = n_pp // 2
    x, c, par = p // 2, lax.rem(p, 2), lax.rem(z, 2)
    mate = 2 * x + 1 - c
    vocab = table_ref.shape[0]
    rows, tok = exp_ref.shape[1:]
    dq = g_ref.shape[3]
    up_y, down_y = lax.rem(y + 1, n_dp), lax.rem(y + n_dp - 1, n_dp)

    def first_row(d):
        return (d * n_pp + p) * rows

    short = vocab - (n_dp * n_pp - 1) * rows

    def table_copies(count, blocks):
        return [pltpu.make_async_copy(table_ref.at[pl.ds(pl.multiple_of(first_row(d), 8), count), pl.ds(q * dq, dq)], part_ref.at[d, q, pl.ds(0, count)], load_s.at[1 + 4 * d + q]) for d in blocks for q in range(4)]

    def each_table_copy(act):
        for cp in table_copies(rows, range(n_dp - 1)):
            act(cp)
        for cond, count in ((p < n_pp - 1, rows), (p == n_pp - 1, short)):
            @pl.when(cond)
            def _(count=count):
                for cp in table_copies(count, (n_dp - 1,)):
                    act(cp)

    each_table_copy(lambda cp: cp.start())
    hid_buf, dx_buf = pre_ref.at[pl.ds(0, tok)], pre_ref.at[pl.ds(tok, tok)]
    sources = ((n_pp - 1, hid_buf, hid_ref, lab_ref), (0, dx_buf, dx_ref, look_ref))
    for source, _, low, _ in sources:
        @pl.when(p == source)
        def _(low=low):
            pltpu.make_async_copy(acts_ref, low, load_s.at[0]).start()

    enter([("pp", lax.rem(p + o, n_pp)) for o in range(1, n_pp)] + [("tp", lax.rem(z + o, n_tp)) for o in range(1, n_tp)] + [("dp", lax.rem(y + o, n_dp)) for o in range(1, n_dp)])

    step_x = 1 - 2 * c
    next_p = 2 * lax.rem(x + step_x + n_x, n_x) + c
    next_z = lax.rem(z + step_x + n_tp, n_tp)
    size = tok // (4 * n_chunk)
    last = n_chunk + lag
    n_group = 3
    per_group = n_chunk // n_group
    group = tok // n_group

    def span(core, parity, k):
        return pl.ds(pl.multiple_of((4 * k + 2 * parity + core) * size, 8), size)

    class Stream:
        def __init__(self, a):
            self.a = a
            self.source, self.buf, self.low, self.ids = sources[a]
            self.is_src = p == self.source
            s_x = self.source // 2
            self.dist = lax.rem(jnp.where(c == 0, x - s_x, s_x - x) + n_x, n_x)

        def hop(self, part, send, recv, where):
            return remote(self.buf.at[part], self.buf.at[part], send, recv, where)

        def feed(self, k):
            return self.hop(span(1 - c, par, k), feed_s.at[self.a, k], recv_x.at[self.a, k], {"pp": mate})

        def ring(self, k):
            return self.hop(span(c, par, k), send_x.at[self.a, k], recv_x.at[self.a, k], {"pp": next_p})

        def plane(self, k, parity):
            return self.hop(span(c, parity, k), send_z.at[self.a, k], recv_z.at[self.a, k], {"tp": next_z})

        def across(self, k, core):
            return self.hop(span(core, par, k), send_d.at[self.a, k], recv_d.at[self.a, k], {"pp": mate})

        def again(self, k, core):
            return self.hop(span(core, 1 - par, k), send_e.at[self.a, k], recv_e.at[self.a, k], {"pp": mate})

        def id_copy(self, o):
            return remote(ids_ref, self.ids, id_s.at[self.a, o - 1], id_r.at[self.a], {"pp": lax.rem(p + o, n_pp)})

        def begin(self, with_ring):
            @pl.when(self.is_src)
            def _():
                pltpu.make_async_copy(acts_ref, self.low, load_s.at[0]).wait()
                self.ids[...] = ids_ref[...]

                @pl.loop(0, n_chunk)
                def _(k):
                    def widen(part):
                        self.buf[part, :] = self.low[part, :].astype(F32)

                    widen(span(1 - c, par, k))
                    self.feed(k).start()
                    widen(span(c, par, k))
                    if n_x > 1 and with_ring:
                        self.ring(k).start()
                    self.across(k, c).start()
                    widen(span(c, 1 - par, k))
                    self.again(k, c).start()

                for o in range(1, n_pp):
                    self.id_copy(o).start()

        def early_ring(self):
            @pl.when(mate == self.source)
            def _():
                @pl.loop(0, n_chunk)
                def _(k):
                    self.ring(k).wait_recv()
                    if n_x > 1:
                        self.ring(k).start()

        def late_ring(self, lo, hi):
            if n_x > 1:
                @pl.when(self.is_src)
                def _():
                    @pl.loop(lo, hi)
                    def _(k):
                        self.ring(k).start()

        def late_plane(self):
            @pl.when(mate == self.source)
            def _():
                @pl.loop(0, n_chunk)
                def _(k):
                    self.plane(k, par).start()

        def steps(self, lo, hi, early=False):
            @pl.when(jnp.logical_not(self.is_src))
            def _():
                @pl.loop(lo, hi)
                def _(k):
                    @pl.when(jnp.logical_and(k < n_chunk, jnp.logical_or(mate != self.source, not early)))
                    def _():
                        self.ring(k).wait_recv()
                        if n_x > 1:
                            @pl.when(self.dist < n_x - 1)
                            def _():
                                if early:
                                    @pl.when(jnp.logical_and(p == n_pp - 1, k >= 2))
                                    def _():
                                        self.ring(k - 2).wait_send()

                                self.ring(k).start()

                        self.plane(k, par).start()

                        @pl.when(mate != self.source)
                        def _():
                            self.across(k, c).start()

                    @pl.when(k >= lag)
                    def _():
                        self.plane(k - lag, 1 - par).wait_recv()

                        @pl.when(mate != self.source)
                        def _():
                            self.again(k - lag, c).start()

        def collect(self, g):
            @pl.when(jnp.logical_not(self.is_src))
            def _():
                if g == 0:
                    self.id_copy(1).wait_recv()

                @pl.loop(g * per_group, (g + 1) * per_group)
                def _(k):
                    self.across(k, 1 - c).wait_recv()
                    self.again(k, 1 - c).wait_recv()

                tile = min(128, group)

                @pl.loop(0, group // tile)
                def _(k):
                    here = pl.ds(pl.multiple_of(g * group + k * tile, tile), tile)
                    self.low[here, :] = self.buf[here, :].astype(BF16)

        def settle(self):
            @pl.when(self.is_src)
            def _():
                for o in range(1, n_pp):
                    self.id_copy(o).wait_send()

            @pl.loop(0, n_chunk)
            def _(k):
                @pl.when(self.is_src)
                def _():
                    self.feed(k).wait_send()

                @pl.when(jnp.logical_not(self.is_src))
                def _():
                    self.plane(k, par).wait_send()

                if n_x > 1:
                    begun = n_chunk if self.a == 0 else n_chunk - 2

                    @pl.when(jnp.logical_and(self.dist < n_x - 1, jnp.logical_or(p != n_pp - 1, k >= begun)))
                    def _():
                        self.ring(k).wait_send()

                @pl.when(mate != self.source)
                def _():
                    self.across(k, c).wait_send()
                    self.again(k, c).wait_send()

    hid_in, dx_in = Stream(0), Stream(1)
    wide = min(256, group)

    def logits(g):
        @pl.loop(0, group // wide)
        def _(j):
            cols = pl.ds(pl.multiple_of(g * group + j * wide, wide), wide)
            h = hid_ref[cols, :]
            top = jnp.full((1, wide), LOW, F32)
            for d in range(n_dp):
                lg = lax.dot_general(tab_ref[d], h, (((1,), (1,)), ((), ())), preferred_element_type=F32)
                if d == n_dp - 1 and short < rows:
                    ok = first_row(d) + lax.broadcasted_iota(jnp.int32, (rows, wide), 0) < vocab
                    lg = jnp.where(ok, lg, LOW)
                exp_ref[d, :, cols] = lg
                top = jnp.maximum(top, jnp.max(lg, axis=0, keepdims=True))
            tot = jnp.zeros((1, wide), F32)
            for d in range(n_dp):
                e = jnp.exp(exp_ref[d, :, cols] - top)
                exp_ref[d, :, cols] = e
                tot = tot + jnp.sum(e, axis=0, keepdims=True)
            stat_ref[0:1, cols] = top
            stat_ref[1:2, cols] = tot

    with scope("begin"):
        hid_in.begin(True)
        dx_in.begin(False)
        each_table_copy(lambda cp: cp.wait())
        for d in range(n_dp):
            for q in range(4):
                tab_ref[d, :, q * dq:(q + 1) * dq] = part_ref[d, q].astype(BF16)
    with scope("early"):
        dx_in.early_ring()
    dist = dx_in.dist

    def clip(value):
        return jnp.clip(jnp.where(p == 1, 0, value), 0, last)

    at_zero = clip(jnp.where(p == n_pp - 1, 0, jnp.where(c == 0, 4 - 2 * dist, 21 - 6 * dist)))
    at_one = jnp.where(c == 0, 11 - 3 * dist, 23 - 5 * dist)
    at_two = jnp.maximum(clip(jnp.where(p == n_pp - 1, last, at_one + 3)), at_zero)
    at_three = jnp.maximum(jnp.maximum(clip(at_one + 6), at_two), min(last, per_group + lag))
    at_one = jnp.maximum(clip(jnp.where(p == n_pp - 1, last, at_one)), at_zero)
    at_two = jnp.maximum(at_two, at_one)
    at_four = jnp.maximum(at_three, min(last, max(n_chunk, 2 * per_group + lag)))

    lo = 0
    for g, hi in enumerate((per_group + lag + 1, 2 * per_group + lag + 1, last)):
        hi = min(hi, last)
        with scope(f"hid{g}"):
            if lo < n_chunk <= hi:
                hid_in.steps(lo, n_chunk)
                dx_in.late_ring(0, 2)
                hid_in.steps(n_chunk, hi)
            else:
                hid_in.steps(lo, hi)
        lo = hi
        if g == n_group - 1:
            dx_in.late_ring(2, n_chunk)
            dx_in.late_plane()
            with scope("dx0"):
                dx_in.steps(0, at_zero, True)
        with scope(f"hid_collect{g}"):
            hid_in.collect(g)
        with scope(f"logits{g}"):
            logits(g)

    def swap(src, buf, send, recv, axis, me, n):
        return [remote(src, buf.at[o - 1], send.at[o - 1], recv.at[o - 1], {axis: lax.rem(me + o, n)}) for o in range(1, n)]

    def merge(src, buf, n):
        top = src[0:1, :]
        for o in range(1, n):
            top = jnp.maximum(top, buf[o - 1, 0:1, :])
        tot = src[1:2, :] * jnp.exp(src[0:1, :] - top)
        for o in range(1, n):
            tot = tot + buf[o - 1, 1:2, :] * jnp.exp(buf[o - 1, 0:1, :] - top)
        return top, tot

    def local_ids(ref, start, count):
        ids = ref[:, start:start + count] - z * vocab
        return jnp.where(ids < vocab, ids, -1)

    def row_ids(d, count):
        return first_row(d) + lax.broadcasted_iota(jnp.int32, (rows, count), 0)

    stage = swap(stat_ref, buf_p, sp_s, sp_r, "pp", p, n_pp)
    for cp in stage:
        cp.start()
    with scope("dx1"):
        if n_x > 1:
            @pl.when(p == n_pp - 1)
            def _():
                @pl.loop(0, n_chunk)
                def _(k):
                    hid_in.ring(k).wait_send()

        dx_in.steps(at_zero, at_one, True)
    with scope("stat1"):
        for cp in stage:
            cp.wait()
    top, tot = merge(stat_ref, buf_p, n_pp)
    mid_ref[0:1, :] = top
    mid_ref[1:2, :] = tot
    stage = swap(mid_ref, buf_z, sz_s, sz_r, "tp", z, n_tp)
    for cp in stage:
        cp.start()
    with scope("dx2"):
        dx_in.steps(at_one, at_two, True)
    with scope("stat2"):
        for cp in stage:
            cp.wait()
    top, tot = merge(mid_ref, buf_z, n_tp)
    mid_ref[0:1, :] = jnp.exp(stat_ref[0:1, :] - top) / (tot * tok)

    def head(d):
        prob = exp_ref[d] * mid_ref[0:1, :]
        hit = local_ids(lab_ref, 0, tok) == row_ids(d, tok)
        dl_ref[...] = jnp.where(hit, prob - 1.0 / tok, prob).astype(BF16)
        for q in range(4):
            part_ref[d, q] = jnp.dot(dl_ref[...], hid_ref[:, q * dq:(q + 1) * dq], preferred_element_type=F32)

    def lookup(g):
        def add(d):
            hot = (local_ids(look_ref, g * group, group) == row_ids(d, group)).astype(BF16)
            dl_ref[:, 0:group] = hot
            for q in range(4):
                part_ref[d, q] += jnp.dot(dl_ref[:, 0:group], dx_ref[g * group:(g + 1) * group, q * dq:(q + 1) * dq], preferred_element_type=F32)
        return add

    with scope("dx3"):
        dx_in.steps(at_two, at_three, True)
    with scope("head"):
        pl.loop(0, n_dp)(head)
    with scope("dx_group0"):
        dx_in.collect(0)
        pl.loop(0, n_dp)(lookup(0))
    with scope("dx4"):
        dx_in.steps(at_three, at_four, True)
    with scope("dx_group1"):
        dx_in.collect(1)
        pl.loop(0, n_dp)(lookup(1))
    with scope("dx5"):
        dx_in.steps(at_four, last, True)
    with scope("dx_group2"):
        dx_in.collect(2)

    lo, hi = pl.ds(0, 2), pl.ds(2, 2)
    far = lax.rem(y + 2, n_dp)
    rel_a = remote(part_ref.at[far, lo], rel_ref.at[0], rs_s.at[0], rs_r.at[0], {"dp": up_y})
    rel_b = remote(part_ref.at[far, hi], rel_ref.at[1], rs_s.at[1], rs_r.at[1], {"dp": down_y})
    one_b = remote(part_ref.at[up_y, hi], one_ref.at[1], rs_s.at[2], rs_r.at[2], {"dp": up_y})
    one_a = remote(part_ref.at[down_y, lo], one_ref.at[0], rs_s.at[3], rs_r.at[3], {"dp": down_y})
    com_a = remote(part_ref.at[up_y, lo], com_ref.at[0], rs_s.at[4], rs_r.at[4], {"dp": up_y})
    com_b = remote(part_ref.at[down_y, hi], com_ref.at[1], rs_s.at[5], rs_r.at[5], {"dp": down_y})
    add = lookup(n_group - 1)
    add(far)
    rel_a.start()
    rel_b.start()
    add(up_y)
    one_b.start()
    add(down_y)
    one_a.start()
    add(y)
    hid_in.settle()
    dx_in.settle()
    n_pre = pre_ref.shape[0] // (3 * rows)
    loads = [pltpu.make_async_copy(ref.at[pl.ds(i * rows, rows)], pre_ref.at[pl.ds((3 * i + a) * rows, rows)], pre_s.at[3 * i + a]) for i in range(n_pre) for a, ref in enumerate((table_ref, avg_ref, sq_ref))]
    for cp in loads:
        cp.start()
    with scope("relay"):
        rel_a.wait_recv()
    part_ref[up_y, lo] += rel_ref[0]
    com_a.start()
    rel_b.wait_recv()
    part_ref[down_y, hi] += rel_ref[1]
    com_b.start()
    own = y * n_pp + p
    square = jnp.zeros((8, 128), F32)
    with scope("one"):
        one_a.wait_recv()
        one_b.wait_recv()
    for half, cp in ((0, com_a), (1, com_b)):
        with scope("com"):
            cp.wait_recv()
        for q in range(2):
            total = (part_ref[y, 2 * half + q] + com_ref[half, q] + one_ref[half, q]) * (1.0 / n_dp)
            g_ref[own, 2 * half + q] = total
            lanes = jnp.sum((total * total).reshape(rows // 8, 8, dq), axis=0)
            for i in range(0, dq, 128):
                square = square + lanes[:, i:i + 128]

    def block(xx, yy):
        return lax.rem(yy + 2 * n_dp, n_dp) * n_pp + 2 * lax.rem(xx + 2 * n_x, n_x) + c

    colours = []
    for q, (axes, sign) in enumerate((("xy", 1), ("xy", -1), ("yx", 1), ("yx", -1))):
        sizes = (n_x, n_dp) if axes == "xy" else (n_dp, n_x)
        to_x = {"pp": 2 * lax.rem(x + sign + n_x, n_x) + c}
        to_y = {"dp": lax.rem(y + sign + n_dp, n_dp)}
        dest = (to_x, to_y) if axes == "xy" else (to_y, to_x)
        colours.append((q, axes, sign, sizes, dest, ring_plan(*sizes)))

    def holder(axes, sign, s, t):
        return block(x - sign * s, y - sign * t) if axes == "xy" else block(x - sign * t, y - sign * s)

    def message(colour, item, coming):
        q, axes, sign, _, dest, plan = colour
        phase, s, t = item
        at = plan.index(item)
        s_at, t_at = (s + coming, t) if phase == 1 else (s, t + coming)
        b = holder(axes, sign, s_at, t_at)
        return remote(g_ref.at[b, q], g_ref.at[b, q], ag_s.at[q, at], ag_r.at[q, at], dest[phase - 1])

    def mate_copy(q, slot, b):
        return remote(g_ref.at[b, q], g_ref.at[b, q], d_s.at[q, slot], d_r.at[q, slot], {"pp": mate})

    sends = []

    def push(cp):
        cp.start()
        sends.append(cp)

    for colour in colours:
        if colour[3][0] > 1:
            push(message(colour, (1, 0, 0), 0))
    for colour in colours:
        if colour[3][1] > 1:
            push(message(colour, (2, 0, 0), 0))

    def norm_swap(value, buf, send, recv, axis, me, n):
        buf[me] = value
        return [remote(buf.at[me], buf.at[me], send.at[o - 1], recv.at[o - 1], {axis: lax.rem(me + o, n)}) for o in range(1, n)], [
            remote(buf.at[lax.rem(me + n - o, n)], buf.at[lax.rem(me + n - o, n)], send.at[o - 1], recv.at[o - 1], {axis: lax.rem(me + o, n)}) for o in range(1, n)]

    norm_out, norm_in = norm_swap(square, nb_p, np_s, np_r, "pp", p, n_pp)
    for cp in norm_out:
        push(cp)
    for q in range(4):
        push(mate_copy(q, 0, own))

    steps = n_x * n_dp - 1
    for i in range(steps):
        for colour in colours:
            q, axes, sign, sizes, dest, plan = colour
            phase, s, t = plan[i]
            message(colour, plan[i], 1).wait_recv()
            if phase == 1:
                if s + 1 < sizes[0] - 1:
                    push(message(colour, (1, s + 1, 0), 0))
                if sizes[1] > 1:
                    push(message(colour, (2, s + 1, 0), 0))
                push(mate_copy(q, i + 1, holder(axes, sign, s + 1, 0)))
            else:
                if t + 1 < sizes[1] - 1:
                    push(message(colour, (2, s, t + 1), 0))
                push(mate_copy(q, i + 1, holder(axes, sign, s, t + 1)))
        if i == 0:
            for cp in norm_in:
                cp.wait_recv()
            total = nb_p[0]
            for o in range(1, n_pp):
                total = total + nb_p[o]
            norm_out, norm_in = norm_swap(total, nb_y, ny_s, ny_r, "dp", y, n_dp)
            for cp in norm_out:
                push(cp)
        if i == 1:
            for cp in norm_in:
                cp.wait_recv()
            total = nb_y[0]
            for o in range(1, n_dp):
                total = total + nb_y[o]
            norm_out, norm_in = norm_swap(total, nb_z, nz_s, nz_r, "tp", z, n_tp)
            for cp in norm_out:
                push(cp)
        if i == 2:
            for cp in norm_in:
                cp.wait_recv()
            total = nb_z[0]
            for o in range(1, n_tp):
                total = total + nb_z[o]
            norm = jnp.sqrt(jnp.sum(total, axis=(0, 1), keepdims=True))
            scale_ref[...] = jnp.broadcast_to(CLIP_NORM / jnp.maximum(norm, CLIP_NORM), (8, 128))

    for q, axes, sign, sizes, dest, plan in colours:
        for i in range(steps + 1):
            if i == 0:
                b = own
            else:
                phase, s, t = plan[i - 1]
                b = holder(axes, sign, s + 1, 0) if phase == 1 else holder(axes, sign, s, t + 1)
            mate_copy(q, i, b + 1 - 2 * c).wait_recv()
    for cp in (rel_a, rel_b, one_a, one_b, com_a, com_b, *sends):
        cp.wait_send()
    for cp in loads:
        cp.wait()


def plane_gradient(master, acts, ids, exp_avg, exp_avg_sq, n_tp, n_dp, n_pp):
    vocab, dim = master.shape
    tok = acts.shape[0]
    rows = -(-vocab // (n_pp * n_dp))
    rows = -(-rows // 8) * 8
    dq = dim // 4
    n_chunk = 12 if tok % (4 * 12 * 8) == 0 else 6
    lag = 2
    steps = (n_pp // 2) * n_dp
    n_pre = max(PRE_BLOCKS, -(-2 * tok // (3 * rows)))
    full = pl.BlockSpec(memory_space=VMEM)
    any_space = pl.BlockSpec(memory_space=pl.ANY)
    half = VMEM((2, 2, rows, dq), F32)
    chunk = DMA((2, n_chunk))
    return pl.pallas_call(
        functools.partial(grad_kernel, n_tp, n_dp, n_pp, n_chunk, lag),
        out_shape=(VMEM((n_dp * n_pp, 4, rows, dq), F32), jax.ShapeDtypeStruct((8, 128), F32), VMEM((3 * n_pre * rows, dim), F32)),
        in_specs=[any_space, any_space, full, any_space, any_space],
        out_specs=(full, full, full),
        scratch_shapes=[
            VMEM((tok, dim), BF16), VMEM((tok, dim), BF16),
            VMEM((1, tok), jnp.int32), VMEM((1, tok), jnp.int32), VMEM((n_dp, rows, dim), BF16),
            VMEM((n_dp, rows, tok), F32), VMEM((rows, tok), BF16), VMEM((n_dp, 4, rows, dq), F32),
            VMEM((2, tok), F32), VMEM((2, tok), F32), VMEM((n_pp - 1, 2, tok), F32), VMEM((n_tp - 1, 2, tok), F32),
            half, half, half,
            VMEM((n_pp, 8, 128), F32), VMEM((n_dp, 8, 128), F32), VMEM((n_tp, 8, 128), F32),
            DMA((1 + 4 * n_dp,)), *[chunk] * 9, DMA((2, n_pp - 1)), DMA((2,)),
            DMA((n_pp - 1,)), DMA((n_pp - 1,)), DMA((n_tp - 1,)), DMA((n_tp - 1,)), DMA((6,)), DMA((6,)),
            DMA((n_pp - 1,)), DMA((n_pp - 1,)), DMA((n_dp - 1,)), DMA((n_dp - 1,)), DMA((n_tp - 1,)), DMA((n_tp - 1,)),
            DMA((4, steps)), DMA((4, steps)), DMA((4, steps)), DMA((4, steps)), DMA((3 * n_pre,)),
        ],
        compiler_params=pltpu.CompilerParams(collective_id=0, has_side_effects=True, vmem_limit_bytes=21 << 20),
        name="plane_gradient",
    )(master, acts, ids, exp_avg, exp_avg_sq)


def adamw_kernel(n_slot, ahead, scale_ref, g_ref, pre_ref, e_hbm, m_hbm, v_hbm, ne_hbm, nm_hbm, nv_hbm, nb_hbm, e_buf, m_buf, v_buf, b_buf, in_s, out_s):
    n_blk, _, rows, dq = g_ref.shape
    vocab = e_hbm.shape[0]
    last = vocab - (n_blk - 1) * rows
    scale = scale_ref[0:1, 0:1]

    def loads(i, count):
        slot = lax.rem(i, n_slot)
        here = pl.ds(pl.multiple_of(i * rows, 8), count)
        return [pltpu.make_async_copy(hbm.at[here], buf.at[slot, pl.ds(0, count)], in_s.at[a, slot]) for a, (hbm, buf) in enumerate(((e_hbm, e_buf), (m_hbm, m_buf), (v_hbm, v_buf)))]

    def stores(i, count):
        slot = lax.rem(i, n_slot)
        here = pl.ds(pl.multiple_of(i * rows, 8), count)
        return [pltpu.make_async_copy(buf.at[slot, pl.ds(0, count)], hbm.at[here], out_s.at[a, slot]) for a, (buf, hbm) in enumerate(((e_buf, ne_hbm), (m_buf, nm_hbm), (v_buf, nv_hbm), (b_buf, nb_hbm)))]

    def each(copies, i, act):
        if last == rows:
            for cp in copies(i, rows):
                act(cp)
            return
        for cond, count in ((i < n_blk - 1, rows), (i == n_blk - 1, last)):
            @pl.when(cond)
            def _(count=count):
                for cp in copies(i, count):
                    act(cp)

    n_pre = pre_ref.shape[0] // (3 * rows)

    for i in range(n_pre, min(ahead, n_blk)):
        each(loads, i, lambda cp: cp.start())

    @pl.loop(0, n_blk)
    def _(i):
        slot = lax.rem(i, n_slot)

        @pl.when(i + ahead < n_blk)
        def _():
            @pl.when(i + ahead >= n_slot)
            def _():
                each(stores, i + ahead - n_slot, lambda cp: cp.wait())

            @pl.when(i + ahead >= n_pre)
            def _():
                each(loads, i + ahead, lambda cp: cp.start())

        def update(read):
            @pl.loop(0, rows // 8, unroll=5 if rows % 40 == 0 else 1)
            def _(r):
                at = pl.ds(pl.multiple_of(r * 8, 8), 8)
                for q in range(4):
                    cols = pl.ds(q * dq, dq)
                    g = g_ref[i, q, at, :] * scale
                    e, m, v = read(r, at, cols)
                    m = BETA_ONE * m + (1.0 - BETA_ONE) * g
                    v = BETA_TWO * v + (1.0 - BETA_TWO) * g * g
                    step = (m * (1.0 / (1.0 - BETA_ONE ** OPT_STEP))) / (jnp.sqrt(v * (1.0 / (1.0 - BETA_TWO ** OPT_STEP))) + ADAM_EPS)
                    ne = e - LEARN_RATE * (step + WEIGHT_DECAY * e)
                    e_buf[slot, at, cols] = ne
                    m_buf[slot, at, cols] = m
                    v_buf[slot, at, cols] = v
                    b_buf[slot, at, cols] = ne.astype(BF16)

        @pl.when(i < n_pre)
        def _():
            def read(r, at, cols):
                return [pre_ref[pl.ds(pl.multiple_of((3 * i + a) * rows + r * 8, 8), 8), cols] for a in range(3)]

            update(read)

        @pl.when(i >= n_pre)
        def _():
            each(loads, i, lambda cp: cp.wait())
            update(lambda r, at, cols: [buf[slot, at, cols] for buf in (e_buf, m_buf, v_buf)])

        each(stores, i, lambda cp: cp.start())

    for i in range(max(0, n_blk - n_slot), n_blk):
        each(stores, i, lambda cp: cp.wait())


def adamw(scale, grad, pre, master, exp_avg, exp_avg_sq):
    vocab, dim = master.shape
    rows = grad.shape[2]
    n_slot = 6
    full = pl.BlockSpec(memory_space=VMEM)
    any_space = pl.BlockSpec(memory_space=pl.ANY)
    f32 = jax.ShapeDtypeStruct((vocab, dim), F32)
    count = vocab * dim
    ring = VMEM((n_slot, rows, dim), F32)
    return pl.pallas_call(
        functools.partial(adamw_kernel, n_slot, 3),
        out_shape=(f32, f32, f32, jax.ShapeDtypeStruct((vocab, dim), BF16)),
        in_specs=[full, full, full, any_space, any_space, any_space],
        out_specs=(any_space,) * 4,
        scratch_shapes=[ring, ring, ring, VMEM((n_slot, rows, dim), BF16), DMA((3, n_slot)), DMA((4, n_slot))],
        cost_estimate=pl.CostEstimate(flops=20 * count, bytes_accessed=30 * count, transcendentals=2 * count),
        compiler_params=pltpu.CompilerParams(vmem_limit_bytes=21 << 20),
        name="adamw",
    )(scale, in_vmem(grad), in_vmem(pre), master, exp_avg, exp_avg_sq)


def solution(mesh):
    n_pp, n_dp, n_tp = mesh.shape["pp"], mesh.shape["dp"], mesh.shape["tp"]
    table_spec = P("tp", None)

    def device_step(master, exp_avg, exp_avg_sq, stage_ids, stage_acts):
        vocab, dim = master.shape
        tok = stage_ids.shape[1] * stage_ids.shape[2]
        acts = stage_acts.reshape(tok, dim)
        grad, scale, pre = plane_gradient(master, acts, stage_ids.reshape(1, tok), exp_avg, exp_avg_sq, n_tp, n_dp, n_pp)
        return adamw(scale, grad, pre, master, exp_avg, exp_avg_sq)

    return jax.shard_map(device_step, mesh=mesh, in_specs=(table_spec, table_spec, table_spec, P("pp", "dp", None), P("pp", "dp", None, None)), out_specs=(table_spec, table_spec, table_spec, table_spec), check_vma=False)
```

```python
import functools

import jax
import jax.numpy as jnp
from jax import lax
from jax.experimental import pallas as pl
from jax.experimental.pallas import tpu as pltpu
from jax.sharding import PartitionSpec as P

LEARN_RATE = 0.003
BETA_ONE = 0.9
BETA_TWO = 0.95
ADAM_EPS = 1e-8
WEIGHT_DECAY = 0.1
CLIP_NORM = 1.0
OPT_STEP = 10

MESH_ID = pl.DeviceIdType.MESH
LOW = -1e30
VMEM = pltpu.VMEM
DMA = pltpu.SemaphoreType.DMA
F32, BF16 = jnp.float32, jnp.bfloat16
PRE_BLOCKS = 6
scope = jax.named_scope


def remote(src, dst, send, recv, where):
    return pltpu.make_async_remote_copy(src_ref=src, dst_ref=dst, send_sem=send, recv_sem=recv, device_id=where, device_id_type=MESH_ID)


def in_vmem(arr):
    return pltpu.with_memory_space_constraint(arr, VMEM)


def enter(groups):
    barrier = pltpu.get_barrier_semaphore()
    for axis, peer in groups:
        pl.semaphore_signal(barrier, inc=1, device_id={axis: peer}, device_id_type=MESH_ID)
    pl.semaphore_wait(barrier, len(groups))


def ring_plan(n_one, n_two):
    items = [(1, s, 0) for s in range(n_one - 1)] + [(2, s, t) for s in range(n_one) for t in range(n_two - 1)]
    return sorted(items, key=lambda i: (i[1] + i[2], i[0], i[2]))


def grad_kernel(n_tp, n_dp, n_pp, n_chunk, lag, table_ref, acts_ref, ids_ref, avg_ref, sq_ref, g_ref, scale_ref, pre_ref, hid_ref, dx_ref, lab_ref, look_ref, tab_ref, exp_ref, dl_ref, part_ref, stat_ref, mid_ref, buf_p, buf_z, rel_ref, one_ref, com_ref, nb_p, nb_y, nb_z, load_s, feed_s, send_x, send_z, send_d, send_e, recv_x, recv_z, recv_d, recv_e, id_s, id_r, sp_s, sp_r, sz_s, sz_r, rs_s, rs_r, np_s, np_r, ny_s, ny_r, nz_s, nz_r, ag_s, ag_r, d_s, d_r, pre_s):
    p, z, y = lax.axis_index("pp"), lax.axis_index("tp"), lax.axis_index("dp")
    n_x = n_pp // 2
    x, c, par = p // 2, lax.rem(p, 2), lax.rem(z, 2)
    mate = 2 * x + 1 - c
    vocab = table_ref.shape[0]
    rows, tok = exp_ref.shape[1:]
    dq = g_ref.shape[3]
    up_y, down_y = lax.rem(y + 1, n_dp), lax.rem(y + n_dp - 1, n_dp)

    def first_row(d):
        return (d * n_pp + p) * rows

    short = vocab - (n_dp * n_pp - 1) * rows

    def table_copies(count, blocks):
        return [pltpu.make_async_copy(table_ref.at[pl.ds(pl.multiple_of(first_row(d), 8), count), pl.ds(q * dq, dq)], part_ref.at[d, q, pl.ds(0, count)], load_s.at[1 + 4 * d + q]) for d in blocks for q in range(4)]

    def each_table_copy(act):
        for cp in table_copies(rows, range(n_dp - 1)):
            act(cp)
        for cond, count in ((p < n_pp - 1, rows), (p == n_pp - 1, short)):
            @pl.when(cond)
            def _(count=count):
                for cp in table_copies(count, (n_dp - 1,)):
                    act(cp)

    each_table_copy(lambda cp: cp.start())
    hid_buf, dx_buf = pre_ref.at[pl.ds(0, tok)], pre_ref.at[pl.ds(tok, tok)]
    sources = ((n_pp - 1, hid_buf, hid_ref, lab_ref), (0, dx_buf, dx_ref, look_ref))
    for source, _, low, _ in sources:
        @pl.when(p == source)
        def _(low=low):
            pltpu.make_async_copy(acts_ref, low, load_s.at[0]).start()

    enter([("pp", lax.rem(p + o, n_pp)) for o in range(1, n_pp)] + [("tp", lax.rem(z + o, n_tp)) for o in range(1, n_tp)] + [("dp", lax.rem(y + o, n_dp)) for o in range(1, n_dp)])

    step_x = 1 - 2 * c
    next_p = 2 * lax.rem(x + step_x + n_x, n_x) + c
    next_z = lax.rem(z + step_x + n_tp, n_tp)
    size = tok // (4 * n_chunk)
    last = n_chunk + lag
    n_group = 3
    per_group = n_chunk // n_group
    group = tok // n_group

    def span(core, parity, k):
        return pl.ds(pl.multiple_of((4 * k + 2 * parity + core) * size, 8), size)

    class Stream:
        def __init__(self, a):
            self.a = a
            self.source, self.buf, self.low, self.ids = sources[a]
            self.is_src = p == self.source
            s_x = self.source // 2
            self.dist = lax.rem(jnp.where(c == 0, x - s_x, s_x - x) + n_x, n_x)

        def hop(self, part, send, recv, where):
            return remote(self.buf.at[part], self.buf.at[part], send, recv, where)

        def feed(self, k):
            return self.hop(span(1 - c, par, k), feed_s.at[self.a, k], recv_x.at[self.a, k], {"pp": mate})

        def ring(self, k):
            return self.hop(span(c, par, k), send_x.at[self.a, k], recv_x.at[self.a, k], {"pp": next_p})

        def plane(self, k, parity):
            return self.hop(span(c, parity, k), send_z.at[self.a, k], recv_z.at[self.a, k], {"tp": next_z})

        def across(self, k, core):
            return self.hop(span(core, par, k), send_d.at[self.a, k], recv_d.at[self.a, k], {"pp": mate})

        def again(self, k, core):
            return self.hop(span(core, 1 - par, k), send_e.at[self.a, k], recv_e.at[self.a, k], {"pp": mate})

        def id_copy(self, o):
            return remote(ids_ref, self.ids, id_s.at[self.a, o - 1], id_r.at[self.a], {"pp": lax.rem(p + o, n_pp)})

        def begin(self, with_ring):
            @pl.when(self.is_src)
            def _():
                pltpu.make_async_copy(acts_ref, self.low, load_s.at[0]).wait()
                self.ids[...] = ids_ref[...]

                @pl.loop(0, n_chunk)
                def _(k):
                    def widen(part):
                        self.buf[part, :] = self.low[part, :].astype(F32)

                    widen(span(1 - c, par, k))
                    self.feed(k).start()
                    widen(span(c, par, k))
                    if n_x > 1 and with_ring:
                        self.ring(k).start()
                    self.across(k, c).start()
                    widen(span(c, 1 - par, k))
                    self.again(k, c).start()

                for o in range(1, n_pp):
                    self.id_copy(o).start()

        def early_ring(self):
            @pl.when(mate == self.source)
            def _():
                @pl.loop(0, n_chunk)
                def _(k):
                    self.ring(k).wait_recv()
                    if n_x > 1:
                        self.ring(k).start()

        def late_ring(self, lo, hi):
            if n_x > 1:
                @pl.when(self.is_src)
                def _():
                    @pl.loop(lo, hi)
                    def _(k):
                        self.ring(k).start()

        def late_plane(self):
            @pl.when(mate == self.source)
            def _():
                @pl.loop(0, n_chunk)
                def _(k):
                    self.plane(k, par).start()

        def steps(self, lo, hi, early=False):
            @pl.when(jnp.logical_not(self.is_src))
            def _():
                @pl.loop(lo, hi)
                def _(k):
                    @pl.when(jnp.logical_and(k < n_chunk, jnp.logical_or(mate != self.source, not early)))
                    def _():
                        self.ring(k).wait_recv()
                        if n_x > 1:
                            @pl.when(self.dist < n_x - 1)
                            def _():
                                if early:
                                    @pl.when(jnp.logical_and(p == n_pp - 1, k >= 2))
                                    def _():
                                        self.ring(k - 2).wait_send()

                                self.ring(k).start()

                        self.plane(k, par).start()

                        @pl.when(mate != self.source)
                        def _():
                            self.across(k, c).start()

                    @pl.when(k >= lag)
                    def _():
                        self.plane(k - lag, 1 - par).wait_recv()

                        @pl.when(mate != self.source)
                        def _():
                            self.again(k - lag, c).start()

        def collect(self, g):
            @pl.when(jnp.logical_not(self.is_src))
            def _():
                if g == 0:
                    self.id_copy(1).wait_recv()

                @pl.loop(g * per_group, (g + 1) * per_group)
                def _(k):
                    self.across(k, 1 - c).wait_recv()
                    self.again(k, 1 - c).wait_recv()

                tile = min(128, group)

                @pl.loop(0, group // tile)
                def _(k):
                    here = pl.ds(pl.multiple_of(g * group + k * tile, tile), tile)
                    self.low[here, :] = self.buf[here, :].astype(BF16)

        def settle(self):
            @pl.when(self.is_src)
            def _():
                for o in range(1, n_pp):
                    self.id_copy(o).wait_send()

            @pl.loop(0, n_chunk)
            def _(k):
                @pl.when(self.is_src)
                def _():
                    self.feed(k).wait_send()

                @pl.when(jnp.logical_not(self.is_src))
                def _():
                    self.plane(k, par).wait_send()

                if n_x > 1:
                    begun = n_chunk if self.a == 0 else n_chunk - 2

                    @pl.when(jnp.logical_and(self.dist < n_x - 1, jnp.logical_or(p != n_pp - 1, k >= begun)))
                    def _():
                        self.ring(k).wait_send()

                @pl.when(mate != self.source)
                def _():
                    self.across(k, c).wait_send()
                    self.again(k, c).wait_send()

    hid_in, dx_in = Stream(0), Stream(1)
    wide = min(256, group)

    def logits(g):
        @pl.loop(0, group // wide)
        def _(j):
            cols = pl.ds(pl.multiple_of(g * group + j * wide, wide), wide)
            h = hid_ref[cols, :]
            top = jnp.full((1, wide), LOW, F32)
            for d in range(n_dp):
                lg = lax.dot_general(tab_ref[d], h, (((1,), (1,)), ((), ())), preferred_element_type=F32)
                if d == n_dp - 1 and short < rows:
                    ok = first_row(d) + lax.broadcasted_iota(jnp.int32, (rows, wide), 0) < vocab
                    lg = jnp.where(ok, lg, LOW)
                exp_ref[d, :, cols] = lg
                top = jnp.maximum(top, jnp.max(lg, axis=0, keepdims=True))
            tot = jnp.zeros((1, wide), F32)
            for d in range(n_dp):
                e = jnp.exp(exp_ref[d, :, cols] - top)
                exp_ref[d, :, cols] = e
                tot = tot + jnp.sum(e, axis=0, keepdims=True)
            stat_ref[0:1, cols] = top
            stat_ref[1:2, cols] = tot

    with scope("begin"):
        hid_in.begin(True)
        dx_in.begin(False)
        each_table_copy(lambda cp: cp.wait())
        for d in range(n_dp):
            for q in range(4):
                tab_ref[d, :, q * dq:(q + 1) * dq] = part_ref[d, q].astype(BF16)
    with scope("early"):
        dx_in.early_ring()
    dist = dx_in.dist

    def clip(value):
        return jnp.clip(jnp.where(p == 1, 0, value), 0, last)

    at_zero = clip(jnp.where(jnp.logical_or(p == n_pp - 1, hid_in.dist == n_x - 1), 0, jnp.where(c == 0, 4 - 2 * dist, 21 - 6 * dist)))
    at_one = jnp.where(c == 0, 11 - 3 * dist, 23 - 5 * dist)
    at_two = jnp.maximum(clip(jnp.where(p == n_pp - 1, last, at_one + 3)), at_zero)
    at_three = jnp.maximum(jnp.maximum(clip(at_one + 6), at_two), min(last, per_group + lag))
    at_one = jnp.maximum(clip(jnp.where(p == n_pp - 1, last, at_one)), at_zero)
    at_two = jnp.maximum(at_two, at_one)
    at_four = jnp.maximum(at_three, min(last, max(n_chunk, 2 * per_group + lag)))

    def prepare(g):
        with scope(f"hid_collect{g}"):
            hid_in.collect(g)
        with scope(f"logits{g}"):
            logits(g)

    at_end = jnp.logical_and(hid_in.dist == n_x - 1, jnp.logical_not(hid_in.is_src))

    @pl.when(at_end)
    def _():
        lo = 0
        for g in range(n_group - 1):
            hi = min(last, (g + 1) * per_group + lag + 1)
            with scope(f"hid{g}"):
                hid_in.steps(lo, hi)
            prepare(g)
            lo = hi
        with scope("hid2"):
            hid_in.steps(lo, last)
        dx_in.late_ring(0, n_chunk)
        dx_in.late_plane()

    @pl.when(jnp.logical_not(at_end))
    def _():
        with scope("hid2"):
            hid_in.steps(0, n_chunk)
            dx_in.late_ring(0, 2)
            hid_in.steps(n_chunk, last)
            dx_in.late_ring(2, n_chunk)
            dx_in.late_plane()
        with scope("dx0"):
            dx_in.steps(0, at_zero, True)
        for g in range(n_group - 1):
            prepare(g)

    prepare(n_group - 1)

    def swap(src, buf, send, recv, axis, me, n):
        return [remote(src, buf.at[o - 1], send.at[o - 1], recv.at[o - 1], {axis: lax.rem(me + o, n)}) for o in range(1, n)]

    def merge(src, buf, n):
        top = src[0:1, :]
        for o in range(1, n):
            top = jnp.maximum(top, buf[o - 1, 0:1, :])
        tot = src[1:2, :] * jnp.exp(src[0:1, :] - top)
        for o in range(1, n):
            tot = tot + buf[o - 1, 1:2, :] * jnp.exp(buf[o - 1, 0:1, :] - top)
        return top, tot

    def local_ids(ref, start, count):
        ids = ref[:, start:start + count] - z * vocab
        return jnp.where(ids < vocab, ids, -1)

    def row_ids(d, count):
        return first_row(d) + lax.broadcasted_iota(jnp.int32, (rows, count), 0)

    stage = swap(stat_ref, buf_p, sp_s, sp_r, "pp", p, n_pp)
    for cp in stage:
        cp.start()
    with scope("dx1"):
        if n_x > 1:
            @pl.when(p == n_pp - 1)
            def _():
                @pl.loop(0, n_chunk)
                def _(k):
                    hid_in.ring(k).wait_send()

        dx_in.steps(at_zero, at_one, True)
    with scope("stat1"):
        for cp in stage:
            cp.wait()
    top, tot = merge(stat_ref, buf_p, n_pp)
    mid_ref[0:1, :] = top
    mid_ref[1:2, :] = tot
    stage = swap(mid_ref, buf_z, sz_s, sz_r, "tp", z, n_tp)
    for cp in stage:
        cp.start()
    with scope("dx2"):
        dx_in.steps(at_one, at_two, True)
    with scope("stat2"):
        for cp in stage:
            cp.wait()
    top, tot = merge(mid_ref, buf_z, n_tp)
    mid_ref[0:1, :] = jnp.exp(stat_ref[0:1, :] - top) / (tot * tok)

    def head(d):
        prob = exp_ref[d] * mid_ref[0:1, :]
        hit = local_ids(lab_ref, 0, tok) == row_ids(d, tok)
        dl_ref[...] = jnp.where(hit, prob - 1.0 / tok, prob).astype(BF16)
        for q in range(4):
            part_ref[d, q] = jnp.dot(dl_ref[...], hid_ref[:, q * dq:(q + 1) * dq], preferred_element_type=F32)

    def lookup(g):
        def add(d):
            hot = (local_ids(look_ref, g * group, group) == row_ids(d, group)).astype(BF16)
            dl_ref[:, 0:group] = hot
            for q in range(4):
                part_ref[d, q] += jnp.dot(dl_ref[:, 0:group], dx_ref[g * group:(g + 1) * group, q * dq:(q + 1) * dq], preferred_element_type=F32)
        return add

    with scope("dx3"):
        dx_in.steps(at_two, at_three, True)
    with scope("head"):
        pl.loop(0, n_dp)(head)
    with scope("dx_group0"):
        dx_in.collect(0)
        pl.loop(0, n_dp)(lookup(0))
    with scope("dx4"):
        dx_in.steps(at_three, at_four, True)
    with scope("dx_group1"):
        dx_in.collect(1)
        pl.loop(0, n_dp)(lookup(1))
    with scope("dx5"):
        dx_in.steps(at_four, last, True)
    with scope("dx_group2"):
        dx_in.collect(2)

    lo, hi = pl.ds(0, 2), pl.ds(2, 2)
    far = lax.rem(y + 2, n_dp)
    rel_a = remote(part_ref.at[far, lo], rel_ref.at[0], rs_s.at[0], rs_r.at[0], {"dp": up_y})
    rel_b = remote(part_ref.at[far, hi], rel_ref.at[1], rs_s.at[1], rs_r.at[1], {"dp": down_y})
    one_b = remote(part_ref.at[up_y, hi], one_ref.at[1], rs_s.at[2], rs_r.at[2], {"dp": up_y})
    one_a = remote(part_ref.at[down_y, lo], one_ref.at[0], rs_s.at[3], rs_r.at[3], {"dp": down_y})
    com_a = remote(part_ref.at[up_y, lo], com_ref.at[0], rs_s.at[4], rs_r.at[4], {"dp": up_y})
    com_b = remote(part_ref.at[down_y, hi], com_ref.at[1], rs_s.at[5], rs_r.at[5], {"dp": down_y})
    add = lookup(n_group - 1)
    add(far)
    rel_a.start()
    rel_b.start()
    add(up_y)
    one_b.start()
    add(down_y)
    one_a.start()
    add(y)
    hid_in.settle()
    dx_in.settle()
    n_pre = pre_ref.shape[0] // (3 * rows)
    loads = [pltpu.make_async_copy(ref.at[pl.ds(i * rows, rows)], pre_ref.at[pl.ds((3 * i + a) * rows, rows)], pre_s.at[3 * i + a]) for i in range(n_pre) for a, ref in enumerate((table_ref, avg_ref, sq_ref))]
    for cp in loads:
        cp.start()
    with scope("relay"):
        rel_a.wait_recv()
    part_ref[up_y, lo] += rel_ref[0]
    com_a.start()
    rel_b.wait_recv()
    part_ref[down_y, hi] += rel_ref[1]
    com_b.start()
    own = y * n_pp + p
    square = jnp.zeros((8, 128), F32)
    with scope("one"):
        one_a.wait_recv()
        one_b.wait_recv()
    for half, cp in ((0, com_a), (1, com_b)):
        with scope("com"):
            cp.wait_recv()
        for q in range(2):
            total = (part_ref[y, 2 * half + q] + com_ref[half, q] + one_ref[half, q]) * (1.0 / n_dp)
            g_ref[own, 2 * half + q] = total
            lanes = jnp.sum((total * total).reshape(rows // 8, 8, dq), axis=0)
            for i in range(0, dq, 128):
                square = square + lanes[:, i:i + 128]

    def block(xx, yy):
        return lax.rem(yy + 2 * n_dp, n_dp) * n_pp + 2 * lax.rem(xx + 2 * n_x, n_x) + c

    colours = []
    for q, (axes, sign) in enumerate((("xy", 1), ("xy", -1), ("yx", 1), ("yx", -1))):
        sizes = (n_x, n_dp) if axes == "xy" else (n_dp, n_x)
        to_x = {"pp": 2 * lax.rem(x + sign + n_x, n_x) + c}
        to_y = {"dp": lax.rem(y + sign + n_dp, n_dp)}
        dest = (to_x, to_y) if axes == "xy" else (to_y, to_x)
        colours.append((q, axes, sign, sizes, dest, ring_plan(*sizes)))

    def holder(axes, sign, s, t):
        return block(x - sign * s, y - sign * t) if axes == "xy" else block(x - sign * t, y - sign * s)

    def message(colour, item, coming):
        q, axes, sign, _, dest, plan = colour
        phase, s, t = item
        at = plan.index(item)
        s_at, t_at = (s + coming, t) if phase == 1 else (s, t + coming)
        b = holder(axes, sign, s_at, t_at)
        return remote(g_ref.at[b, q], g_ref.at[b, q], ag_s.at[q, at], ag_r.at[q, at], dest[phase - 1])

    def mate_copy(q, slot, b):
        return remote(g_ref.at[b, q], g_ref.at[b, q], d_s.at[q, slot], d_r.at[q, slot], {"pp": mate})

    sends = []

    def push(cp):
        cp.start()
        sends.append(cp)

    for colour in colours:
        if colour[3][0] > 1:
            push(message(colour, (1, 0, 0), 0))
    for colour in colours:
        if colour[3][1] > 1:
            push(message(colour, (2, 0, 0), 0))

    def norm_swap(value, buf, send, recv, axis, me, n):
        buf[me] = value
        return [remote(buf.at[me], buf.at[me], send.at[o - 1], recv.at[o - 1], {axis: lax.rem(me + o, n)}) for o in range(1, n)], [
            remote(buf.at[lax.rem(me + n - o, n)], buf.at[lax.rem(me + n - o, n)], send.at[o - 1], recv.at[o - 1], {axis: lax.rem(me + o, n)}) for o in range(1, n)]

    norm_out, norm_in = norm_swap(square, nb_p, np_s, np_r, "pp", p, n_pp)
    for cp in norm_out:
        push(cp)
    for q in range(4):
        push(mate_copy(q, 0, own))

    steps = n_x * n_dp - 1
    for i in range(steps):
        for colour in colours:
            q, axes, sign, sizes, dest, plan = colour
            phase, s, t = plan[i]
            message(colour, plan[i], 1).wait_recv()
            if phase == 1:
                if s + 1 < sizes[0] - 1:
                    push(message(colour, (1, s + 1, 0), 0))
                if sizes[1] > 1:
                    push(message(colour, (2, s + 1, 0), 0))
                push(mate_copy(q, i + 1, holder(axes, sign, s + 1, 0)))
            else:
                if t + 1 < sizes[1] - 1:
                    push(message(colour, (2, s, t + 1), 0))
                push(mate_copy(q, i + 1, holder(axes, sign, s, t + 1)))
        if i == 0:
            for cp in norm_in:
                cp.wait_recv()
            total = nb_p[0]
            for o in range(1, n_pp):
                total = total + nb_p[o]
            norm_out, norm_in = norm_swap(total, nb_y, ny_s, ny_r, "dp", y, n_dp)
            for cp in norm_out:
                push(cp)
        if i == 1:
            for cp in norm_in:
                cp.wait_recv()
            total = nb_y[0]
            for o in range(1, n_dp):
                total = total + nb_y[o]
            norm_out, norm_in = norm_swap(total, nb_z, nz_s, nz_r, "tp", z, n_tp)
            for cp in norm_out:
                push(cp)
        if i == 2:
            for cp in norm_in:
                cp.wait_recv()
            total = nb_z[0]
            for o in range(1, n_tp):
                total = total + nb_z[o]
            norm = jnp.sqrt(jnp.sum(total, axis=(0, 1), keepdims=True))
            scale_ref[...] = jnp.broadcast_to(CLIP_NORM / jnp.maximum(norm, CLIP_NORM), (8, 128))

    for q, axes, sign, sizes, dest, plan in colours:
        for i in range(steps + 1):
            if i == 0:
                b = own
            else:
                phase, s, t = plan[i - 1]
                b = holder(axes, sign, s + 1, 0) if phase == 1 else holder(axes, sign, s, t + 1)
            mate_copy(q, i, b + 1 - 2 * c).wait_recv()
    for cp in (rel_a, rel_b, one_a, one_b, com_a, com_b, *sends):
        cp.wait_send()
    for cp in loads:
        cp.wait()


def plane_gradient(master, acts, ids, exp_avg, exp_avg_sq, n_tp, n_dp, n_pp):
    vocab, dim = master.shape
    tok = acts.shape[0]
    rows = -(-vocab // (n_pp * n_dp))
    rows = -(-rows // 8) * 8
    dq = dim // 4
    n_chunk = 12 if tok % (4 * 12 * 8) == 0 else 6
    lag = 2
    steps = (n_pp // 2) * n_dp
    n_pre = max(PRE_BLOCKS, -(-2 * tok // (3 * rows)))
    full = pl.BlockSpec(memory_space=VMEM)
    any_space = pl.BlockSpec(memory_space=pl.ANY)
    half = VMEM((2, 2, rows, dq), F32)
    chunk = DMA((2, n_chunk))
    return pl.pallas_call(
        functools.partial(grad_kernel, n_tp, n_dp, n_pp, n_chunk, lag),
        out_shape=(VMEM((n_dp * n_pp, 4, rows, dq), F32), jax.ShapeDtypeStruct((8, 128), F32), VMEM((3 * n_pre * rows, dim), F32)),
        in_specs=[any_space, any_space, full, any_space, any_space],
        out_specs=(full, full, full),
        scratch_shapes=[
            VMEM((tok, dim), BF16), VMEM((tok, dim), BF16),
            VMEM((1, tok), jnp.int32), VMEM((1, tok), jnp.int32), VMEM((n_dp, rows, dim), BF16),
            VMEM((n_dp, rows, tok), F32), VMEM((rows, tok), BF16), VMEM((n_dp, 4, rows, dq), F32),
            VMEM((2, tok), F32), VMEM((2, tok), F32), VMEM((n_pp - 1, 2, tok), F32), VMEM((n_tp - 1, 2, tok), F32),
            half, half, half,
            VMEM((n_pp, 8, 128), F32), VMEM((n_dp, 8, 128), F32), VMEM((n_tp, 8, 128), F32),
            DMA((1 + 4 * n_dp,)), *[chunk] * 9, DMA((2, n_pp - 1)), DMA((2,)),
            DMA((n_pp - 1,)), DMA((n_pp - 1,)), DMA((n_tp - 1,)), DMA((n_tp - 1,)), DMA((6,)), DMA((6,)),
            DMA((n_pp - 1,)), DMA((n_pp - 1,)), DMA((n_dp - 1,)), DMA((n_dp - 1,)), DMA((n_tp - 1,)), DMA((n_tp - 1,)),
            DMA((4, steps)), DMA((4, steps)), DMA((4, steps)), DMA((4, steps)), DMA((3 * n_pre,)),
        ],
        compiler_params=pltpu.CompilerParams(collective_id=0, has_side_effects=True, vmem_limit_bytes=21 << 20),
        name="plane_gradient",
    )(master, acts, ids, exp_avg, exp_avg_sq)


def adamw_kernel(n_slot, ahead, scale_ref, g_ref, pre_ref, e_hbm, m_hbm, v_hbm, ne_hbm, nm_hbm, nv_hbm, nb_hbm, e_buf, m_buf, v_buf, b_buf, in_s, out_s):
    n_blk, _, rows, dq = g_ref.shape
    vocab = e_hbm.shape[0]
    last = vocab - (n_blk - 1) * rows
    scale = scale_ref[0:1, 0:1]

    def loads(i, count):
        slot = lax.rem(i, n_slot)
        here = pl.ds(pl.multiple_of(i * rows, 8), count)
        return [pltpu.make_async_copy(hbm.at[here], buf.at[slot, pl.ds(0, count)], in_s.at[a, slot]) for a, (hbm, buf) in enumerate(((e_hbm, e_buf), (m_hbm, m_buf), (v_hbm, v_buf)))]

    def stores(i, count):
        slot = lax.rem(i, n_slot)
        here = pl.ds(pl.multiple_of(i * rows, 8), count)
        return [pltpu.make_async_copy(buf.at[slot, pl.ds(0, count)], hbm.at[here], out_s.at[a, slot]) for a, (buf, hbm) in enumerate(((e_buf, ne_hbm), (m_buf, nm_hbm), (v_buf, nv_hbm), (b_buf, nb_hbm)))]

    def each(copies, i, act):
        if last == rows:
            for cp in copies(i, rows):
                act(cp)
            return
        for cond, count in ((i < n_blk - 1, rows), (i == n_blk - 1, last)):
            @pl.when(cond)
            def _(count=count):
                for cp in copies(i, count):
                    act(cp)

    n_pre = pre_ref.shape[0] // (3 * rows)

    for i in range(n_pre, min(ahead, n_blk)):
        each(loads, i, lambda cp: cp.start())

    @pl.loop(0, n_blk)
    def _(i):
        slot = lax.rem(i, n_slot)

        @pl.when(i + ahead < n_blk)
        def _():
            @pl.when(i + ahead >= n_slot)
            def _():
                each(stores, i + ahead - n_slot, lambda cp: cp.wait())

            @pl.when(i + ahead >= n_pre)
            def _():
                each(loads, i + ahead, lambda cp: cp.start())

        def update(read):
            @pl.loop(0, rows // 8, unroll=5 if rows % 40 == 0 else 1)
            def _(r):
                at = pl.ds(pl.multiple_of(r * 8, 8), 8)
                for q in range(4):
                    cols = pl.ds(q * dq, dq)
                    g = g_ref[i, q, at, :] * scale
                    e, m, v = read(r, at, cols)
                    m = BETA_ONE * m + (1.0 - BETA_ONE) * g
                    v = BETA_TWO * v + (1.0 - BETA_TWO) * g * g
                    step = (m * (1.0 / (1.0 - BETA_ONE ** OPT_STEP))) / (jnp.sqrt(v * (1.0 / (1.0 - BETA_TWO ** OPT_STEP))) + ADAM_EPS)
                    ne = e - LEARN_RATE * (step + WEIGHT_DECAY * e)
                    e_buf[slot, at, cols] = ne
                    m_buf[slot, at, cols] = m
                    v_buf[slot, at, cols] = v
                    b_buf[slot, at, cols] = ne.astype(BF16)

        @pl.when(i < n_pre)
        def _():
            def read(r, at, cols):
                return [pre_ref[pl.ds(pl.multiple_of((3 * i + a) * rows + r * 8, 8), 8), cols] for a in range(3)]

            update(read)

        @pl.when(i >= n_pre)
        def _():
            each(loads, i, lambda cp: cp.wait())
            update(lambda r, at, cols: [buf[slot, at, cols] for buf in (e_buf, m_buf, v_buf)])

        each(stores, i, lambda cp: cp.start())

    for i in range(max(0, n_blk - n_slot), n_blk):
        each(stores, i, lambda cp: cp.wait())


def adamw(scale, grad, pre, master, exp_avg, exp_avg_sq):
    vocab, dim = master.shape
    rows = grad.shape[2]
    n_slot = 6
    full = pl.BlockSpec(memory_space=VMEM)
    any_space = pl.BlockSpec(memory_space=pl.ANY)
    f32 = jax.ShapeDtypeStruct((vocab, dim), F32)
    count = vocab * dim
    ring = VMEM((n_slot, rows, dim), F32)
    return pl.pallas_call(
        functools.partial(adamw_kernel, n_slot, 3),
        out_shape=(f32, f32, f32, jax.ShapeDtypeStruct((vocab, dim), BF16)),
        in_specs=[full, full, full, any_space, any_space, any_space],
        out_specs=(any_space,) * 4,
        scratch_shapes=[ring, ring, ring, VMEM((n_slot, rows, dim), BF16), DMA((3, n_slot)), DMA((4, n_slot))],
        cost_estimate=pl.CostEstimate(flops=20 * count, bytes_accessed=30 * count, transcendentals=2 * count),
        compiler_params=pltpu.CompilerParams(vmem_limit_bytes=21 << 20),
        name="adamw",
    )(scale, in_vmem(grad), in_vmem(pre), master, exp_avg, exp_avg_sq)


def solution(mesh):
    n_pp, n_dp, n_tp = mesh.shape["pp"], mesh.shape["dp"], mesh.shape["tp"]
    table_spec = P("tp", None)

    def device_step(master, exp_avg, exp_avg_sq, stage_ids, stage_acts):
        vocab, dim = master.shape
        tok = stage_ids.shape[1] * stage_ids.shape[2]
        acts = stage_acts.reshape(tok, dim)
        grad, scale, pre = plane_gradient(master, acts, stage_ids.reshape(1, tok), exp_avg, exp_avg_sq, n_tp, n_dp, n_pp)
        return adamw(scale, grad, pre, master, exp_avg, exp_avg_sq)

    return jax.shard_map(device_step, mesh=mesh, in_specs=(table_spec, table_spec, table_spec, P("pp", "dp", None), P("pp", "dp", None, None)), out_specs=(table_spec, table_spec, table_spec, table_spec), check_vma=False)
```

```python
import functools

import jax
import jax.numpy as jnp
from jax import lax
from jax.experimental import pallas as pl
from jax.experimental.pallas import tpu as pltpu
from jax.sharding import PartitionSpec as P

LEARN_RATE = 0.003
BETA_ONE = 0.9
BETA_TWO = 0.95
ADAM_EPS = 1e-8
WEIGHT_DECAY = 0.1
CLIP_NORM = 1.0
OPT_STEP = 10

MESH_ID = pl.DeviceIdType.MESH
LOW = -1e30
VMEM = pltpu.VMEM
DMA = pltpu.SemaphoreType.DMA
F32, BF16 = jnp.float32, jnp.bfloat16
PRE_BLOCKS = 6
scope = jax.named_scope


def remote(src, dst, send, recv, where):
    return pltpu.make_async_remote_copy(src_ref=src, dst_ref=dst, send_sem=send, recv_sem=recv, device_id=where, device_id_type=MESH_ID)


def in_vmem(arr):
    return pltpu.with_memory_space_constraint(arr, VMEM)


def enter(groups):
    barrier = pltpu.get_barrier_semaphore()
    for axis, peer in groups:
        pl.semaphore_signal(barrier, inc=1, device_id={axis: peer}, device_id_type=MESH_ID)
    pl.semaphore_wait(barrier, len(groups))


def ring_plan(n_one, n_two):
    items = [(1, s, 0) for s in range(n_one - 1)] + [(2, s, t) for s in range(n_one) for t in range(n_two - 1)]
    return sorted(items, key=lambda i: (i[1] + i[2], i[0], i[2]))


def grad_kernel(n_tp, n_dp, n_pp, n_chunk, lag, table_ref, acts_ref, ids_ref, avg_ref, sq_ref, g_ref, scale_ref, pre_ref, hid_ref, dx_ref, lab_ref, look_ref, tab_ref, exp_ref, dl_ref, part_ref, stat_ref, mid_ref, buf_p, buf_z, rel_ref, one_ref, com_ref, nb_p, nb_y, nb_z, load_s, feed_s, send_x, send_z, send_d, send_e, recv_x, recv_z, recv_d, recv_e, id_s, id_r, sp_s, sp_r, sz_s, sz_r, rs_s, rs_r, np_s, np_r, ny_s, ny_r, nz_s, nz_r, ag_s, ag_r, d_s, d_r, pre_s):
    p, z, y = lax.axis_index("pp"), lax.axis_index("tp"), lax.axis_index("dp")
    n_x = n_pp // 2
    x, c, par = p // 2, lax.rem(p, 2), lax.rem(z, 2)
    mate = 2 * x + 1 - c
    vocab = table_ref.shape[0]
    rows, tok = exp_ref.shape[1:]
    dq = g_ref.shape[3]
    up_y, down_y = lax.rem(y + 1, n_dp), lax.rem(y + n_dp - 1, n_dp)

    def first_row(d):
        return (d * n_pp + p) * rows

    short = vocab - (n_dp * n_pp - 1) * rows

    def table_copies(count, blocks):
        return [pltpu.make_async_copy(table_ref.at[pl.ds(pl.multiple_of(first_row(d), 8), count), pl.ds(q * dq, dq)], part_ref.at[d, q, pl.ds(0, count)], load_s.at[1 + 4 * d + q]) for d in blocks for q in range(4)]

    def each_table_copy(act):
        for cp in table_copies(rows, range(n_dp - 1)):
            act(cp)
        for cond, count in ((p < n_pp - 1, rows), (p == n_pp - 1, short)):
            @pl.when(cond)
            def _(count=count):
                for cp in table_copies(count, (n_dp - 1,)):
                    act(cp)

    each_table_copy(lambda cp: cp.start())
    hid_buf, dx_buf = pre_ref.at[pl.ds(0, tok)], pre_ref.at[pl.ds(tok, tok)]
    sources = ((n_pp - 1, hid_buf, hid_ref, lab_ref), (0, dx_buf, dx_ref, look_ref))
    for source, _, low, _ in sources:
        @pl.when(p == source)
        def _(low=low):
            pltpu.make_async_copy(acts_ref, low, load_s.at[0]).start()

    enter([("pp", lax.rem(p + o, n_pp)) for o in range(1, n_pp)] + [("tp", lax.rem(z + o, n_tp)) for o in range(1, n_tp)] + [("dp", lax.rem(y + o, n_dp)) for o in range(1, n_dp)])

    step_x = 1 - 2 * c
    next_p = 2 * lax.rem(x + step_x + n_x, n_x) + c
    next_z = lax.rem(z + step_x + n_tp, n_tp)
    size = tok // (4 * n_chunk)
    last = n_chunk + lag
    n_piece, n_group = 6, 3
    per_group = n_chunk // n_group
    group = tok // n_group

    def span(core, parity, k):
        return pl.ds(pl.multiple_of((4 * k + 2 * parity + core) * size, 8), size)

    class Stream:
        def __init__(self, a):
            self.a = a
            self.source, self.buf, self.low, self.ids = sources[a]
            self.is_src = p == self.source
            s_x = self.source // 2
            self.dist = lax.rem(jnp.where(c == 0, x - s_x, s_x - x) + n_x, n_x)

        def hop(self, part, send, recv, where):
            return remote(self.buf.at[part], self.buf.at[part], send, recv, where)

        def feed(self, k):
            return self.hop(span(1 - c, par, k), feed_s.at[self.a, k], recv_x.at[self.a, k], {"pp": mate})

        def ring(self, k):
            return self.hop(span(c, par, k), send_x.at[self.a, k], recv_x.at[self.a, k], {"pp": next_p})

        def plane(self, k, parity):
            return self.hop(span(c, parity, k), send_z.at[self.a, k], recv_z.at[self.a, k], {"tp": next_z})

        def across(self, k, core):
            return self.hop(span(core, par, k), send_d.at[self.a, k], recv_d.at[self.a, k], {"pp": mate})

        def again(self, k, core):
            return self.hop(span(core, 1 - par, k), send_e.at[self.a, k], recv_e.at[self.a, k], {"pp": mate})

        def id_copy(self, o):
            return remote(ids_ref, self.ids, id_s.at[self.a, o - 1], id_r.at[self.a], {"pp": lax.rem(p + o, n_pp)})

        def begin(self, with_ring):
            @pl.when(self.is_src)
            def _():
                pltpu.make_async_copy(acts_ref, self.low, load_s.at[0]).wait()
                self.ids[...] = ids_ref[...]

                @pl.loop(0, n_chunk)
                def _(k):
                    def widen(part):
                        self.buf[part, :] = self.low[part, :].astype(F32)

                    widen(span(1 - c, par, k))
                    self.feed(k).start()
                    widen(span(c, par, k))
                    if n_x > 1 and with_ring:
                        self.ring(k).start()
                    self.across(k, c).start()
                    widen(span(c, 1 - par, k))
                    self.again(k, c).start()

                for o in range(1, n_pp):
                    self.id_copy(o).start()

        def early_ring(self):
            @pl.when(mate == self.source)
            def _():
                @pl.loop(0, n_chunk)
                def _(k):
                    self.ring(k).wait_recv()
                    if n_x > 1:
                        self.ring(k).start()

        def late_ring(self, lo, hi):
            if n_x > 1:
                @pl.when(self.is_src)
                def _():
                    @pl.loop(lo, hi)
                    def _(k):
                        self.ring(k).start()

        def late_plane(self):
            @pl.when(mate == self.source)
            def _():
                @pl.loop(0, n_chunk)
                def _(k):
                    self.plane(k, par).start()

        def steps(self, lo, hi, early=False):
            @pl.when(jnp.logical_not(self.is_src))
            def _():
                @pl.loop(lo, hi)
                def _(k):
                    @pl.when(jnp.logical_and(k < n_chunk, jnp.logical_or(mate != self.source, not early)))
                    def _():
                        self.ring(k).wait_recv()
                        if n_x > 1:
                            @pl.when(self.dist < n_x - 1)
                            def _():
                                if early:
                                    @pl.when(jnp.logical_and(p == n_pp - 1, k >= 2))
                                    def _():
                                        self.ring(k - 2).wait_send()

                                self.ring(k).start()

                        self.plane(k, par).start()

                        @pl.when(mate != self.source)
                        def _():
                            self.across(k, c).start()

                    @pl.when(k >= lag)
                    def _():
                        self.plane(k - lag, 1 - par).wait_recv()

                        @pl.when(mate != self.source)
                        def _():
                            self.again(k - lag, c).start()

        def collect(self, g, parts):
            @pl.when(jnp.logical_not(self.is_src))
            def _():
                if g == 0:
                    self.id_copy(1).wait_recv()

                per_part, count = n_chunk // parts, tok // parts

                @pl.loop(g * per_part, (g + 1) * per_part)
                def _(k):
                    self.across(k, 1 - c).wait_recv()
                    self.again(k, 1 - c).wait_recv()

                tile = min(128, count)

                @pl.loop(0, count // tile)
                def _(k):
                    here = pl.ds(pl.multiple_of(g * count + k * tile, tile), tile)
                    self.low[here, :] = self.buf[here, :].astype(BF16)

        def settle(self):
            @pl.when(self.is_src)
            def _():
                for o in range(1, n_pp):
                    self.id_copy(o).wait_send()

            @pl.loop(0, n_chunk)
            def _(k):
                @pl.when(self.is_src)
                def _():
                    self.feed(k).wait_send()

                @pl.when(jnp.logical_not(self.is_src))
                def _():
                    self.plane(k, par).wait_send()

                if n_x > 1:
                    begun = n_chunk if self.a == 0 else n_chunk - 2

                    @pl.when(jnp.logical_and(self.dist < n_x - 1, jnp.logical_or(p != n_pp - 1, k >= begun)))
                    def _():
                        self.ring(k).wait_send()

                @pl.when(mate != self.source)
                def _():
                    self.across(k, c).wait_send()
                    self.again(k, c).wait_send()

    hid_in, dx_in = Stream(0), Stream(1)
    wide = tok // n_piece

    def logits(g):
        cols = pl.ds(g * wide, wide)
        h = hid_ref[cols, :]
        top = jnp.full((1, wide), LOW, F32)
        for d in range(n_dp):
            lg = lax.dot_general(tab_ref[d], h, (((1,), (1,)), ((), ())), preferred_element_type=F32)
            if d == n_dp - 1 and short < rows:
                ok = first_row(d) + lax.broadcasted_iota(jnp.int32, (rows, wide), 0) < vocab
                lg = jnp.where(ok, lg, LOW)
            exp_ref[d, :, cols] = lg
            top = jnp.maximum(top, jnp.max(lg, axis=0, keepdims=True))
        tot = jnp.zeros((1, wide), F32)
        for d in range(n_dp):
            e = jnp.exp(exp_ref[d, :, cols] - top)
            exp_ref[d, :, cols] = e
            tot = tot + jnp.sum(e, axis=0, keepdims=True)
        stat_ref[0:1, cols] = top
        stat_ref[1:2, cols] = tot

    with scope("begin"):
        hid_in.begin(True)
        dx_in.begin(False)
        each_table_copy(lambda cp: cp.wait())
        for d in range(n_dp):
            for q in range(4):
                tab_ref[d, :, q * dq:(q + 1) * dq] = part_ref[d, q].astype(BF16)
    with scope("early"):
        dx_in.early_ring()
    dist = dx_in.dist

    def clip(value):
        return jnp.clip(jnp.where(p == 1, 0, value), 0, last)

    near = jnp.where(jnp.logical_or(jnp.logical_and(c == 0, dist == 1), jnp.logical_and(c == 1, dist >= 2)), 1, 0)
    near = jnp.where(jnp.logical_or(p == n_pp - 1, hid_in.dist == n_x - 1), 0, near)
    at_zero = near * jnp.where(c == 0, 2, jnp.maximum(12 - 3 * dist, 0))
    at_zero = jnp.minimum(at_zero, last - (n_piece - 2))
    at_half = at_zero + (n_piece - 2) * near
    at_one = jnp.where(p == n_pp - 1, last, jnp.where(c == 0, 11 - 3 * dist, 18 - 3 * dist))
    at_two = jnp.where(p == n_pp - 1, last, jnp.where(c == 0, at_one + 2, at_one + 3))
    at_three = jnp.where(p == n_pp - 1, last, jnp.where(c == 0, at_one + 5, at_one + 6))
    at_one = jnp.maximum(clip(at_one), at_half)
    at_two = jnp.maximum(clip(at_two), at_one)
    at_three = jnp.maximum(jnp.maximum(clip(at_three), at_two), min(last, per_group + lag))
    at_four = jnp.maximum(at_three, min(last, max(n_chunk, 2 * per_group + lag)))

    def prepare(g):
        with scope(f"hid_collect{g}"):
            hid_in.collect(g, n_piece)
        with scope(f"logits{g}"):
            logits(g)

    at_end = jnp.logical_and(hid_in.dist == n_x - 1, jnp.logical_not(hid_in.is_src))
    pair = n_chunk // n_piece

    @pl.when(at_end)
    def _():
        lo = 0
        for g in range(n_piece - 2):
            hi = min(last, (g + 1) * pair + lag + 1)
            with scope(f"hid{g}"):
                hid_in.steps(lo, hi)
            prepare(g)
            lo = hi
        with scope("hid_end"):
            hid_in.steps(lo, last)
        dx_in.late_ring(0, n_chunk)
        dx_in.late_plane()

    @pl.when(jnp.logical_not(at_end))
    def _():
        with scope("hid_end"):
            hid_in.steps(0, n_chunk)
            dx_in.late_ring(0, 2)
            hid_in.steps(n_chunk, last)
            dx_in.late_ring(2, n_chunk)
            dx_in.late_plane()
        with scope("dx0"):
            dx_in.steps(0, at_zero, True)
        for g in range(n_piece - 2):
            prepare(g)
            dx_in.steps(at_zero + g * near, at_zero + (g + 1) * near, True)

    for g in range(n_piece - 2, n_piece):
        prepare(g)

    def swap(src, buf, send, recv, axis, me, n):
        return [remote(src, buf.at[o - 1], send.at[o - 1], recv.at[o - 1], {axis: lax.rem(me + o, n)}) for o in range(1, n)]

    def merge(src, buf, n):
        top = src[0:1, :]
        for o in range(1, n):
            top = jnp.maximum(top, buf[o - 1, 0:1, :])
        tot = src[1:2, :] * jnp.exp(src[0:1, :] - top)
        for o in range(1, n):
            tot = tot + buf[o - 1, 1:2, :] * jnp.exp(buf[o - 1, 0:1, :] - top)
        return top, tot

    def local_ids(ref, start, count):
        ids = ref[:, start:start + count] - z * vocab
        return jnp.where(ids < vocab, ids, -1)

    def row_ids(d, count):
        return first_row(d) + lax.broadcasted_iota(jnp.int32, (rows, count), 0)

    stage = swap(stat_ref, buf_p, sp_s, sp_r, "pp", p, n_pp)
    for cp in stage:
        cp.start()
    with scope("dx1"):
        if n_x > 1:
            @pl.when(p == n_pp - 1)
            def _():
                @pl.loop(0, n_chunk)
                def _(k):
                    hid_in.ring(k).wait_send()

        dx_in.steps(at_half, at_one, True)
    with scope("stat1"):
        for cp in stage:
            cp.wait()
    top, tot = merge(stat_ref, buf_p, n_pp)
    mid_ref[0:1, :] = top
    mid_ref[1:2, :] = tot
    stage = swap(mid_ref, buf_z, sz_s, sz_r, "tp", z, n_tp)
    for cp in stage:
        cp.start()
    with scope("dx2"):
        dx_in.steps(at_one, at_two, True)
    with scope("stat2"):
        for cp in stage:
            cp.wait()
    top, tot = merge(mid_ref, buf_z, n_tp)
    mid_ref[0:1, :] = jnp.exp(stat_ref[0:1, :] - top) / (tot * tok)

    def head(d):
        prob = exp_ref[d] * mid_ref[0:1, :]
        hit = local_ids(lab_ref, 0, tok) == row_ids(d, tok)
        dl_ref[...] = jnp.where(hit, prob - 1.0 / tok, prob).astype(BF16)
        for q in range(4):
            part_ref[d, q] = jnp.dot(dl_ref[...], hid_ref[:, q * dq:(q + 1) * dq], preferred_element_type=F32)

    def lookup(g):
        def add(d):
            hot = (local_ids(look_ref, g * group, group) == row_ids(d, group)).astype(BF16)
            dl_ref[:, 0:group] = hot
            for q in range(4):
                part_ref[d, q] += jnp.dot(dl_ref[:, 0:group], dx_ref[g * group:(g + 1) * group, q * dq:(q + 1) * dq], preferred_element_type=F32)
        return add

    with scope("dx3"):
        dx_in.steps(at_two, at_three, True)
    with scope("head"):
        pl.loop(0, n_dp)(head)
    with scope("dx_group0"):
        dx_in.collect(0, n_group)
        pl.loop(0, n_dp)(lookup(0))
    with scope("dx4"):
        dx_in.steps(at_three, at_four, True)
    with scope("dx_group1"):
        dx_in.collect(1, n_group)
        pl.loop(0, n_dp)(lookup(1))
    with scope("dx5"):
        dx_in.steps(at_four, last, True)
    with scope("dx_group2"):
        dx_in.collect(2, n_group)

    lo, hi = pl.ds(0, 2), pl.ds(2, 2)
    far = lax.rem(y + 2, n_dp)
    rel_a = remote(part_ref.at[far, lo], rel_ref.at[0], rs_s.at[0], rs_r.at[0], {"dp": up_y})
    rel_b = remote(part_ref.at[far, hi], rel_ref.at[1], rs_s.at[1], rs_r.at[1], {"dp": down_y})
    one_b = remote(part_ref.at[up_y, hi], one_ref.at[1], rs_s.at[2], rs_r.at[2], {"dp": up_y})
    one_a = remote(part_ref.at[down_y, lo], one_ref.at[0], rs_s.at[3], rs_r.at[3], {"dp": down_y})
    com_a = remote(part_ref.at[up_y, lo], com_ref.at[0], rs_s.at[4], rs_r.at[4], {"dp": up_y})
    com_b = remote(part_ref.at[down_y, hi], com_ref.at[1], rs_s.at[5], rs_r.at[5], {"dp": down_y})
    add = lookup(n_group - 1)
    add(far)
    rel_a.start()
    rel_b.start()
    add(up_y)
    one_b.start()
    add(down_y)
    one_a.start()
    add(y)
    hid_in.settle()
    dx_in.settle()
    n_pre = pre_ref.shape[0] // (3 * rows)
    loads = [pltpu.make_async_copy(ref.at[pl.ds(i * rows, rows)], pre_ref.at[pl.ds((3 * i + a) * rows, rows)], pre_s.at[3 * i + a]) for i in range(n_pre) for a, ref in enumerate((table_ref, avg_ref, sq_ref))]
    for cp in loads:
        cp.start()
    with scope("relay"):
        rel_a.wait_recv()
    part_ref[up_y, lo] += rel_ref[0]
    com_a.start()
    rel_b.wait_recv()
    part_ref[down_y, hi] += rel_ref[1]
    com_b.start()
    own = y * n_pp + p
    square = jnp.zeros((8, 128), F32)
    with scope("one"):
        one_a.wait_recv()
        one_b.wait_recv()
    for half, cp in ((0, com_a), (1, com_b)):
        with scope("com"):
            cp.wait_recv()
        for q in range(2):
            total = (part_ref[y, 2 * half + q] + com_ref[half, q] + one_ref[half, q]) * (1.0 / n_dp)
            g_ref[own, 2 * half + q] = total
            lanes = jnp.sum((total * total).reshape(rows // 8, 8, dq), axis=0)
            for i in range(0, dq, 128):
                square = square + lanes[:, i:i + 128]

    def block(xx, yy):
        return lax.rem(yy + 2 * n_dp, n_dp) * n_pp + 2 * lax.rem(xx + 2 * n_x, n_x) + c

    colours = []
    for q, (axes, sign) in enumerate((("xy", 1), ("xy", -1), ("yx", 1), ("yx", -1))):
        sizes = (n_x, n_dp) if axes == "xy" else (n_dp, n_x)
        to_x = {"pp": 2 * lax.rem(x + sign + n_x, n_x) + c}
        to_y = {"dp": lax.rem(y + sign + n_dp, n_dp)}
        dest = (to_x, to_y) if axes == "xy" else (to_y, to_x)
        colours.append((q, axes, sign, sizes, dest, ring_plan(*sizes)))

    def holder(axes, sign, s, t):
        return block(x - sign * s, y - sign * t) if axes == "xy" else block(x - sign * t, y - sign * s)

    def message(colour, item, coming):
        q, axes, sign, _, dest, plan = colour
        phase, s, t = item
        at = plan.index(item)
        s_at, t_at = (s + coming, t) if phase == 1 else (s, t + coming)
        b = holder(axes, sign, s_at, t_at)
        return remote(g_ref.at[b, q], g_ref.at[b, q], ag_s.at[q, at], ag_r.at[q, at], dest[phase - 1])

    def mate_copy(q, slot, b):
        return remote(g_ref.at[b, q], g_ref.at[b, q], d_s.at[q, slot], d_r.at[q, slot], {"pp": mate})

    sends = []

    def push(cp):
        cp.start()
        sends.append(cp)

    for colour in colours:
        if colour[3][0] > 1:
            push(message(colour, (1, 0, 0), 0))
    for colour in colours:
        if colour[3][1] > 1:
            push(message(colour, (2, 0, 0), 0))

    def norm_swap(value, buf, send, recv, axis, me, n):
        buf[me] = value
        return [remote(buf.at[me], buf.at[me], send.at[o - 1], recv.at[o - 1], {axis: lax.rem(me + o, n)}) for o in range(1, n)], [
            remote(buf.at[lax.rem(me + n - o, n)], buf.at[lax.rem(me + n - o, n)], send.at[o - 1], recv.at[o - 1], {axis: lax.rem(me + o, n)}) for o in range(1, n)]

    norm_out, norm_in = norm_swap(square, nb_p, np_s, np_r, "pp", p, n_pp)
    for cp in norm_out:
        push(cp)
    for q in range(4):
        push(mate_copy(q, 0, own))

    steps = n_x * n_dp - 1
    for i in range(steps):
        for colour in colours:
            q, axes, sign, sizes, dest, plan = colour
            phase, s, t = plan[i]
            message(colour, plan[i], 1).wait_recv()
            if phase == 1:
                if s + 1 < sizes[0] - 1:
                    push(message(colour, (1, s + 1, 0), 0))
                if sizes[1] > 1:
                    push(message(colour, (2, s + 1, 0), 0))
                push(mate_copy(q, i + 1, holder(axes, sign, s + 1, 0)))
            else:
                if t + 1 < sizes[1] - 1:
                    push(message(colour, (2, s, t + 1), 0))
                push(mate_copy(q, i + 1, holder(axes, sign, s, t + 1)))
        if i == 0:
            for cp in norm_in:
                cp.wait_recv()
            total = nb_p[0]
            for o in range(1, n_pp):
                total = total + nb_p[o]
            norm_out, norm_in = norm_swap(total, nb_y, ny_s, ny_r, "dp", y, n_dp)
            for cp in norm_out:
                push(cp)
        if i == 1:
            for cp in norm_in:
                cp.wait_recv()
            total = nb_y[0]
            for o in range(1, n_dp):
                total = total + nb_y[o]
            norm_out, norm_in = norm_swap(total, nb_z, nz_s, nz_r, "tp", z, n_tp)
            for cp in norm_out:
                push(cp)
        if i == 2:
            for cp in norm_in:
                cp.wait_recv()
            total = nb_z[0]
            for o in range(1, n_tp):
                total = total + nb_z[o]
            norm = jnp.sqrt(jnp.sum(total, axis=(0, 1), keepdims=True))
            scale_ref[...] = jnp.broadcast_to(CLIP_NORM / jnp.maximum(norm, CLIP_NORM), (8, 128))

    for q, axes, sign, sizes, dest, plan in colours:
        for i in range(steps + 1):
            if i == 0:
                b = own
            else:
                phase, s, t = plan[i - 1]
                b = holder(axes, sign, s + 1, 0) if phase == 1 else holder(axes, sign, s, t + 1)
            mate_copy(q, i, b + 1 - 2 * c).wait_recv()
    for cp in (rel_a, rel_b, one_a, one_b, com_a, com_b, *sends):
        cp.wait_send()
    for cp in loads:
        cp.wait()


def plane_gradient(master, acts, ids, exp_avg, exp_avg_sq, n_tp, n_dp, n_pp):
    vocab, dim = master.shape
    tok = acts.shape[0]
    rows = -(-vocab // (n_pp * n_dp))
    rows = -(-rows // 8) * 8
    dq = dim // 4
    n_chunk = 12 if tok % (4 * 12 * 8) == 0 else 6
    lag = 2
    steps = (n_pp // 2) * n_dp
    n_pre = max(PRE_BLOCKS, -(-2 * tok // (3 * rows)))
    full = pl.BlockSpec(memory_space=VMEM)
    any_space = pl.BlockSpec(memory_space=pl.ANY)
    half = VMEM((2, 2, rows, dq), F32)
    chunk = DMA((2, n_chunk))
    return pl.pallas_call(
        functools.partial(grad_kernel, n_tp, n_dp, n_pp, n_chunk, lag),
        out_shape=(VMEM((n_dp * n_pp, 4, rows, dq), F32), jax.ShapeDtypeStruct((8, 128), F32), VMEM((3 * n_pre * rows, dim), F32)),
        in_specs=[any_space, any_space, full, any_space, any_space],
        out_specs=(full, full, full),
        scratch_shapes=[
            VMEM((tok, dim), BF16), VMEM((tok, dim), BF16),
            VMEM((1, tok), jnp.int32), VMEM((1, tok), jnp.int32), VMEM((n_dp, rows, dim), BF16),
            VMEM((n_dp, rows, tok), F32), VMEM((rows, tok), BF16), VMEM((n_dp, 4, rows, dq), F32),
            VMEM((2, tok), F32), VMEM((2, tok), F32), VMEM((n_pp - 1, 2, tok), F32), VMEM((n_tp - 1, 2, tok), F32),
            half, half, half,
            VMEM((n_pp, 8, 128), F32), VMEM((n_dp, 8, 128), F32), VMEM((n_tp, 8, 128), F32),
            DMA((1 + 4 * n_dp,)), *[chunk] * 9, DMA((2, n_pp - 1)), DMA((2,)),
            DMA((n_pp - 1,)), DMA((n_pp - 1,)), DMA((n_tp - 1,)), DMA((n_tp - 1,)), DMA((6,)), DMA((6,)),
            DMA((n_pp - 1,)), DMA((n_pp - 1,)), DMA((n_dp - 1,)), DMA((n_dp - 1,)), DMA((n_tp - 1,)), DMA((n_tp - 1,)),
            DMA((4, steps)), DMA((4, steps)), DMA((4, steps)), DMA((4, steps)), DMA((3 * n_pre,)),
        ],
        compiler_params=pltpu.CompilerParams(collective_id=0, has_side_effects=True, vmem_limit_bytes=21 << 20),
        name="plane_gradient",
    )(master, acts, ids, exp_avg, exp_avg_sq)


def adamw_kernel(n_slot, ahead, scale_ref, g_ref, pre_ref, e_hbm, m_hbm, v_hbm, ne_hbm, nm_hbm, nv_hbm, nb_hbm, e_buf, m_buf, v_buf, b_buf, in_s, out_s):
    n_blk, _, rows, dq = g_ref.shape
    vocab = e_hbm.shape[0]
    last = vocab - (n_blk - 1) * rows
    scale = scale_ref[0:1, 0:1]

    def loads(i, count):
        slot = lax.rem(i, n_slot)
        here = pl.ds(pl.multiple_of(i * rows, 8), count)
        return [pltpu.make_async_copy(hbm.at[here], buf.at[slot, pl.ds(0, count)], in_s.at[a, slot]) for a, (hbm, buf) in enumerate(((e_hbm, e_buf), (m_hbm, m_buf), (v_hbm, v_buf)))]

    def stores(i, count):
        slot = lax.rem(i, n_slot)
        here = pl.ds(pl.multiple_of(i * rows, 8), count)
        return [pltpu.make_async_copy(buf.at[slot, pl.ds(0, count)], hbm.at[here], out_s.at[a, slot]) for a, (buf, hbm) in enumerate(((e_buf, ne_hbm), (m_buf, nm_hbm), (v_buf, nv_hbm), (b_buf, nb_hbm)))]

    def each(copies, i, act):
        if last == rows:
            for cp in copies(i, rows):
                act(cp)
            return
        for cond, count in ((i < n_blk - 1, rows), (i == n_blk - 1, last)):
            @pl.when(cond)
            def _(count=count):
                for cp in copies(i, count):
                    act(cp)

    n_pre = pre_ref.shape[0] // (3 * rows)

    for i in range(n_pre, min(ahead, n_blk)):
        each(loads, i, lambda cp: cp.start())

    @pl.loop(0, n_blk)
    def _(i):
        slot = lax.rem(i, n_slot)

        @pl.when(i + ahead < n_blk)
        def _():
            @pl.when(i + ahead >= n_slot)
            def _():
                each(stores, i + ahead - n_slot, lambda cp: cp.wait())

            @pl.when(i + ahead >= n_pre)
            def _():
                each(loads, i + ahead, lambda cp: cp.start())

        def update(read):
            @pl.loop(0, rows // 8, unroll=5 if rows % 40 == 0 else 1)
            def _(r):
                at = pl.ds(pl.multiple_of(r * 8, 8), 8)
                for q in range(4):
                    cols = pl.ds(q * dq, dq)
                    g = g_ref[i, q, at, :] * scale
                    e, m, v = read(r, at, cols)
                    m = BETA_ONE * m + (1.0 - BETA_ONE) * g
                    v = BETA_TWO * v + (1.0 - BETA_TWO) * g * g
                    step = (m * (1.0 / (1.0 - BETA_ONE ** OPT_STEP))) / (jnp.sqrt(v * (1.0 / (1.0 - BETA_TWO ** OPT_STEP))) + ADAM_EPS)
                    ne = e - LEARN_RATE * (step + WEIGHT_DECAY * e)
                    e_buf[slot, at, cols] = ne
                    m_buf[slot, at, cols] = m
                    v_buf[slot, at, cols] = v
                    b_buf[slot, at, cols] = ne.astype(BF16)

        @pl.when(i < n_pre)
        def _():
            def read(r, at, cols):
                return [pre_ref[pl.ds(pl.multiple_of((3 * i + a) * rows + r * 8, 8), 8), cols] for a in range(3)]

            update(read)

        @pl.when(i >= n_pre)
        def _():
            each(loads, i, lambda cp: cp.wait())
            update(lambda r, at, cols: [buf[slot, at, cols] for buf in (e_buf, m_buf, v_buf)])

        each(stores, i, lambda cp: cp.start())

    for i in range(max(0, n_blk - n_slot), n_blk):
        each(stores, i, lambda cp: cp.wait())


def adamw(scale, grad, pre, master, exp_avg, exp_avg_sq):
    vocab, dim = master.shape
    rows = grad.shape[2]
    n_slot = 6
    full = pl.BlockSpec(memory_space=VMEM)
    any_space = pl.BlockSpec(memory_space=pl.ANY)
    f32 = jax.ShapeDtypeStruct((vocab, dim), F32)
    count = vocab * dim
    ring = VMEM((n_slot, rows, dim), F32)
    return pl.pallas_call(
        functools.partial(adamw_kernel, n_slot, 3),
        out_shape=(f32, f32, f32, jax.ShapeDtypeStruct((vocab, dim), BF16)),
        in_specs=[full, full, full, any_space, any_space, any_space],
        out_specs=(any_space,) * 4,
        scratch_shapes=[ring, ring, ring, VMEM((n_slot, rows, dim), BF16), DMA((3, n_slot)), DMA((4, n_slot))],
        cost_estimate=pl.CostEstimate(flops=20 * count, bytes_accessed=30 * count, transcendentals=2 * count),
        compiler_params=pltpu.CompilerParams(vmem_limit_bytes=21 << 20),
        name="adamw",
    )(scale, in_vmem(grad), in_vmem(pre), master, exp_avg, exp_avg_sq)


def solution(mesh):
    n_pp, n_dp, n_tp = mesh.shape["pp"], mesh.shape["dp"], mesh.shape["tp"]
    table_spec = P("tp", None)

    def device_step(master, exp_avg, exp_avg_sq, stage_ids, stage_acts):
        vocab, dim = master.shape
        tok = stage_ids.shape[1] * stage_ids.shape[2]
        acts = stage_acts.reshape(tok, dim)
        grad, scale, pre = plane_gradient(master, acts, stage_ids.reshape(1, tok), exp_avg, exp_avg_sq, n_tp, n_dp, n_pp)
        return adamw(scale, grad, pre, master, exp_avg, exp_avg_sq)

    return jax.shard_map(device_step, mesh=mesh, in_specs=(table_spec, table_spec, table_spec, P("pp", "dp", None), P("pp", "dp", None, None)), out_specs=(table_spec, table_spec, table_spec, table_spec), check_vma=False)
```

```python
import functools

import jax
import jax.numpy as jnp
from jax import lax
from jax.experimental import pallas as pl
from jax.experimental.pallas import tpu as pltpu
from jax.sharding import PartitionSpec as P

LEARN_RATE = 0.003
BETA_ONE = 0.9
BETA_TWO = 0.95
ADAM_EPS = 1e-8
WEIGHT_DECAY = 0.1
CLIP_NORM = 1.0
OPT_STEP = 10

MESH_ID = pl.DeviceIdType.MESH
LOW = -1e30
VMEM = pltpu.VMEM
DMA = pltpu.SemaphoreType.DMA
F32, BF16 = jnp.float32, jnp.bfloat16
SMALL_GRANT = 21 << 19
scope = jax.named_scope


def remote(src, dst, send, recv, where):
    return pltpu.make_async_remote_copy(src_ref=src, dst_ref=dst, send_sem=send, recv_sem=recv, device_id=where, device_id_type=MESH_ID)


def in_vmem(arr):
    return pltpu.with_memory_space_constraint(arr, VMEM)


def enter(groups):
    barrier = pltpu.get_barrier_semaphore()
    for axis, peer in groups:
        pl.semaphore_signal(barrier, inc=1, device_id={axis: peer}, device_id_type=MESH_ID)
    pl.semaphore_wait(barrier, len(groups))


def ring_plan(n_one, n_two):
    items = [(1, s, 0) for s in range(n_one - 1)] + [(2, s, t) for s in range(n_one) for t in range(n_two - 1)]
    return sorted(items, key=lambda i: (i[1] + i[2], i[0], i[2]))


def grad_kernel(n_tp, n_dp, n_pp, n_chunk, lag, table_ref, acts_ref, ids_ref, sq_ref, g_ref, scale_ref, big_ref, hid_ref, dx_ref, lab_ref, look_ref, tab_ref, dl_ref, stat_ref, mid_ref, buf_p, buf_z, nb_p, nb_y, nb_z, load_s, feed_s, send_x, send_z, send_d, send_e, recv_x, recv_z, recv_d, recv_e, id_s, id_r, sp_s, sp_r, sz_s, sz_r, rs_s, rs_r, np_s, np_r, ny_s, ny_r, nz_s, nz_r, ag_s, ag_r, d_s, d_r, pre_s):
    p, z, y = lax.axis_index("pp"), lax.axis_index("tp"), lax.axis_index("dp")
    n_x = n_pp // 2
    x, c, par = p // 2, lax.rem(p, 2), lax.rem(z, 2)
    mate = 2 * x + 1 - c
    vocab = table_ref.shape[0]
    rows, tok = dl_ref.shape
    dq = g_ref.shape[3]
    up_y, down_y = lax.rem(y + 1, n_dp), lax.rem(y + n_dp - 1, n_dp)

    def first_row(d):
        return (d * n_pp + p) * rows

    n_piece, n_group = 6, 3
    wide = tok // n_piece
    per_band = min(n_piece, table_ref.shape[1] // wide)
    exp_row = 2 * tok
    part_row = exp_row + -(-n_piece // per_band) * n_dp * rows
    rel_row, one_row, com_row = (part_row + (n_dp + i) * rows for i in range(3))

    def exp_at(g, d, count=1):
        return big_ref.at[pl.ds(exp_row + (g // per_band) * n_dp * rows + d * rows, rows), pl.ds((g % per_band) * wide, count * wide)]

    def part_at(d, q, count=1):
        return big_ref.at[pl.ds(pl.multiple_of(part_row + d * rows, 8), rows), pl.ds(q * dq, count * dq)]

    def half_at(row, half):
        return big_ref.at[pl.ds(row, rows), pl.ds(2 * half * dq, 2 * dq)]

    short = vocab - (n_dp * n_pp - 1) * rows

    def table_copies(count, blocks):
        return [pltpu.make_async_copy(table_ref.at[pl.ds(pl.multiple_of(first_row(d), 8), count)], big_ref.at[pl.ds(part_row + d * rows, count)], load_s.at[1 + d]) for d in blocks]

    def each_table_copy(act):
        for cp in table_copies(rows, range(n_dp - 1)):
            act(cp)
        for cond, count in ((p < n_pp - 1, rows), (p == n_pp - 1, short)):
            @pl.when(cond)
            def _(count=count):
                for cp in table_copies(count, (n_dp - 1,)):
                    act(cp)

    each_table_copy(lambda cp: cp.start())
    hid_buf, dx_buf = big_ref.at[pl.ds(0, tok)], big_ref.at[pl.ds(tok, tok)]
    sources = ((n_pp - 1, hid_buf, hid_ref, lab_ref), (0, dx_buf, dx_ref, look_ref))
    for source, _, low, _ in sources:
        @pl.when(p == source)
        def _(low=low):
            pltpu.make_async_copy(acts_ref, low, load_s.at[0]).start()

    enter([("pp", lax.rem(p + o, n_pp)) for o in range(1, n_pp)] + [("tp", lax.rem(z + o, n_tp)) for o in range(1, n_tp)] + [("dp", lax.rem(y + o, n_dp)) for o in range(1, n_dp)])

    step_x = 1 - 2 * c
    next_p = 2 * lax.rem(x + step_x + n_x, n_x) + c
    next_z = lax.rem(z + step_x + n_tp, n_tp)
    size = tok // (4 * n_chunk)
    last = n_chunk + lag
    per_group = n_chunk // n_group
    group = tok // n_group

    def span(core, parity, k):
        return pl.ds(pl.multiple_of((4 * k + 2 * parity + core) * size, 8), size)

    class Stream:
        def __init__(self, a):
            self.a = a
            self.source, self.buf, self.low, self.ids = sources[a]
            self.is_src = p == self.source
            s_x = self.source // 2
            self.dist = lax.rem(jnp.where(c == 0, x - s_x, s_x - x) + n_x, n_x)

        def hop(self, part, send, recv, where):
            return remote(self.buf.at[part], self.buf.at[part], send, recv, where)

        def feed(self, k):
            return self.hop(span(1 - c, par, k), feed_s.at[self.a, k], recv_x.at[self.a, k], {"pp": mate})

        def ring(self, k):
            return self.hop(span(c, par, k), send_x.at[self.a, k], recv_x.at[self.a, k], {"pp": next_p})

        def plane(self, k, parity):
            return self.hop(span(c, parity, k), send_z.at[self.a, k], recv_z.at[self.a, k], {"tp": next_z})

        def across(self, k, core):
            return self.hop(span(core, par, k), send_d.at[self.a, k], recv_d.at[self.a, k], {"pp": mate})

        def again(self, k, core):
            return self.hop(span(core, 1 - par, k), send_e.at[self.a, k], recv_e.at[self.a, k], {"pp": mate})

        def id_copy(self, o):
            return remote(ids_ref, self.ids, id_s.at[self.a, o - 1], id_r.at[self.a], {"pp": lax.rem(p + o, n_pp)})

        def begin(self, with_ring):
            @pl.when(self.is_src)
            def _():
                pltpu.make_async_copy(acts_ref, self.low, load_s.at[0]).wait()
                self.ids[...] = ids_ref[...]

                @pl.loop(0, n_chunk)
                def _(k):
                    def widen(part):
                        self.buf[part, :] = self.low[part, :].astype(F32)

                    widen(span(1 - c, par, k))
                    self.feed(k).start()
                    widen(span(c, par, k))
                    if n_x > 1 and with_ring:
                        self.ring(k).start()
                    self.across(k, c).start()
                    widen(span(c, 1 - par, k))
                    self.again(k, c).start()

                for o in range(1, n_pp):
                    self.id_copy(o).start()

        def early_ring(self):
            @pl.when(mate == self.source)
            def _():
                @pl.loop(0, n_chunk)
                def _(k):
                    self.ring(k).wait_recv()
                    if n_x > 1:
                        self.ring(k).start()

        def late_ring(self, lo, hi):
            if n_x > 1:
                @pl.when(self.is_src)
                def _():
                    @pl.loop(lo, hi)
                    def _(k):
                        self.ring(k).start()

        def late_plane(self):
            @pl.when(mate == self.source)
            def _():
                @pl.loop(0, n_chunk)
                def _(k):
                    self.plane(k, par).start()

        def steps(self, lo, hi, early=False):
            @pl.when(jnp.logical_not(self.is_src))
            def _():
                @pl.loop(lo, hi)
                def _(k):
                    @pl.when(jnp.logical_and(k < n_chunk, jnp.logical_or(mate != self.source, not early)))
                    def _():
                        self.ring(k).wait_recv()
                        if n_x > 1:
                            @pl.when(self.dist < n_x - 1)
                            def _():
                                if early:
                                    @pl.when(jnp.logical_and(p == n_pp - 1, k >= 2))
                                    def _():
                                        self.ring(k - 2).wait_send()

                                self.ring(k).start()

                        self.plane(k, par).start()

                        @pl.when(mate != self.source)
                        def _():
                            self.across(k, c).start()

                    @pl.when(k >= lag)
                    def _():
                        self.plane(k - lag, 1 - par).wait_recv()

                        @pl.when(mate != self.source)
                        def _():
                            self.again(k - lag, c).start()

        def collect(self, g, parts):
            @pl.when(jnp.logical_not(self.is_src))
            def _():
                if g == 0:
                    self.id_copy(1).wait_recv()

                per_part, count = n_chunk // parts, tok // parts

                @pl.loop(g * per_part, (g + 1) * per_part)
                def _(k):
                    self.across(k, 1 - c).wait_recv()
                    self.again(k, 1 - c).wait_recv()

                tile = min(128, count)

                @pl.loop(0, count // tile)
                def _(k):
                    here = pl.ds(pl.multiple_of(g * count + k * tile, tile), tile)
                    self.low[here, :] = self.buf[here, :].astype(BF16)

        def settle(self):
            @pl.when(self.is_src)
            def _():
                for o in range(1, n_pp):
                    self.id_copy(o).wait_send()

            @pl.loop(0, n_chunk)
            def _(k):
                @pl.when(self.is_src)
                def _():
                    self.feed(k).wait_send()

                @pl.when(jnp.logical_not(self.is_src))
                def _():
                    self.plane(k, par).wait_send()

                if n_x > 1:
                    begun = n_chunk if self.a == 0 else n_chunk - 2

                    @pl.when(jnp.logical_and(self.dist < n_x - 1, jnp.logical_or(p != n_pp - 1, k >= begun)))
                    def _():
                        self.ring(k).wait_send()

                @pl.when(mate != self.source)
                def _():
                    self.across(k, c).wait_send()
                    self.again(k, c).wait_send()

    hid_in, dx_in = Stream(0), Stream(1)
    def logits(g):
        cols = pl.ds(g * wide, wide)
        h = hid_ref[cols, :]
        top = jnp.full((1, wide), LOW, F32)
        for d in range(n_dp):
            lg = lax.dot_general(tab_ref[d], h, (((1,), (1,)), ((), ())), preferred_element_type=F32)
            if d == n_dp - 1 and short < rows:
                ok = first_row(d) + lax.broadcasted_iota(jnp.int32, (rows, wide), 0) < vocab
                lg = jnp.where(ok, lg, LOW)
            exp_at(g, d)[...] = lg
            top = jnp.maximum(top, jnp.max(lg, axis=0, keepdims=True))
        tot = jnp.zeros((1, wide), F32)
        for d in range(n_dp):
            e = jnp.exp(exp_at(g, d)[...] - top)
            exp_at(g, d)[...] = e
            tot = tot + jnp.sum(e, axis=0, keepdims=True)
        stat_ref[0:1, cols] = top
        stat_ref[1:2, cols] = tot

    with scope("begin"):
        hid_in.begin(True)
        dx_in.begin(False)
        each_table_copy(lambda cp: cp.wait())
        for d in range(n_dp):
            tab_ref[d] = part_at(d, 0, 4)[...].astype(BF16)
    with scope("early"):
        dx_in.early_ring()
    dist = dx_in.dist

    def clip(value):
        return jnp.clip(jnp.where(p == 1, 0, value), 0, last)

    near = jnp.where(jnp.logical_or(jnp.logical_and(c == 0, dist == 1), jnp.logical_and(c == 1, dist >= 2)), 1, 0)
    near = jnp.where(jnp.logical_or(p == n_pp - 1, hid_in.dist == n_x - 1), 0, near)
    at_zero = near * jnp.where(c == 0, 2, jnp.maximum(12 - 3 * dist, 0))
    at_zero = jnp.minimum(at_zero, last - (n_piece - 2))
    at_half = at_zero + (n_piece - 2) * near
    at_one = jnp.where(p == n_pp - 1, last, jnp.where(c == 0, 11 - 3 * dist, 18 - 3 * dist))
    at_two = jnp.where(p == n_pp - 1, last, jnp.where(c == 0, at_one + 2, at_one + 3))
    at_one = jnp.maximum(clip(at_one), at_half)
    at_two = jnp.maximum(clip(at_two), at_one)
    at_three = jnp.maximum(jnp.minimum(at_two + jnp.where(p == 1, 0, n_dp), last), min(last, per_group + lag))
    at_four = jnp.maximum(at_three, min(last, max(n_chunk, 2 * per_group + lag)))

    def prepare(g):
        with scope(f"hid_collect{g}"):
            hid_in.collect(g, n_piece)
        with scope(f"logits{g}"):
            logits(g)

    at_end = jnp.logical_and(hid_in.dist == n_x - 1, jnp.logical_not(hid_in.is_src))
    pair = n_chunk // n_piece

    @pl.when(at_end)
    def _():
        lo = 0
        for g in range(n_piece - 2):
            hi = min(last, (g + 1) * pair + lag + 1)
            with scope(f"hid{g}"):
                hid_in.steps(lo, hi)
            prepare(g)
            lo = hi
        with scope("hid_end"):
            hid_in.steps(lo, last)
        dx_in.late_ring(0, n_chunk)
        dx_in.late_plane()

    @pl.when(jnp.logical_not(at_end))
    def _():
        with scope("hid_end"):
            hid_in.steps(0, n_chunk)
            dx_in.late_ring(0, 2)
            hid_in.steps(n_chunk, last)
            dx_in.late_ring(2, n_chunk)
            dx_in.late_plane()
        with scope("dx0"):
            dx_in.steps(0, at_zero, True)
        for g in range(n_piece - 2):
            prepare(g)
            dx_in.steps(at_zero + g * near, at_zero + (g + 1) * near, True)

    for g in range(n_piece - 2, n_piece):
        prepare(g)

    def swap(src, buf, send, recv, axis, me, n):
        return [remote(src, buf.at[o - 1], send.at[o - 1], recv.at[o - 1], {axis: lax.rem(me + o, n)}) for o in range(1, n)]

    def merge(src, buf, n):
        top = src[0:1, :]
        for o in range(1, n):
            top = jnp.maximum(top, buf[o - 1, 0:1, :])
        tot = src[1:2, :] * jnp.exp(src[0:1, :] - top)
        for o in range(1, n):
            tot = tot + buf[o - 1, 1:2, :] * jnp.exp(buf[o - 1, 0:1, :] - top)
        return top, tot

    def local_ids(ref, start, count):
        ids = ref[:, start:start + count] - z * vocab
        return jnp.where(ids < vocab, ids, -1)

    def row_ids(d, count):
        return first_row(d) + lax.broadcasted_iota(jnp.int32, (rows, count), 0)

    stage = swap(stat_ref, buf_p, sp_s, sp_r, "pp", p, n_pp)
    for cp in stage:
        cp.start()
    with scope("dx1"):
        if n_x > 1:
            @pl.when(p == n_pp - 1)
            def _():
                @pl.loop(0, n_chunk)
                def _(k):
                    hid_in.ring(k).wait_send()

        dx_in.steps(at_half, at_one, True)
    with scope("stat1"):
        for cp in stage:
            cp.wait()
    top, tot = merge(stat_ref, buf_p, n_pp)
    mid_ref[0:1, :] = top
    mid_ref[1:2, :] = tot
    stage = swap(mid_ref, buf_z, sz_s, sz_r, "tp", z, n_tp)
    for cp in stage:
        cp.start()
    with scope("dx2"):
        dx_in.steps(at_one, at_two, True)
    with scope("stat2"):
        for cp in stage:
            cp.wait()
    top, tot = merge(mid_ref, buf_z, n_tp)
    mid_ref[0:1, :] = jnp.exp(stat_ref[0:1, :] - top) / (tot * tok)

    def head(d):
        for g in range(0, n_piece, per_band):
            count = min(per_band, n_piece - g)
            cols = pl.ds(g * wide, count * wide)
            prob = big_ref[pl.ds(pl.multiple_of(exp_row + (g // per_band) * n_dp * rows + d * rows, 8), rows), pl.ds(0, count * wide)] * mid_ref[0:1, cols]
            hit = local_ids(lab_ref, g * wide, count * wide) == row_ids(d, count * wide)
            dl_ref[:, cols] = jnp.where(hit, prob - 1.0 / tok, prob).astype(BF16)
        for q in range(4):
            part_at(d, q)[...] = jnp.dot(dl_ref[...], hid_ref[:, q * dq:(q + 1) * dq], preferred_element_type=F32)

    def lookup(g):
        def add(d):
            hot = (local_ids(look_ref, g * group, group) == row_ids(d, group)).astype(BF16)
            dl_ref[:, 0:group] = hot
            for q in range(4):
                part_at(d, q)[...] += jnp.dot(dl_ref[:, 0:group], dx_ref[g * group:(g + 1) * group, q * dq:(q + 1) * dq], preferred_element_type=F32)
        return add

    with scope("head"):
        @pl.loop(0, n_dp)
        def _(d):
            head(d)
            dx_in.steps(jnp.minimum(at_two + d, at_three), jnp.minimum(at_two + d + 1, at_three), True)

        dx_in.steps(jnp.minimum(at_two + n_dp, at_three), at_three, True)
    with scope("dx_group0"):
        dx_in.collect(0, n_group)
        pl.loop(0, n_dp)(lookup(0))
    with scope("dx4"):
        dx_in.steps(at_three, at_four, True)
    with scope("dx_group1"):
        dx_in.collect(1, n_group)
        pl.loop(0, n_dp)(lookup(1))
    with scope("dx5"):
        dx_in.steps(at_four, last, True)
    with scope("dx_group2"):
        dx_in.collect(2, n_group)

    far = lax.rem(y + 2, n_dp)

    def reduce_copy(i, d, half, row, where):
        return remote(part_at(d, 2 * half, 2), half_at(row, half), rs_s.at[i], rs_r.at[i], {"dp": where})

    rel_a = reduce_copy(0, far, 0, rel_row, up_y)
    rel_b = reduce_copy(1, far, 1, rel_row, down_y)
    one_b = reduce_copy(2, up_y, 1, one_row, up_y)
    one_a = reduce_copy(3, down_y, 0, one_row, down_y)
    com_a = reduce_copy(4, up_y, 0, com_row, up_y)
    com_b = reduce_copy(5, down_y, 1, com_row, down_y)
    add = lookup(n_group - 1)
    add(far)
    rel_a.start()
    rel_b.start()
    add(up_y)
    one_b.start()
    add(down_y)
    one_a.start()
    add(y)
    hid_in.settle()
    dx_in.settle()

    def moments(lo, hi, sem):
        return pltpu.make_async_copy(sq_ref.at[pl.ds(lo, hi - lo)], big_ref.at[pl.ds(lo, hi - lo)], pre_s.at[sem])

    loads = [moments(0, min(part_row, vocab), 0)]
    loads[0].start()
    with scope("relay"):
        rel_a.wait_recv()
    part_at(up_y, 0, 2)[...] += half_at(rel_row, 0)[...]
    com_a.start()
    rel_b.wait_recv()
    part_at(down_y, 2, 2)[...] += half_at(rel_row, 1)[...]
    com_b.start()
    own = y * n_pp + p
    square = jnp.zeros((8, 128), F32)
    with scope("one"):
        one_a.wait_recv()
        one_b.wait_recv()
    for half, cp in ((0, com_a), (1, com_b)):
        with scope("com"):
            cp.wait_recv()
        for q in range(2):
            cols = pl.ds((2 * half + q) * dq, dq)
            total = (part_at(y, 2 * half + q)[...] + big_ref[pl.ds(com_row, rows), cols] + big_ref[pl.ds(one_row, rows), cols]) * (1.0 / n_dp)
            g_ref[own, 2 * half + q] = total
            lanes = jnp.sum((total * total).reshape(rows // 8, 8, dq), axis=0)
            for i in range(0, dq, 128):
                square = square + lanes[:, i:i + 128]

    def block(xx, yy):
        return lax.rem(yy + 2 * n_dp, n_dp) * n_pp + 2 * lax.rem(xx + 2 * n_x, n_x) + c

    colours = []
    for q, (axes, sign) in enumerate((("xy", 1), ("xy", -1), ("yx", 1), ("yx", -1))):
        sizes = (n_x, n_dp) if axes == "xy" else (n_dp, n_x)
        to_x = {"pp": 2 * lax.rem(x + sign + n_x, n_x) + c}
        to_y = {"dp": lax.rem(y + sign + n_dp, n_dp)}
        dest = (to_x, to_y) if axes == "xy" else (to_y, to_x)
        colours.append((q, axes, sign, sizes, dest, ring_plan(*sizes)))

    def holder(axes, sign, s, t):
        return block(x - sign * s, y - sign * t) if axes == "xy" else block(x - sign * t, y - sign * s)

    def message(colour, item, coming):
        q, axes, sign, _, dest, plan = colour
        phase, s, t = item
        at = plan.index(item)
        s_at, t_at = (s + coming, t) if phase == 1 else (s, t + coming)
        b = holder(axes, sign, s_at, t_at)
        return remote(g_ref.at[b, q], g_ref.at[b, q], ag_s.at[q, at], ag_r.at[q, at], dest[phase - 1])

    def mate_copy(q, slot, b):
        return remote(g_ref.at[b, q], g_ref.at[b, q], d_s.at[q, slot], d_r.at[q, slot], {"pp": mate})

    sends = []

    def push(cp):
        cp.start()
        sends.append(cp)

    for colour in colours:
        if colour[3][0] > 1:
            push(message(colour, (1, 0, 0), 0))
    for colour in colours:
        if colour[3][1] > 1:
            push(message(colour, (2, 0, 0), 0))

    def norm_swap(value, buf, send, recv, axis, me, n):
        buf[me] = value
        return [remote(buf.at[me], buf.at[me], send.at[o - 1], recv.at[o - 1], {axis: lax.rem(me + o, n)}) for o in range(1, n)], [
            remote(buf.at[lax.rem(me + n - o, n)], buf.at[lax.rem(me + n - o, n)], send.at[o - 1], recv.at[o - 1], {axis: lax.rem(me + o, n)}) for o in range(1, n)]

    norm_out, norm_in = norm_swap(square, nb_p, np_s, np_r, "pp", p, n_pp)
    for cp in norm_out:
        push(cp)
    for q in range(4):
        push(mate_copy(q, 0, own))

    for cp in (rel_a, rel_b, one_a, one_b, com_a, com_b):
        cp.wait_send()
    if part_row < vocab:
        loads.append(moments(part_row, vocab, 1))
        loads[1].start()

    steps = n_x * n_dp - 1
    for i in range(steps):
        for colour in colours:
            q, axes, sign, sizes, dest, plan = colour
            phase, s, t = plan[i]
            message(colour, plan[i], 1).wait_recv()
            if phase == 1:
                if s + 1 < sizes[0] - 1:
                    push(message(colour, (1, s + 1, 0), 0))
                if sizes[1] > 1:
                    push(message(colour, (2, s + 1, 0), 0))
                push(mate_copy(q, i + 1, holder(axes, sign, s + 1, 0)))
            else:
                if t + 1 < sizes[1] - 1:
                    push(message(colour, (2, s, t + 1), 0))
                push(mate_copy(q, i + 1, holder(axes, sign, s, t + 1)))
        if i == 0:
            for cp in norm_in:
                cp.wait_recv()
            total = nb_p[0]
            for o in range(1, n_pp):
                total = total + nb_p[o]
            norm_out, norm_in = norm_swap(total, nb_y, ny_s, ny_r, "dp", y, n_dp)
            for cp in norm_out:
                push(cp)
        if i == 1:
            for cp in norm_in:
                cp.wait_recv()
            total = nb_y[0]
            for o in range(1, n_dp):
                total = total + nb_y[o]
            norm_out, norm_in = norm_swap(total, nb_z, nz_s, nz_r, "tp", z, n_tp)
            for cp in norm_out:
                push(cp)
        if i == 2:
            for cp in norm_in:
                cp.wait_recv()
            total = nb_z[0]
            for o in range(1, n_tp):
                total = total + nb_z[o]
            norm = jnp.sqrt(jnp.sum(total, axis=(0, 1), keepdims=True))
            scale_ref[...] = jnp.broadcast_to(CLIP_NORM / jnp.maximum(norm, CLIP_NORM), (8, 128))

    for q, axes, sign, sizes, dest, plan in colours:
        for i in range(steps + 1):
            if i == 0:
                b = own
            else:
                phase, s, t = plan[i - 1]
                b = holder(axes, sign, s + 1, 0) if phase == 1 else holder(axes, sign, s, t + 1)
            mate_copy(q, i, b + 1 - 2 * c).wait_recv()
    for cp in sends:
        cp.wait_send()
    for cp in loads:
        cp.wait()


def plane_gradient(master, acts, ids, exp_avg_sq, n_tp, n_dp, n_pp):
    vocab, dim = master.shape
    tok = acts.shape[0]
    rows = -(-vocab // (n_pp * n_dp))
    rows = -(-rows // 8) * 8
    dq = dim // 4
    n_chunk = 12 if tok % (4 * 12 * 8) == 0 else 6
    lag = 2
    steps = (n_pp // 2) * n_dp
    per_band = min(6, dim // (tok // 6))
    big = max(n_dp * n_pp * rows, 2 * tok + (-(-6 // per_band) * n_dp + n_dp + 3) * rows)
    full = pl.BlockSpec(memory_space=VMEM)
    any_space = pl.BlockSpec(memory_space=pl.ANY)
    chunk = DMA((2, n_chunk))
    return pl.pallas_call(
        functools.partial(grad_kernel, n_tp, n_dp, n_pp, n_chunk, lag),
        out_shape=(VMEM((n_dp * n_pp, 4, rows, dq), F32), jax.ShapeDtypeStruct((8, 128), F32), VMEM((big, dim), F32)),
        in_specs=[any_space, any_space, full, any_space],
        out_specs=(full, full, full),
        scratch_shapes=[
            VMEM((tok, dim), BF16), VMEM((tok, dim), BF16),
            VMEM((1, tok), jnp.int32), VMEM((1, tok), jnp.int32), VMEM((n_dp, rows, dim), BF16), VMEM((rows, tok), BF16),
            VMEM((2, tok), F32), VMEM((2, tok), F32), VMEM((n_pp - 1, 2, tok), F32), VMEM((n_tp - 1, 2, tok), F32),
            VMEM((n_pp, 8, 128), F32), VMEM((n_dp, 8, 128), F32), VMEM((n_tp, 8, 128), F32),
            DMA((1 + n_dp,)), *[chunk] * 9, DMA((2, n_pp - 1)), DMA((2,)),
            DMA((n_pp - 1,)), DMA((n_pp - 1,)), DMA((n_tp - 1,)), DMA((n_tp - 1,)), DMA((6,)), DMA((6,)),
            DMA((n_pp - 1,)), DMA((n_pp - 1,)), DMA((n_dp - 1,)), DMA((n_dp - 1,)), DMA((n_tp - 1,)), DMA((n_tp - 1,)),
            DMA((4, steps)), DMA((4, steps)), DMA((4, steps)), DMA((4, steps)), DMA((2,)),
        ],
        compiler_params=pltpu.CompilerParams(collective_id=0, has_side_effects=True, vmem_limit_bytes=SMALL_GRANT),
        name="plane_gradient",
    )(master, acts, ids, exp_avg_sq)


def adamw_kernel(n_slot, ahead, tile, scale_ref, g_ref, v_ref, e_hbm, m_hbm, ne_hbm, nm_hbm, nv_hbm, nb_hbm, e_buf, m_buf, v_buf, b_buf, in_s, out_s):
    rows, dq = g_ref.shape[2:]
    per_block, per_tile = rows // 8, tile // 8
    n_tile = e_hbm.shape[0] // tile
    scale = scale_ref[0:1, 0:1]

    def span(i):
        return pl.ds(pl.multiple_of(i * tile, 8), tile)

    def loads(i):
        slot = lax.rem(i, n_slot)
        return [pltpu.make_async_copy(hbm.at[span(i)], buf.at[slot], in_s.at[a, slot]) for a, (hbm, buf) in enumerate(((e_hbm, e_buf), (m_hbm, m_buf)))]

    def stores(i):
        slot = lax.rem(i, n_slot)
        return [pltpu.make_async_copy(buf.at[slot], hbm.at[span(i)], out_s.at[a, slot]) for a, (buf, hbm) in enumerate(((e_buf, ne_hbm), (m_buf, nm_hbm), (v_buf, nv_hbm), (b_buf, nb_hbm)))]

    for i in range(min(ahead, n_tile)):
        for cp in loads(i):
            cp.start()

    @pl.loop(0, n_tile)
    def _(i):
        slot = lax.rem(i, n_slot)

        @pl.when(i + ahead < n_tile)
        def _():
            @pl.when(i + ahead >= n_slot)
            def _():
                for cp in stores(i + ahead - n_slot):
                    cp.wait()

            for cp in loads(i + ahead):
                cp.start()

        for cp in loads(i):
            cp.wait()
        for r in range(per_tile):
            group = i * per_tile + r
            blk = group // per_block
            inside = pl.ds(pl.multiple_of((group - blk * per_block) * 8, 8), 8)
            at = pl.ds(8 * r, 8)
            for q in range(4):
                cols = pl.ds(q * dq, dq)
                g = g_ref[blk, q, inside, :] * scale
                e = e_buf[slot, at, cols]
                m = BETA_ONE * m_buf[slot, at, cols] + (1.0 - BETA_ONE) * g
                v = BETA_TWO * v_ref[pl.ds(pl.multiple_of(group * 8, 8), 8), cols] + (1.0 - BETA_TWO) * g * g
                step = (m * (1.0 / (1.0 - BETA_ONE ** OPT_STEP))) / (jnp.sqrt(v * (1.0 / (1.0 - BETA_TWO ** OPT_STEP))) + ADAM_EPS)
                ne = e - LEARN_RATE * (step + WEIGHT_DECAY * e)
                e_buf[slot, at, cols] = ne
                m_buf[slot, at, cols] = m
                v_buf[slot, at, cols] = v
                b_buf[slot, at, cols] = ne.astype(BF16)
        for cp in stores(i):
            cp.start()

    for i in range(max(0, n_tile - n_slot), n_tile):
        for cp in stores(i):
            cp.wait()


def adamw(scale, grad, second, master, exp_avg):
    vocab, dim = master.shape
    tile = next(t for t in (48, 32, 16, 8) if vocab % t == 0)
    n_slot = 14
    full = pl.BlockSpec(memory_space=VMEM)
    any_space = pl.BlockSpec(memory_space=pl.ANY)
    f32 = jax.ShapeDtypeStruct((vocab, dim), F32)
    count = vocab * dim
    ring = VMEM((n_slot, tile, dim), F32)
    return pl.pallas_call(
        functools.partial(adamw_kernel, n_slot, 8, tile),
        out_shape=(f32, f32, f32, jax.ShapeDtypeStruct((vocab, dim), BF16)),
        in_specs=[full, full, full, any_space, any_space],
        out_specs=(any_space,) * 4,
        scratch_shapes=[ring, ring, ring, VMEM((n_slot, tile, dim), BF16), DMA((2, n_slot)), DMA((4, n_slot))],
        cost_estimate=pl.CostEstimate(flops=20 * count, bytes_accessed=22 * count, transcendentals=2 * count),
        compiler_params=pltpu.CompilerParams(vmem_limit_bytes=SMALL_GRANT),
        name="adamw",
    )(scale, in_vmem(grad), in_vmem(second), master, exp_avg)


def solution(mesh):
    n_pp, n_dp, n_tp = mesh.shape["pp"], mesh.shape["dp"], mesh.shape["tp"]
    table_spec = P("tp", None)

    def device_step(master, exp_avg, exp_avg_sq, stage_ids, stage_acts):
        vocab, dim = master.shape
        tok = stage_ids.shape[1] * stage_ids.shape[2]
        acts = stage_acts.reshape(tok, dim)
        grad, scale, second = plane_gradient(master, acts, stage_ids.reshape(1, tok), exp_avg_sq, n_tp, n_dp, n_pp)
        return adamw(scale, grad, second, master, exp_avg)

    return jax.shard_map(device_step, mesh=mesh, in_specs=(table_spec, table_spec, table_spec, P("pp", "dp", None), P("pp", "dp", None, None)), out_specs=(table_spec, table_spec, table_spec, table_spec), check_vma=False)
```

```python
import functools

import jax
import jax.numpy as jnp
from jax import lax
from jax.experimental import pallas as pl
from jax.experimental.pallas import tpu as pltpu
from jax.sharding import PartitionSpec as P

LEARN_RATE = 0.003
BETA_ONE = 0.9
BETA_TWO = 0.95
ADAM_EPS = 1e-8
WEIGHT_DECAY = 0.1
CLIP_NORM = 1.0
OPT_STEP = 10

MESH_ID = pl.DeviceIdType.MESH
LOW = -1e30
VMEM = pltpu.VMEM
DMA = pltpu.SemaphoreType.DMA
F32, BF16 = jnp.float32, jnp.bfloat16
SMALL_GRANT = 21 << 19
scope = jax.named_scope


def remote(src, dst, send, recv, where):
    return pltpu.make_async_remote_copy(src_ref=src, dst_ref=dst, send_sem=send, recv_sem=recv, device_id=where, device_id_type=MESH_ID)


def in_vmem(arr):
    return pltpu.with_memory_space_constraint(arr, VMEM)


def enter(groups):
    barrier = pltpu.get_barrier_semaphore()
    for axis, peer in groups:
        pl.semaphore_signal(barrier, inc=1, device_id={axis: peer}, device_id_type=MESH_ID)
    pl.semaphore_wait(barrier, len(groups))


def ring_plan(n_one, n_two):
    items = [(1, s, 0) for s in range(n_one - 1)] + [(2, s, t) for s in range(n_one) for t in range(n_two - 1)]
    return sorted(items, key=lambda i: (i[1] + i[2], i[0], i[2]))


def grad_kernel(n_tp, n_dp, n_pp, n_chunk, lag, table_ref, acts_ref, ids_ref, sq_ref, g_ref, scale_ref, big_ref, hid_ref, dx_ref, lab_ref, look_ref, tab_ref, dl_ref, stat_ref, mid_ref, buf_p, buf_z, nb_p, nb_y, nb_z, load_s, feed_s, send_x, send_z, send_d, send_e, recv_x, recv_z, recv_d, recv_e, id_s, id_r, sp_s, sp_r, sz_s, sz_r, rs_s, rs_r, np_s, np_r, ny_s, ny_r, nz_s, nz_r, ag_s, ag_r, d_s, d_r, pre_s):
    p, z, y = lax.axis_index("pp"), lax.axis_index("tp"), lax.axis_index("dp")
    n_x = n_pp // 2
    x, c, par = p // 2, lax.rem(p, 2), lax.rem(z, 2)
    mate = 2 * x + 1 - c
    vocab = table_ref.shape[0]
    rows, tok = dl_ref.shape
    dq = g_ref.shape[3]
    up_y, down_y = lax.rem(y + 1, n_dp), lax.rem(y + n_dp - 1, n_dp)

    def first_row(d):
        return (d * n_pp + p) * rows

    n_piece, n_group = 6, 3
    wide = tok // n_piece
    per_band = min(n_piece, table_ref.shape[1] // wide)
    exp_row = 2 * tok
    part_row = exp_row + -(-n_piece // per_band) * n_dp * rows
    rel_row, one_row, com_row = (part_row + (n_dp + i) * rows for i in range(3))

    def exp_at(g, d, count=1):
        return big_ref.at[pl.ds(exp_row + (g // per_band) * n_dp * rows + d * rows, rows), pl.ds((g % per_band) * wide, count * wide)]

    def part_at(d, q, count=1):
        return big_ref.at[pl.ds(pl.multiple_of(part_row + d * rows, 8), rows), pl.ds(q * dq, count * dq)]

    def half_at(row, half):
        return big_ref.at[pl.ds(row, rows), pl.ds(2 * half * dq, 2 * dq)]

    short = vocab - (n_dp * n_pp - 1) * rows

    def table_copies(count, blocks):
        return [pltpu.make_async_copy(table_ref.at[pl.ds(pl.multiple_of(first_row(d), 8), count)], big_ref.at[pl.ds(part_row + d * rows, count)], load_s.at[1 + d]) for d in blocks]

    def each_table_copy(act):
        for cp in table_copies(rows, range(n_dp - 1)):
            act(cp)
        for cond, count in ((p < n_pp - 1, rows), (p == n_pp - 1, short)):
            @pl.when(cond)
            def _(count=count):
                for cp in table_copies(count, (n_dp - 1,)):
                    act(cp)

    each_table_copy(lambda cp: cp.start())
    hid_buf, dx_buf = big_ref.at[pl.ds(0, tok)], big_ref.at[pl.ds(tok, tok)]
    sources = ((n_pp - 1, hid_buf, hid_ref, lab_ref), (0, dx_buf, dx_ref, look_ref))
    for source, _, low, _ in sources:
        @pl.when(p == source)
        def _(low=low):
            pltpu.make_async_copy(acts_ref, low, load_s.at[0]).start()

    enter([("pp", lax.rem(p + o, n_pp)) for o in range(1, n_pp)] + [("tp", lax.rem(z + o, n_tp)) for o in range(1, n_tp)] + [("dp", lax.rem(y + o, n_dp)) for o in range(1, n_dp)])

    step_x = 1 - 2 * c
    next_p = 2 * lax.rem(x + step_x + n_x, n_x) + c
    next_z = lax.rem(z + step_x + n_tp, n_tp)
    size = tok // (4 * n_chunk)
    last = n_chunk + lag
    per_group = n_chunk // n_group
    group = tok // n_group

    def span(core, parity, k):
        return pl.ds(pl.multiple_of((4 * k + 2 * parity + core) * size, 8), size)

    class Stream:
        def __init__(self, a):
            self.a = a
            self.source, self.buf, self.low, self.ids = sources[a]
            self.is_src = p == self.source
            s_x = self.source // 2
            self.dist = lax.rem(jnp.where(c == 0, x - s_x, s_x - x) + n_x, n_x)
            self.cut = a == 1 and n_x > 2
            ends = jnp.where(c == 0, n_x - 2, n_x - 1) if self.cut else n_x - 1
            self.passes = self.dist < ends

        def hop(self, part, send, recv, where):
            return remote(self.buf.at[part], self.buf.at[part], send, recv, where)

        def feed(self, k):
            return self.hop(span(1 - c, par, k), feed_s.at[self.a, k], recv_x.at[self.a, k], {"pp": mate})

        def ring(self, k):
            return self.hop(span(c, par, k), send_x.at[self.a, k], recv_x.at[self.a, k], {"pp": next_p})

        def direct(self, k):
            return self.hop(span(c, par, k), send_z.at[self.a, k], recv_x.at[self.a, k], {"pp": lax.rem(p + n_pp - 2, n_pp)})

        def plane(self, k, parity):
            return self.hop(span(c, parity, k), send_z.at[self.a, k], recv_z.at[self.a, k], {"tp": next_z})

        def across(self, k, core):
            return self.hop(span(core, par, k), send_d.at[self.a, k], recv_d.at[self.a, k], {"pp": mate})

        def again(self, k, core):
            return self.hop(span(core, 1 - par, k), send_e.at[self.a, k], recv_e.at[self.a, k], {"pp": mate})

        def id_copy(self, o):
            return remote(ids_ref, self.ids, id_s.at[self.a, o - 1], id_r.at[self.a], {"pp": lax.rem(p + o, n_pp)})

        def begin(self, with_ring):
            @pl.when(self.is_src)
            def _():
                pltpu.make_async_copy(acts_ref, self.low, load_s.at[0]).wait()
                self.ids[...] = ids_ref[...]

                @pl.loop(0, n_chunk)
                def _(k):
                    def widen(part):
                        self.buf[part, :] = self.low[part, :].astype(F32)

                    widen(span(1 - c, par, k))
                    self.feed(k).start()
                    widen(span(c, par, k))
                    if n_x > 1 and with_ring:
                        self.ring(k).start()
                    self.across(k, c).start()
                    widen(span(c, 1 - par, k))
                    self.again(k, c).start()

                for o in range(1, n_pp):
                    self.id_copy(o).start()

        def early_ring(self):
            @pl.when(mate == self.source)
            def _():
                @pl.loop(0, n_chunk)
                def _(k):
                    self.ring(k).wait_recv()
                    if n_x > 1:
                        self.ring(k).start()

        def late_ring(self, lo, hi):
            if n_x > 1:
                @pl.when(self.is_src)
                def _():
                    @pl.loop(lo, hi)
                    def _(k):
                        self.ring(k).start()
                        if self.cut:
                            self.direct(k).start()

        def late_plane(self):
            @pl.when(mate == self.source)
            def _():
                @pl.loop(0, n_chunk)
                def _(k):
                    self.plane(k, par).start()

        def steps(self, lo, hi, early=False):
            @pl.when(jnp.logical_not(self.is_src))
            def _():
                @pl.loop(lo, hi)
                def _(k):
                    @pl.when(jnp.logical_and(k < n_chunk, jnp.logical_or(mate != self.source, not early)))
                    def _():
                        self.ring(k).wait_recv()
                        if n_x > 1:
                            @pl.when(self.passes)
                            def _():
                                if early:
                                    @pl.when(jnp.logical_and(p == n_pp - 1, k >= 2))
                                    def _():
                                        self.ring(k - 2).wait_send()

                                self.ring(k).start()

                        self.plane(k, par).start()

                        @pl.when(mate != self.source)
                        def _():
                            self.across(k, c).start()

                    @pl.when(k >= lag)
                    def _():
                        self.plane(k - lag, 1 - par).wait_recv()

                        @pl.when(mate != self.source)
                        def _():
                            self.again(k - lag, c).start()

        def collect(self, g, parts):
            @pl.when(jnp.logical_not(self.is_src))
            def _():
                if g == 0:
                    self.id_copy(1).wait_recv()

                per_part, count = n_chunk // parts, tok // parts

                @pl.loop(g * per_part, (g + 1) * per_part)
                def _(k):
                    self.across(k, 1 - c).wait_recv()
                    self.again(k, 1 - c).wait_recv()

                tile = min(128, count)

                @pl.loop(0, count // tile)
                def _(k):
                    here = pl.ds(pl.multiple_of(g * count + k * tile, tile), tile)
                    self.low[here, :] = self.buf[here, :].astype(BF16)

        def settle(self):
            @pl.when(self.is_src)
            def _():
                for o in range(1, n_pp):
                    self.id_copy(o).wait_send()

            @pl.loop(0, n_chunk)
            def _(k):
                @pl.when(self.is_src)
                def _():
                    self.feed(k).wait_send()
                    if self.cut:
                        self.direct(k).wait_send()

                @pl.when(jnp.logical_not(self.is_src))
                def _():
                    self.plane(k, par).wait_send()

                if n_x > 1:
                    begun = n_chunk if self.a == 0 else n_chunk - 2

                    @pl.when(jnp.logical_and(self.passes, jnp.logical_or(p != n_pp - 1, k >= begun)))
                    def _():
                        self.ring(k).wait_send()

                @pl.when(mate != self.source)
                def _():
                    self.across(k, c).wait_send()
                    self.again(k, c).wait_send()

    hid_in, dx_in = Stream(0), Stream(1)
    def logits(g):
        cols = pl.ds(g * wide, wide)
        h = hid_ref[cols, :]
        top = jnp.full((1, wide), LOW, F32)
        for d in range(n_dp):
            lg = lax.dot_general(tab_ref[d], h, (((1,), (1,)), ((), ())), preferred_element_type=F32)
            if d == n_dp - 1 and short < rows:
                ok = first_row(d) + lax.broadcasted_iota(jnp.int32, (rows, wide), 0) < vocab
                lg = jnp.where(ok, lg, LOW)
            exp_at(g, d)[...] = lg
            top = jnp.maximum(top, jnp.max(lg, axis=0, keepdims=True))
        tot = jnp.zeros((1, wide), F32)
        for d in range(n_dp):
            e = jnp.exp(exp_at(g, d)[...] - top)
            exp_at(g, d)[...] = e
            tot = tot + jnp.sum(e, axis=0, keepdims=True)
        stat_ref[0:1, cols] = top
        stat_ref[1:2, cols] = tot

    with scope("begin"):
        hid_in.begin(True)
        dx_in.begin(False)
        each_table_copy(lambda cp: cp.wait())
        for d in range(n_dp):
            tab_ref[d] = part_at(d, 0, 4)[...].astype(BF16)
    with scope("early"):
        dx_in.early_ring()
    dist = jnp.where(jnp.logical_and(c == 0, dx_in.dist == n_x - 1), 1, dx_in.dist)

    def clip(value):
        return jnp.clip(jnp.where(p == 1, 0, value), 0, last)

    near = jnp.where(jnp.logical_or(jnp.logical_and(c == 0, dx_in.dist == 1), jnp.logical_and(c == 1, dist >= 2)), 1, 0)
    near = jnp.where(jnp.logical_or(p == n_pp - 1, hid_in.dist == n_x - 1), 0, near)
    at_zero = near * jnp.where(c == 0, 2, jnp.maximum(12 - 3 * dist, 0))
    at_zero = jnp.minimum(at_zero, last - (n_piece - 2))
    at_half = at_zero + (n_piece - 2) * near
    at_one = jnp.where(p == n_pp - 1, last, jnp.where(c == 0, 11 - 3 * dist, 18 - 3 * dist))
    at_two = jnp.where(p == n_pp - 1, last, jnp.where(c == 0, at_one + 2, at_one + 3))
    at_one = jnp.maximum(clip(at_one), at_half)
    at_two = jnp.maximum(clip(at_two), at_one)
    at_three = jnp.maximum(jnp.minimum(at_two + jnp.where(p == 1, 0, n_dp), last), min(last, per_group + lag))
    at_four = jnp.maximum(at_three, min(last, max(n_chunk, 2 * per_group + lag)))

    def prepare(g):
        with scope(f"hid_collect{g}"):
            hid_in.collect(g, n_piece)
        with scope(f"logits{g}"):
            logits(g)

    at_end = jnp.logical_and(hid_in.dist == n_x - 1, jnp.logical_not(hid_in.is_src))
    pair = n_chunk // n_piece

    @pl.when(at_end)
    def _():
        lo = 0
        for g in range(n_piece - 2):
            hi = min(last, (g + 1) * pair + lag + 1)
            with scope(f"hid{g}"):
                hid_in.steps(lo, hi)
            prepare(g)
            lo = hi
        with scope("hid_end"):
            hid_in.steps(lo, last)
        dx_in.late_ring(0, n_chunk)
        dx_in.late_plane()

    @pl.when(jnp.logical_not(at_end))
    def _():
        with scope("hid_end"):
            hid_in.steps(0, n_chunk)
            dx_in.late_ring(0, 2)
            hid_in.steps(n_chunk, last)
            dx_in.late_ring(2, n_chunk)
            dx_in.late_plane()
        with scope("dx0"):
            dx_in.steps(0, at_zero, True)
        for g in range(n_piece - 2):
            prepare(g)
            dx_in.steps(at_zero + g * near, at_zero + (g + 1) * near, True)

    for g in range(n_piece - 2, n_piece):
        prepare(g)

    def swap(src, buf, send, recv, axis, me, n):
        return [remote(src, buf.at[o - 1], send.at[o - 1], recv.at[o - 1], {axis: lax.rem(me + o, n)}) for o in range(1, n)]

    def merge(src, buf, n):
        top = src[0:1, :]
        for o in range(1, n):
            top = jnp.maximum(top, buf[o - 1, 0:1, :])
        tot = src[1:2, :] * jnp.exp(src[0:1, :] - top)
        for o in range(1, n):
            tot = tot + buf[o - 1, 1:2, :] * jnp.exp(buf[o - 1, 0:1, :] - top)
        return top, tot

    def local_ids(ref, start, count):
        ids = ref[:, start:start + count] - z * vocab
        return jnp.where(ids < vocab, ids, -1)

    def row_ids(d, count):
        return first_row(d) + lax.broadcasted_iota(jnp.int32, (rows, count), 0)

    stage = swap(stat_ref, buf_p, sp_s, sp_r, "pp", p, n_pp)
    for cp in stage:
        cp.start()
    with scope("dx1"):
        if n_x > 1:
            @pl.when(p == n_pp - 1)
            def _():
                @pl.loop(0, n_chunk)
                def _(k):
                    hid_in.ring(k).wait_send()

        dx_in.steps(at_half, at_one, True)
    with scope("stat1"):
        for cp in stage:
            cp.wait()
    top, tot = merge(stat_ref, buf_p, n_pp)
    mid_ref[0:1, :] = top
    mid_ref[1:2, :] = tot
    stage = swap(mid_ref, buf_z, sz_s, sz_r, "tp", z, n_tp)
    for cp in stage:
        cp.start()
    with scope("dx2"):
        dx_in.steps(at_one, at_two, True)
    with scope("stat2"):
        for cp in stage:
            cp.wait()
    top, tot = merge(mid_ref, buf_z, n_tp)
    mid_ref[0:1, :] = jnp.exp(stat_ref[0:1, :] - top) / (tot * tok)

    def head(d):
        for g in range(0, n_piece, per_band):
            count = min(per_band, n_piece - g)
            cols = pl.ds(g * wide, count * wide)
            prob = big_ref[pl.ds(pl.multiple_of(exp_row + (g // per_band) * n_dp * rows + d * rows, 8), rows), pl.ds(0, count * wide)] * mid_ref[0:1, cols]
            hit = local_ids(lab_ref, g * wide, count * wide) == row_ids(d, count * wide)
            dl_ref[:, cols] = jnp.where(hit, prob - 1.0 / tok, prob).astype(BF16)
        for q in range(4):
            part_at(d, q)[...] = jnp.dot(dl_ref[...], hid_ref[:, q * dq:(q + 1) * dq], preferred_element_type=F32)

    def lookup(g):
        def add(d):
            hot = (local_ids(look_ref, g * group, group) == row_ids(d, group)).astype(BF16)
            dl_ref[:, 0:group] = hot
            for q in range(4):
                part_at(d, q)[...] += jnp.dot(dl_ref[:, 0:group], dx_ref[g * group:(g + 1) * group, q * dq:(q + 1) * dq], preferred_element_type=F32)
        return add

    with scope("head"):
        @pl.loop(0, n_dp)
        def _(d):
            head(d)
            dx_in.steps(jnp.minimum(at_two + d, at_three), jnp.minimum(at_two + d + 1, at_three), True)

        dx_in.steps(jnp.minimum(at_two + n_dp, at_three), at_three, True)
    with scope("dx_group0"):
        dx_in.collect(0, n_group)
        pl.loop(0, n_dp)(lookup(0))
    with scope("dx4"):
        dx_in.steps(at_three, at_four, True)
    with scope("dx_group1"):
        dx_in.collect(1, n_group)
        pl.loop(0, n_dp)(lookup(1))
    with scope("dx5"):
        dx_in.steps(at_four, last, True)
    with scope("dx_group2"):
        dx_in.collect(2, n_group)

    far = lax.rem(y + 2, n_dp)

    def reduce_copy(i, d, half, row, where):
        return remote(part_at(d, 2 * half, 2), half_at(row, half), rs_s.at[i], rs_r.at[i], {"dp": where})

    rel_a = reduce_copy(0, far, 0, rel_row, up_y)
    rel_b = reduce_copy(1, far, 1, rel_row, down_y)
    one_b = reduce_copy(2, up_y, 1, one_row, up_y)
    one_a = reduce_copy(3, down_y, 0, one_row, down_y)
    com_a = reduce_copy(4, up_y, 0, com_row, up_y)
    com_b = reduce_copy(5, down_y, 1, com_row, down_y)
    add = lookup(n_group - 1)
    add(far)
    rel_a.start()
    rel_b.start()
    add(up_y)
    one_b.start()
    add(down_y)
    one_a.start()
    add(y)
    hid_in.settle()
    dx_in.settle()

    def moments(lo, hi, sem):
        return pltpu.make_async_copy(sq_ref.at[pl.ds(lo, hi - lo)], big_ref.at[pl.ds(lo, hi - lo)], pre_s.at[sem])

    loads = [moments(0, min(part_row, vocab), 0)]
    loads[0].start()
    with scope("relay"):
        rel_a.wait_recv()
    part_at(up_y, 0, 2)[...] += half_at(rel_row, 0)[...]
    com_a.start()
    rel_b.wait_recv()
    part_at(down_y, 2, 2)[...] += half_at(rel_row, 1)[...]
    com_b.start()
    own = y * n_pp + p
    square = jnp.zeros((8, 128), F32)
    with scope("one"):
        one_a.wait_recv()
        one_b.wait_recv()
    for half, cp in ((0, com_a), (1, com_b)):
        with scope("com"):
            cp.wait_recv()
        for q in range(2):
            cols = pl.ds((2 * half + q) * dq, dq)
            total = (part_at(y, 2 * half + q)[...] + big_ref[pl.ds(com_row, rows), cols] + big_ref[pl.ds(one_row, rows), cols]) * (1.0 / n_dp)
            g_ref[own, 2 * half + q] = total
            lanes = jnp.sum((total * total).reshape(rows // 8, 8, dq), axis=0)
            for i in range(0, dq, 128):
                square = square + lanes[:, i:i + 128]

    def block(xx, yy):
        return lax.rem(yy + 2 * n_dp, n_dp) * n_pp + 2 * lax.rem(xx + 2 * n_x, n_x) + c

    colours = []
    for q, (axes, sign) in enumerate((("xy", 1), ("xy", -1), ("yx", 1), ("yx", -1))):
        sizes = (n_x, n_dp) if axes == "xy" else (n_dp, n_x)
        to_x = {"pp": 2 * lax.rem(x + sign + n_x, n_x) + c}
        to_y = {"dp": lax.rem(y + sign + n_dp, n_dp)}
        dest = (to_x, to_y) if axes == "xy" else (to_y, to_x)
        colours.append((q, axes, sign, sizes, dest, ring_plan(*sizes)))

    def holder(axes, sign, s, t):
        return block(x - sign * s, y - sign * t) if axes == "xy" else block(x - sign * t, y - sign * s)

    def message(colour, item, coming):
        q, axes, sign, _, dest, plan = colour
        phase, s, t = item
        at = plan.index(item)
        s_at, t_at = (s + coming, t) if phase == 1 else (s, t + coming)
        b = holder(axes, sign, s_at, t_at)
        return remote(g_ref.at[b, q], g_ref.at[b, q], ag_s.at[q, at], ag_r.at[q, at], dest[phase - 1])

    def mate_copy(q, slot, b):
        return remote(g_ref.at[b, q], g_ref.at[b, q], d_s.at[q, slot], d_r.at[q, slot], {"pp": mate})

    sends = []

    def push(cp):
        cp.start()
        sends.append(cp)

    for colour in colours:
        if colour[3][0] > 1:
            push(message(colour, (1, 0, 0), 0))
    for colour in colours:
        if colour[3][1] > 1:
            push(message(colour, (2, 0, 0), 0))

    def norm_swap(value, buf, send, recv, axis, me, n):
        buf[me] = value
        return [remote(buf.at[me], buf.at[me], send.at[o - 1], recv.at[o - 1], {axis: lax.rem(me + o, n)}) for o in range(1, n)], [
            remote(buf.at[lax.rem(me + n - o, n)], buf.at[lax.rem(me + n - o, n)], send.at[o - 1], recv.at[o - 1], {axis: lax.rem(me + o, n)}) for o in range(1, n)]

    norm_out, norm_in = norm_swap(square, nb_p, np_s, np_r, "pp", p, n_pp)
    for cp in norm_out:
        push(cp)
    for q in range(4):
        push(mate_copy(q, 0, own))

    for cp in (rel_a, rel_b, one_a, one_b, com_a, com_b):
        cp.wait_send()
    if part_row < vocab:
        loads.append(moments(part_row, vocab, 1))
        loads[1].start()

    steps = n_x * n_dp - 1
    for i in range(steps):
        for colour in colours:
            q, axes, sign, sizes, dest, plan = colour
            phase, s, t = plan[i]
            message(colour, plan[i], 1).wait_recv()
            if phase == 1:
                if s + 1 < sizes[0] - 1:
                    push(message(colour, (1, s + 1, 0), 0))
                if sizes[1] > 1:
                    push(message(colour, (2, s + 1, 0), 0))
                push(mate_copy(q, i + 1, holder(axes, sign, s + 1, 0)))
            else:
                if t + 1 < sizes[1] - 1:
                    push(message(colour, (2, s, t + 1), 0))
                push(mate_copy(q, i + 1, holder(axes, sign, s, t + 1)))
        if i == 0:
            for cp in norm_in:
                cp.wait_recv()
            total = nb_p[0]
            for o in range(1, n_pp):
                total = total + nb_p[o]
            norm_out, norm_in = norm_swap(total, nb_y, ny_s, ny_r, "dp", y, n_dp)
            for cp in norm_out:
                push(cp)
        if i == 1:
            for cp in norm_in:
                cp.wait_recv()
            total = nb_y[0]
            for o in range(1, n_dp):
                total = total + nb_y[o]
            norm_out, norm_in = norm_swap(total, nb_z, nz_s, nz_r, "tp", z, n_tp)
            for cp in norm_out:
                push(cp)
        if i == 2:
            for cp in norm_in:
                cp.wait_recv()
            total = nb_z[0]
            for o in range(1, n_tp):
                total = total + nb_z[o]
            norm = jnp.sqrt(jnp.sum(total, axis=(0, 1), keepdims=True))
            scale_ref[...] = jnp.broadcast_to(CLIP_NORM / jnp.maximum(norm, CLIP_NORM), (8, 128))

    for q, axes, sign, sizes, dest, plan in colours:
        for i in range(steps + 1):
            if i == 0:
                b = own
            else:
                phase, s, t = plan[i - 1]
                b = holder(axes, sign, s + 1, 0) if phase == 1 else holder(axes, sign, s, t + 1)
            mate_copy(q, i, b + 1 - 2 * c).wait_recv()
    for cp in sends:
        cp.wait_send()
    for cp in loads:
        cp.wait()


def plane_gradient(master, acts, ids, exp_avg_sq, n_tp, n_dp, n_pp):
    vocab, dim = master.shape
    tok = acts.shape[0]
    rows = -(-vocab // (n_pp * n_dp))
    rows = -(-rows // 8) * 8
    dq = dim // 4
    n_chunk = 12 if tok % (4 * 12 * 8) == 0 else 6
    lag = 2
    steps = (n_pp // 2) * n_dp
    per_band = min(6, dim // (tok // 6))
    big = max(n_dp * n_pp * rows, 2 * tok + (-(-6 // per_band) * n_dp + n_dp + 3) * rows)
    full = pl.BlockSpec(memory_space=VMEM)
    any_space = pl.BlockSpec(memory_space=pl.ANY)
    chunk = DMA((2, n_chunk))
    return pl.pallas_call(
        functools.partial(grad_kernel, n_tp, n_dp, n_pp, n_chunk, lag),
        out_shape=(VMEM((n_dp * n_pp, 4, rows, dq), F32), jax.ShapeDtypeStruct((8, 128), F32), VMEM((big, dim), F32)),
        in_specs=[any_space, any_space, full, any_space],
        out_specs=(full, full, full),
        scratch_shapes=[
            VMEM((tok, dim), BF16), VMEM((tok, dim), BF16),
            VMEM((1, tok), jnp.int32), VMEM((1, tok), jnp.int32), VMEM((n_dp, rows, dim), BF16), VMEM((rows, tok), BF16),
            VMEM((2, tok), F32), VMEM((2, tok), F32), VMEM((n_pp - 1, 2, tok), F32), VMEM((n_tp - 1, 2, tok), F32),
            VMEM((n_pp, 8, 128), F32), VMEM((n_dp, 8, 128), F32), VMEM((n_tp, 8, 128), F32),
            DMA((1 + n_dp,)), *[chunk] * 9, DMA((2, n_pp - 1)), DMA((2,)),
            DMA((n_pp - 1,)), DMA((n_pp - 1,)), DMA((n_tp - 1,)), DMA((n_tp - 1,)), DMA((6,)), DMA((6,)),
            DMA((n_pp - 1,)), DMA((n_pp - 1,)), DMA((n_dp - 1,)), DMA((n_dp - 1,)), DMA((n_tp - 1,)), DMA((n_tp - 1,)),
            DMA((4, steps)), DMA((4, steps)), DMA((4, steps)), DMA((4, steps)), DMA((2,)),
        ],
        compiler_params=pltpu.CompilerParams(collective_id=0, has_side_effects=True, vmem_limit_bytes=SMALL_GRANT),
        name="plane_gradient",
    )(master, acts, ids, exp_avg_sq)


def adamw_kernel(n_slot, ahead, tile, scale_ref, g_ref, v_ref, e_hbm, m_hbm, ne_hbm, nm_hbm, nv_hbm, nb_hbm, e_buf, m_buf, v_buf, b_buf, in_s, out_s):
    rows, dq = g_ref.shape[2:]
    per_block, per_tile = rows // 8, tile // 8
    n_tile = e_hbm.shape[0] // tile
    scale = scale_ref[0:1, 0:1]

    def span(i):
        return pl.ds(pl.multiple_of(i * tile, 8), tile)

    def loads(i):
        slot = lax.rem(i, n_slot)
        return [pltpu.make_async_copy(hbm.at[span(i)], buf.at[slot], in_s.at[a, slot]) for a, (hbm, buf) in enumerate(((e_hbm, e_buf), (m_hbm, m_buf)))]

    def stores(i):
        slot = lax.rem(i, n_slot)
        return [pltpu.make_async_copy(buf.at[slot], hbm.at[span(i)], out_s.at[a, slot]) for a, (buf, hbm) in enumerate(((e_buf, ne_hbm), (m_buf, nm_hbm), (v_buf, nv_hbm), (b_buf, nb_hbm)))]

    for i in range(min(ahead, n_tile)):
        for cp in loads(i):
            cp.start()

    @pl.loop(0, n_tile)
    def _(i):
        slot = lax.rem(i, n_slot)

        @pl.when(i + ahead < n_tile)
        def _():
            @pl.when(i + ahead >= n_slot)
            def _():
                for cp in stores(i + ahead - n_slot):
                    cp.wait()

            for cp in loads(i + ahead):
                cp.start()

        for cp in loads(i):
            cp.wait()
        for r in range(per_tile):
            group = i * per_tile + r
            blk = group // per_block
            inside = pl.ds(pl.multiple_of((group - blk * per_block) * 8, 8), 8)
            at = pl.ds(8 * r, 8)
            for q in range(4):
                cols = pl.ds(q * dq, dq)
                g = g_ref[blk, q, inside, :] * scale
                e = e_buf[slot, at, cols]
                m = BETA_ONE * m_buf[slot, at, cols] + (1.0 - BETA_ONE) * g
                v = BETA_TWO * v_ref[pl.ds(pl.multiple_of(group * 8, 8), 8), cols] + (1.0 - BETA_TWO) * g * g
                step = (m * (1.0 / (1.0 - BETA_ONE ** OPT_STEP))) / (jnp.sqrt(v * (1.0 / (1.0 - BETA_TWO ** OPT_STEP))) + ADAM_EPS)
                ne = e - LEARN_RATE * (step + WEIGHT_DECAY * e)
                e_buf[slot, at, cols] = ne
                m_buf[slot, at, cols] = m
                v_buf[slot, at, cols] = v
                b_buf[slot, at, cols] = ne.astype(BF16)
        for cp in stores(i):
            cp.start()

    for i in range(max(0, n_tile - n_slot), n_tile):
        for cp in stores(i):
            cp.wait()


def adamw(scale, grad, second, master, exp_avg):
    vocab, dim = master.shape
    tile = next(t for t in (48, 32, 16, 8) if vocab % t == 0)
    n_slot = 14
    full = pl.BlockSpec(memory_space=VMEM)
    any_space = pl.BlockSpec(memory_space=pl.ANY)
    f32 = jax.ShapeDtypeStruct((vocab, dim), F32)
    count = vocab * dim
    ring = VMEM((n_slot, tile, dim), F32)
    return pl.pallas_call(
        functools.partial(adamw_kernel, n_slot, 8, tile),
        out_shape=(f32, f32, f32, jax.ShapeDtypeStruct((vocab, dim), BF16)),
        in_specs=[full, full, full, any_space, any_space],
        out_specs=(any_space,) * 4,
        scratch_shapes=[ring, ring, ring, VMEM((n_slot, tile, dim), BF16), DMA((2, n_slot)), DMA((4, n_slot))],
        cost_estimate=pl.CostEstimate(flops=20 * count, bytes_accessed=22 * count, transcendentals=2 * count),
        compiler_params=pltpu.CompilerParams(vmem_limit_bytes=SMALL_GRANT),
        name="adamw",
    )(scale, in_vmem(grad), in_vmem(second), master, exp_avg)


def solution(mesh):
    n_pp, n_dp, n_tp = mesh.shape["pp"], mesh.shape["dp"], mesh.shape["tp"]
    table_spec = P("tp", None)

    def device_step(master, exp_avg, exp_avg_sq, stage_ids, stage_acts):
        vocab, dim = master.shape
        tok = stage_ids.shape[1] * stage_ids.shape[2]
        acts = stage_acts.reshape(tok, dim)
        grad, scale, second = plane_gradient(master, acts, stage_ids.reshape(1, tok), exp_avg_sq, n_tp, n_dp, n_pp)
        return adamw(scale, grad, second, master, exp_avg)

    return jax.shard_map(device_step, mesh=mesh, in_specs=(table_spec, table_spec, table_spec, P("pp", "dp", None), P("pp", "dp", None, None)), out_specs=(table_spec, table_spec, table_spec, table_spec), check_vma=False)
```

```python
import functools

import jax
import jax.numpy as jnp
from jax import lax
from jax.experimental import pallas as pl
from jax.experimental.pallas import tpu as pltpu
from jax.sharding import PartitionSpec as P

LEARN_RATE = 0.003
BETA_ONE = 0.9
BETA_TWO = 0.95
ADAM_EPS = 1e-8
WEIGHT_DECAY = 0.1
CLIP_NORM = 1.0
OPT_STEP = 10

MESH_ID = pl.DeviceIdType.MESH
LOW = -1e30
VMEM = pltpu.VMEM
DMA = pltpu.SemaphoreType.DMA
F32, BF16 = jnp.float32, jnp.bfloat16
SMALL_GRANT = 21 << 19
scope = jax.named_scope


def remote(src, dst, send, recv, where):
    return pltpu.make_async_remote_copy(src_ref=src, dst_ref=dst, send_sem=send, recv_sem=recv, device_id=where, device_id_type=MESH_ID)


def in_vmem(arr):
    return pltpu.with_memory_space_constraint(arr, VMEM)


def enter(groups):
    barrier = pltpu.get_barrier_semaphore()
    for axis, peer in groups:
        pl.semaphore_signal(barrier, inc=1, device_id={axis: peer}, device_id_type=MESH_ID)
    pl.semaphore_wait(barrier, len(groups))


def ring_plan(n_one, n_two):
    items = [(1, s, 0) for s in range(n_one - 1)] + [(2, s, t) for s in range(n_one) for t in range(n_two - 1)]
    return sorted(items, key=lambda i: (i[1] + i[2], i[0], i[2]))


def grad_kernel(n_tp, n_dp, n_pp, n_chunk, lag, table_ref, acts_ref, ids_ref, sq_ref, g_ref, scale_ref, big_ref, hid_ref, dx_ref, lab_ref, look_ref, tab_ref, dl_ref, stat_ref, mid_ref, buf_p, buf_z, nb_p, nb_y, nb_z, load_s, feed_s, send_x, send_z, send_d, send_e, recv_x, recv_z, recv_d, recv_e, id_s, id_r, sp_s, sp_r, sz_s, sz_r, rs_s, rs_r, np_s, np_r, ny_s, ny_r, nz_s, nz_r, ag_s, ag_r, d_s, d_r, pre_s):
    p, z, y = lax.axis_index("pp"), lax.axis_index("tp"), lax.axis_index("dp")
    n_x = n_pp // 2
    x, c, par = p // 2, lax.rem(p, 2), lax.rem(z, 2)
    mate = 2 * x + 1 - c
    vocab = table_ref.shape[0]
    rows, tok = dl_ref.shape
    dq = g_ref.shape[3]
    up_y, down_y = lax.rem(y + 1, n_dp), lax.rem(y + n_dp - 1, n_dp)

    def first_row(d):
        return (d * n_pp + p) * rows

    n_piece, n_group = 6, 3
    wide = tok // n_piece
    per_band = min(n_piece, table_ref.shape[1] // wide)
    exp_row = 2 * tok
    part_row = exp_row + -(-n_piece // per_band) * n_dp * rows
    rel_row, one_row, com_row = (part_row + (n_dp + i) * rows for i in range(3))

    def exp_at(g, d, count=1):
        return big_ref.at[pl.ds(exp_row + (g // per_band) * n_dp * rows + d * rows, rows), pl.ds((g % per_band) * wide, count * wide)]

    def part_at(d, q, count=1):
        return big_ref.at[pl.ds(pl.multiple_of(part_row + d * rows, 8), rows), pl.ds(q * dq, count * dq)]

    def half_at(row, half):
        return big_ref.at[pl.ds(row, rows), pl.ds(2 * half * dq, 2 * dq)]

    short = vocab - (n_dp * n_pp - 1) * rows

    def table_copies(count, blocks):
        return [pltpu.make_async_copy(table_ref.at[pl.ds(pl.multiple_of(first_row(d), 8), count)], big_ref.at[pl.ds(part_row + d * rows, count)], load_s.at[1 + d]) for d in blocks]

    def each_table_copy(act):
        for cp in table_copies(rows, range(n_dp - 1)):
            act(cp)
        for cond, count in ((p < n_pp - 1, rows), (p == n_pp - 1, short)):
            @pl.when(cond)
            def _(count=count):
                for cp in table_copies(count, (n_dp - 1,)):
                    act(cp)

    each_table_copy(lambda cp: cp.start())
    hid_buf, dx_buf = big_ref.at[pl.ds(0, tok)], big_ref.at[pl.ds(tok, tok)]
    sources = ((n_pp - 1, hid_buf, hid_ref, lab_ref), (0, dx_buf, dx_ref, look_ref))
    for source, _, low, _ in sources:
        @pl.when(p == source)
        def _(low=low):
            pltpu.make_async_copy(acts_ref, low, load_s.at[0]).start()

    enter([("pp", lax.rem(p + o, n_pp)) for o in range(1, n_pp)] + [("tp", lax.rem(z + o, n_tp)) for o in range(1, n_tp)] + [("dp", lax.rem(y + o, n_dp)) for o in range(1, n_dp)])

    step_x = 1 - 2 * c
    next_p = 2 * lax.rem(x + step_x + n_x, n_x) + c
    next_z = lax.rem(z + step_x + n_tp, n_tp)
    size = tok // (4 * n_chunk)
    last = n_chunk + lag
    per_group = n_chunk // n_group
    group = tok // n_group

    def span(core, parity, k):
        return pl.ds(pl.multiple_of((4 * k + 2 * parity + core) * size, 8), size)

    class Stream:
        def __init__(self, a):
            self.a = a
            self.source, self.buf, self.low, self.ids = sources[a]
            self.is_src = p == self.source
            s_x = self.source // 2
            self.dist = lax.rem(jnp.where(c == 0, x - s_x, s_x - x) + n_x, n_x)
            self.cut = a == 1 and n_x > 2
            ends = jnp.where(c == 0, n_x - 2, n_x - 1) if self.cut else n_x - 1
            self.passes = self.dist < ends

        def hop(self, part, send, recv, where):
            return remote(self.buf.at[part], self.buf.at[part], send, recv, where)

        def feed(self, k):
            return self.hop(span(1 - c, par, k), feed_s.at[self.a, k], recv_x.at[self.a, k], {"pp": mate})

        def ring(self, k):
            return self.hop(span(c, par, k), send_x.at[self.a, k], recv_x.at[self.a, k], {"pp": next_p})

        def direct(self, k):
            return self.hop(span(c, par, k), send_z.at[self.a, k], recv_x.at[self.a, k], {"pp": lax.rem(p + n_pp - 2, n_pp)})

        def plane(self, k, parity):
            return self.hop(span(c, parity, k), send_z.at[self.a, k], recv_z.at[self.a, k], {"tp": next_z})

        def across(self, k, core):
            return self.hop(span(core, par, k), send_d.at[self.a, k], recv_d.at[self.a, k], {"pp": mate})

        def again(self, k, core):
            return self.hop(span(core, 1 - par, k), send_e.at[self.a, k], recv_e.at[self.a, k], {"pp": mate})

        def id_copy(self, o):
            return remote(ids_ref, self.ids, id_s.at[self.a, o - 1], id_r.at[self.a], {"pp": lax.rem(p + o, n_pp)})

        def begin(self, with_ring):
            @pl.when(self.is_src)
            def _():
                pltpu.make_async_copy(acts_ref, self.low, load_s.at[0]).wait()
                self.ids[...] = ids_ref[...]

                @pl.loop(0, n_chunk)
                def _(k):
                    def widen(part):
                        self.buf[part, :] = self.low[part, :].astype(F32)

                    widen(span(1 - c, par, k))
                    self.feed(k).start()
                    widen(span(c, par, k))
                    if n_x > 1 and with_ring:
                        self.ring(k).start()
                    self.across(k, c).start()
                    widen(span(c, 1 - par, k))
                    self.again(k, c).start()

                for o in range(1, n_pp):
                    self.id_copy(o).start()

        def early_ring(self):
            @pl.when(mate == self.source)
            def _():
                @pl.loop(0, n_chunk)
                def _(k):
                    self.ring(k).wait_recv()
                    if n_x > 1:
                        self.ring(k).start()

        def late_ring(self, lo, hi):
            if n_x > 1:
                @pl.when(self.is_src)
                def _():
                    @pl.loop(lo, hi)
                    def _(k):
                        self.ring(k).start()
                        if self.cut:
                            self.direct(k).start()

        def late_plane(self):
            @pl.when(mate == self.source)
            def _():
                @pl.loop(0, n_chunk)
                def _(k):
                    self.plane(k, par).start()

        def steps(self, lo, hi, early=False):
            @pl.when(jnp.logical_not(self.is_src))
            def _():
                @pl.loop(lo, hi)
                def _(k):
                    @pl.when(jnp.logical_and(k < n_chunk, jnp.logical_or(mate != self.source, not early)))
                    def _():
                        self.ring(k).wait_recv()
                        if n_x > 1:
                            @pl.when(self.passes)
                            def _():
                                if early:
                                    @pl.when(jnp.logical_and(p == n_pp - 1, k >= 2))
                                    def _():
                                        self.ring(k - 2).wait_send()

                                self.ring(k).start()

                        self.plane(k, par).start()

                        @pl.when(mate != self.source)
                        def _():
                            self.across(k, c).start()

                    @pl.when(k >= lag)
                    def _():
                        self.plane(k - lag, 1 - par).wait_recv()

                        @pl.when(mate != self.source)
                        def _():
                            self.again(k - lag, c).start()

        def collect(self, g, parts):
            @pl.when(jnp.logical_not(self.is_src))
            def _():
                if g == 0:
                    self.id_copy(1).wait_recv()

                per_part, count = n_chunk // parts, tok // parts

                @pl.loop(g * per_part, (g + 1) * per_part)
                def _(k):
                    self.across(k, 1 - c).wait_recv()
                    self.again(k, 1 - c).wait_recv()

                tile = min(128, count)

                @pl.loop(0, count // tile)
                def _(k):
                    here = pl.ds(pl.multiple_of(g * count + k * tile, tile), tile)
                    self.low[here, :] = self.buf[here, :].astype(BF16)

        def settle(self):
            @pl.when(self.is_src)
            def _():
                for o in range(1, n_pp):
                    self.id_copy(o).wait_send()

            @pl.loop(0, n_chunk)
            def _(k):
                @pl.when(self.is_src)
                def _():
                    self.feed(k).wait_send()
                    if self.cut:
                        self.direct(k).wait_send()

                @pl.when(jnp.logical_not(self.is_src))
                def _():
                    self.plane(k, par).wait_send()

                if n_x > 1:
                    begun = n_chunk if self.a == 0 else n_chunk - 2

                    @pl.when(jnp.logical_and(self.passes, jnp.logical_or(p != n_pp - 1, k >= begun)))
                    def _():
                        self.ring(k).wait_send()

                @pl.when(mate != self.source)
                def _():
                    self.across(k, c).wait_send()
                    self.again(k, c).wait_send()

    hid_in, dx_in = Stream(0), Stream(1)
    def logits(g):
        cols = pl.ds(g * wide, wide)
        h = hid_ref[cols, :]
        top = jnp.full((1, wide), LOW, F32)
        for d in range(n_dp):
            lg = lax.dot_general(tab_ref[d], h, (((1,), (1,)), ((), ())), preferred_element_type=F32)
            if d == n_dp - 1 and short < rows:
                ok = first_row(d) + lax.broadcasted_iota(jnp.int32, (rows, wide), 0) < vocab
                lg = jnp.where(ok, lg, LOW)
            exp_at(g, d)[...] = lg
            top = jnp.maximum(top, jnp.max(lg, axis=0, keepdims=True))
        tot = jnp.zeros((1, wide), F32)
        for d in range(n_dp):
            e = jnp.exp(exp_at(g, d)[...] - top)
            exp_at(g, d)[...] = e
            tot = tot + jnp.sum(e, axis=0, keepdims=True)
        stat_ref[0:1, cols] = top
        stat_ref[1:2, cols] = tot

    with scope("begin"):
        hid_in.begin(True)
        dx_in.begin(False)
        each_table_copy(lambda cp: cp.wait())
        for d in range(n_dp):
            tab_ref[d] = part_at(d, 0, 4)[...].astype(BF16)
    with scope("early"):
        dx_in.early_ring()
    dist = jnp.where(jnp.logical_and(c == 0, dx_in.dist == n_x - 1), 1, dx_in.dist)

    def clip(value):
        return jnp.clip(jnp.where(p == 1, 0, value), 0, last)

    near = jnp.where(jnp.logical_or(jnp.logical_and(c == 0, dx_in.dist == 1), jnp.logical_and(c == 1, dist >= 2)), 1, 0)
    near = jnp.where(jnp.logical_or(p == n_pp - 1, hid_in.dist == n_x - 1), 0, near)
    at_zero = near * jnp.where(c == 0, 2, jnp.maximum(12 - 3 * dist, 0))
    at_zero = jnp.minimum(at_zero, last - (n_piece - 2))
    at_half = at_zero + (n_piece - 2) * near
    at_one = jnp.where(p == n_pp - 1, last, jnp.where(c == 0, 11 - 3 * dist, 18 - 3 * dist))
    at_two = jnp.where(p == n_pp - 1, last, jnp.where(c == 0, at_one + 2, at_one + 3))
    at_one = jnp.maximum(clip(at_one), at_half)
    at_two = jnp.maximum(clip(at_two), at_one)
    at_three = jnp.maximum(jnp.minimum(at_two + jnp.where(p == 1, 0, n_dp), last), min(last, per_group + lag))
    at_four = jnp.maximum(at_three, min(last, max(n_chunk, 2 * per_group + lag)))

    def prepare(g):
        with scope(f"hid_collect{g}"):
            hid_in.collect(g, n_piece)
        with scope(f"logits{g}"):
            logits(g)

    at_end = jnp.logical_and(hid_in.dist == n_x - 1, jnp.logical_not(hid_in.is_src))
    pair = n_chunk // n_piece

    @pl.when(at_end)
    def _():
        lo = 0
        for g in range(n_piece - 2):
            hi = min(last, (g + 1) * pair + lag + 1)
            with scope(f"hid{g}"):
                hid_in.steps(lo, hi)
            prepare(g)
            lo = hi
        with scope("hid_end"):
            hid_in.steps(lo, last)
        dx_in.late_ring(0, n_chunk)
        dx_in.late_plane()

    @pl.when(jnp.logical_not(at_end))
    def _():
        with scope("hid_end"):
            hid_in.steps(0, n_chunk)
            dx_in.late_ring(0, n_chunk)
            hid_in.steps(n_chunk, last)
            dx_in.late_plane()
        with scope("dx0"):
            dx_in.steps(0, at_zero, True)
        for g in range(n_piece - 2):
            prepare(g)
            dx_in.steps(at_zero + g * near, at_zero + (g + 1) * near, True)

    for g in range(n_piece - 2, n_piece):
        prepare(g)

    def swap(src, buf, send, recv, axis, me, n):
        return [remote(src, buf.at[o - 1], send.at[o - 1], recv.at[o - 1], {axis: lax.rem(me + o, n)}) for o in range(1, n)]

    def merge(src, buf, n):
        top = src[0:1, :]
        for o in range(1, n):
            top = jnp.maximum(top, buf[o - 1, 0:1, :])
        tot = src[1:2, :] * jnp.exp(src[0:1, :] - top)
        for o in range(1, n):
            tot = tot + buf[o - 1, 1:2, :] * jnp.exp(buf[o - 1, 0:1, :] - top)
        return top, tot

    def local_ids(ref, start, count):
        ids = ref[:, start:start + count] - z * vocab
        return jnp.where(ids < vocab, ids, -1)

    def row_ids(d, count):
        return first_row(d) + lax.broadcasted_iota(jnp.int32, (rows, count), 0)

    stage = swap(stat_ref, buf_p, sp_s, sp_r, "pp", p, n_pp)
    for cp in stage:
        cp.start()
    with scope("dx1"):
        if n_x > 1:
            @pl.when(p == n_pp - 1)
            def _():
                @pl.loop(0, n_chunk)
                def _(k):
                    hid_in.ring(k).wait_send()

        dx_in.steps(at_half, at_one, True)
    with scope("stat1"):
        for cp in stage:
            cp.wait()
    top, tot = merge(stat_ref, buf_p, n_pp)
    mid_ref[0:1, :] = top
    mid_ref[1:2, :] = tot
    stage = swap(mid_ref, buf_z, sz_s, sz_r, "tp", z, n_tp)
    for cp in stage:
        cp.start()
    with scope("dx2"):
        dx_in.steps(at_one, at_two, True)
    with scope("stat2"):
        for cp in stage:
            cp.wait()
    top, tot = merge(mid_ref, buf_z, n_tp)
    mid_ref[0:1, :] = jnp.exp(stat_ref[0:1, :] - top) / (tot * tok)

    def head(d):
        for g in range(0, n_piece, per_band):
            count = min(per_band, n_piece - g)
            cols = pl.ds(g * wide, count * wide)
            prob = big_ref[pl.ds(pl.multiple_of(exp_row + (g // per_band) * n_dp * rows + d * rows, 8), rows), pl.ds(0, count * wide)] * mid_ref[0:1, cols]
            hit = local_ids(lab_ref, g * wide, count * wide) == row_ids(d, count * wide)
            dl_ref[:, cols] = jnp.where(hit, prob - 1.0 / tok, prob).astype(BF16)
        for q in range(4):
            part_at(d, q)[...] = jnp.dot(dl_ref[...], hid_ref[:, q * dq:(q + 1) * dq], preferred_element_type=F32)

    def lookup(g):
        def add(d):
            hot = (local_ids(look_ref, g * group, group) == row_ids(d, group)).astype(BF16)
            dl_ref[:, 0:group] = hot
            for q in range(4):
                part_at(d, q)[...] += jnp.dot(dl_ref[:, 0:group], dx_ref[g * group:(g + 1) * group, q * dq:(q + 1) * dq], preferred_element_type=F32)
        return add

    with scope("head"):
        @pl.loop(0, n_dp)
        def _(d):
            head(d)
            dx_in.steps(jnp.minimum(at_two + d, at_three), jnp.minimum(at_two + d + 1, at_three), True)

        dx_in.steps(jnp.minimum(at_two + n_dp, at_three), at_three, True)
    with scope("dx_group0"):
        dx_in.collect(0, n_group)
        pl.loop(0, n_dp)(lookup(0))
    with scope("dx4"):
        dx_in.steps(at_three, at_four, True)
    with scope("dx_group1"):
        dx_in.collect(1, n_group)
        pl.loop(0, n_dp)(lookup(1))
    with scope("dx5"):
        dx_in.steps(at_four, last, True)
    with scope("dx_group2"):
        dx_in.collect(2, n_group)

    far = lax.rem(y + 2, n_dp)

    def reduce_copy(i, d, half, row, where):
        return remote(part_at(d, 2 * half, 2), half_at(row, half), rs_s.at[i], rs_r.at[i], {"dp": where})

    rel_a = reduce_copy(0, far, 0, rel_row, up_y)
    rel_b = reduce_copy(1, far, 1, rel_row, down_y)
    one_b = reduce_copy(2, up_y, 1, one_row, up_y)
    one_a = reduce_copy(3, down_y, 0, one_row, down_y)
    com_a = reduce_copy(4, up_y, 0, com_row, up_y)
    com_b = reduce_copy(5, down_y, 1, com_row, down_y)
    add = lookup(n_group - 1)
    add(far)
    rel_a.start()
    rel_b.start()
    add(up_y)
    one_b.start()
    add(down_y)
    one_a.start()
    add(y)
    hid_in.settle()
    dx_in.settle()

    def moments(lo, hi, sem):
        return pltpu.make_async_copy(sq_ref.at[pl.ds(lo, hi - lo)], big_ref.at[pl.ds(lo, hi - lo)], pre_s.at[sem])

    loads = [moments(0, min(part_row, vocab), 0)]
    loads[0].start()
    with scope("relay"):
        rel_a.wait_recv()
    part_at(up_y, 0, 2)[...] += half_at(rel_row, 0)[...]
    com_a.start()
    rel_b.wait_recv()
    part_at(down_y, 2, 2)[...] += half_at(rel_row, 1)[...]
    com_b.start()
    own = y * n_pp + p
    square = jnp.zeros((8, 128), F32)
    with scope("one"):
        one_a.wait_recv()
        one_b.wait_recv()
    for half, cp in ((0, com_a), (1, com_b)):
        with scope("com"):
            cp.wait_recv()
        for q in range(2):
            cols = pl.ds((2 * half + q) * dq, dq)
            total = (part_at(y, 2 * half + q)[...] + big_ref[pl.ds(com_row, rows), cols] + big_ref[pl.ds(one_row, rows), cols]) * (1.0 / n_dp)
            g_ref[own, 2 * half + q] = total
            lanes = jnp.sum((total * total).reshape(rows // 8, 8, dq), axis=0)
            for i in range(0, dq, 128):
                square = square + lanes[:, i:i + 128]

    def block(xx, yy):
        return lax.rem(yy + 2 * n_dp, n_dp) * n_pp + 2 * lax.rem(xx + 2 * n_x, n_x) + c

    colours = []
    for q, (axes, sign) in enumerate((("xy", 1), ("xy", -1), ("yx", 1), ("yx", -1))):
        sizes = (n_x, n_dp) if axes == "xy" else (n_dp, n_x)
        to_x = {"pp": 2 * lax.rem(x + sign + n_x, n_x) + c}
        to_y = {"dp": lax.rem(y + sign + n_dp, n_dp)}
        dest = (to_x, to_y) if axes == "xy" else (to_y, to_x)
        colours.append((q, axes, sign, sizes, dest, ring_plan(*sizes)))

    def holder(axes, sign, s, t):
        return block(x - sign * s, y - sign * t) if axes == "xy" else block(x - sign * t, y - sign * s)

    def message(colour, item, coming):
        q, axes, sign, _, dest, plan = colour
        phase, s, t = item
        at = plan.index(item)
        s_at, t_at = (s + coming, t) if phase == 1 else (s, t + coming)
        b = holder(axes, sign, s_at, t_at)
        return remote(g_ref.at[b, q], g_ref.at[b, q], ag_s.at[q, at], ag_r.at[q, at], dest[phase - 1])

    def mate_copy(q, slot, b):
        return remote(g_ref.at[b, q], g_ref.at[b, q], d_s.at[q, slot], d_r.at[q, slot], {"pp": mate})

    sends = []

    def push(cp):
        cp.start()
        sends.append(cp)

    for colour in colours:
        if colour[3][0] > 1:
            push(message(colour, (1, 0, 0), 0))
    for colour in colours:
        if colour[3][1] > 1:
            push(message(colour, (2, 0, 0), 0))

    def norm_swap(value, buf, send, recv, axis, me, n):
        buf[me] = value
        return [remote(buf.at[me], buf.at[me], send.at[o - 1], recv.at[o - 1], {axis: lax.rem(me + o, n)}) for o in range(1, n)], [
            remote(buf.at[lax.rem(me + n - o, n)], buf.at[lax.rem(me + n - o, n)], send.at[o - 1], recv.at[o - 1], {axis: lax.rem(me + o, n)}) for o in range(1, n)]

    norm_out, norm_in = norm_swap(square, nb_p, np_s, np_r, "pp", p, n_pp)
    for cp in norm_out:
        push(cp)
    for q in range(4):
        push(mate_copy(q, 0, own))

    for cp in (rel_a, rel_b, one_a, one_b, com_a, com_b):
        cp.wait_send()
    if part_row < vocab:
        loads.append(moments(part_row, vocab, 1))
        loads[1].start()

    steps = n_x * n_dp - 1
    for i in range(steps):
        for colour in colours:
            q, axes, sign, sizes, dest, plan = colour
            phase, s, t = plan[i]
            message(colour, plan[i], 1).wait_recv()
            if phase == 1:
                if s + 1 < sizes[0] - 1:
                    push(message(colour, (1, s + 1, 0), 0))
                if sizes[1] > 1:
                    push(message(colour, (2, s + 1, 0), 0))
                push(mate_copy(q, i + 1, holder(axes, sign, s + 1, 0)))
            else:
                if t + 1 < sizes[1] - 1:
                    push(message(colour, (2, s, t + 1), 0))
                push(mate_copy(q, i + 1, holder(axes, sign, s, t + 1)))
        if i == 0:
            for cp in norm_in:
                cp.wait_recv()
            total = nb_p[0]
            for o in range(1, n_pp):
                total = total + nb_p[o]
            norm_out, norm_in = norm_swap(total, nb_y, ny_s, ny_r, "dp", y, n_dp)
            for cp in norm_out:
                push(cp)
        if i == 1:
            for cp in norm_in:
                cp.wait_recv()
            total = nb_y[0]
            for o in range(1, n_dp):
                total = total + nb_y[o]
            norm_out, norm_in = norm_swap(total, nb_z, nz_s, nz_r, "tp", z, n_tp)
            for cp in norm_out:
                push(cp)
        if i == 2:
            for cp in norm_in:
                cp.wait_recv()
            total = nb_z[0]
            for o in range(1, n_tp):
                total = total + nb_z[o]
            norm = jnp.sqrt(jnp.sum(total, axis=(0, 1), keepdims=True))
            scale_ref[...] = jnp.broadcast_to(CLIP_NORM / jnp.maximum(norm, CLIP_NORM), (8, 128))

    for q, axes, sign, sizes, dest, plan in colours:
        for i in range(steps + 1):
            if i == 0:
                b = own
            else:
                phase, s, t = plan[i - 1]
                b = holder(axes, sign, s + 1, 0) if phase == 1 else holder(axes, sign, s, t + 1)
            mate_copy(q, i, b + 1 - 2 * c).wait_recv()
    for cp in sends:
        cp.wait_send()
    for cp in loads:
        cp.wait()


def plane_gradient(master, acts, ids, exp_avg_sq, n_tp, n_dp, n_pp):
    vocab, dim = master.shape
    tok = acts.shape[0]
    rows = -(-vocab // (n_pp * n_dp))
    rows = -(-rows // 8) * 8
    dq = dim // 4
    n_chunk = 12 if tok % (4 * 12 * 8) == 0 else 6
    lag = 2
    steps = (n_pp // 2) * n_dp
    per_band = min(6, dim // (tok // 6))
    big = max(n_dp * n_pp * rows, 2 * tok + (-(-6 // per_band) * n_dp + n_dp + 3) * rows)
    full = pl.BlockSpec(memory_space=VMEM)
    any_space = pl.BlockSpec(memory_space=pl.ANY)
    chunk = DMA((2, n_chunk))
    return pl.pallas_call(
        functools.partial(grad_kernel, n_tp, n_dp, n_pp, n_chunk, lag),
        out_shape=(VMEM((n_dp * n_pp, 4, rows, dq), F32), jax.ShapeDtypeStruct((8, 128), F32), VMEM((big, dim), F32)),
        in_specs=[any_space, any_space, full, any_space],
        out_specs=(full, full, full),
        scratch_shapes=[
            VMEM((tok, dim), BF16), VMEM((tok, dim), BF16),
            VMEM((1, tok), jnp.int32), VMEM((1, tok), jnp.int32), VMEM((n_dp, rows, dim), BF16), VMEM((rows, tok), BF16),
            VMEM((2, tok), F32), VMEM((2, tok), F32), VMEM((n_pp - 1, 2, tok), F32), VMEM((n_tp - 1, 2, tok), F32),
            VMEM((n_pp, 8, 128), F32), VMEM((n_dp, 8, 128), F32), VMEM((n_tp, 8, 128), F32),
            DMA((1 + n_dp,)), *[chunk] * 9, DMA((2, n_pp - 1)), DMA((2,)),
            DMA((n_pp - 1,)), DMA((n_pp - 1,)), DMA((n_tp - 1,)), DMA((n_tp - 1,)), DMA((6,)), DMA((6,)),
            DMA((n_pp - 1,)), DMA((n_pp - 1,)), DMA((n_dp - 1,)), DMA((n_dp - 1,)), DMA((n_tp - 1,)), DMA((n_tp - 1,)),
            DMA((4, steps)), DMA((4, steps)), DMA((4, steps)), DMA((4, steps)), DMA((2,)),
        ],
        compiler_params=pltpu.CompilerParams(collective_id=0, has_side_effects=True, vmem_limit_bytes=SMALL_GRANT),
        name="plane_gradient",
    )(master, acts, ids, exp_avg_sq)


def adamw_kernel(n_slot, ahead, tile, scale_ref, g_ref, v_ref, e_hbm, m_hbm, ne_hbm, nm_hbm, nv_hbm, nb_hbm, e_buf, m_buf, v_buf, b_buf, in_s, out_s):
    rows, dq = g_ref.shape[2:]
    per_block, per_tile = rows // 8, tile // 8
    n_tile = e_hbm.shape[0] // tile
    scale = scale_ref[0:1, 0:1]

    def span(i):
        return pl.ds(pl.multiple_of(i * tile, 8), tile)

    def loads(i):
        slot = lax.rem(i, n_slot)
        return [pltpu.make_async_copy(hbm.at[span(i)], buf.at[slot], in_s.at[a, slot]) for a, (hbm, buf) in enumerate(((e_hbm, e_buf), (m_hbm, m_buf)))]

    def stores(i):
        slot = lax.rem(i, n_slot)
        return [pltpu.make_async_copy(buf.at[slot], hbm.at[span(i)], out_s.at[a, slot]) for a, (buf, hbm) in enumerate(((e_buf, ne_hbm), (m_buf, nm_hbm), (v_buf, nv_hbm), (b_buf, nb_hbm)))]

    for i in range(min(ahead, n_tile)):
        for cp in loads(i):
            cp.start()

    @pl.loop(0, n_tile)
    def _(i):
        slot = lax.rem(i, n_slot)

        @pl.when(i + ahead < n_tile)
        def _():
            @pl.when(i + ahead >= n_slot)
            def _():
                for cp in stores(i + ahead - n_slot):
                    cp.wait()

            for cp in loads(i + ahead):
                cp.start()

        for cp in loads(i):
            cp.wait()
        for r in range(per_tile):
            group = i * per_tile + r
            blk = group // per_block
            inside = pl.ds(pl.multiple_of((group - blk * per_block) * 8, 8), 8)
            at = pl.ds(8 * r, 8)
            for q in range(4):
                cols = pl.ds(q * dq, dq)
                g = g_ref[blk, q, inside, :] * scale
                e = e_buf[slot, at, cols]
                m = BETA_ONE * m_buf[slot, at, cols] + (1.0 - BETA_ONE) * g
                v = BETA_TWO * v_ref[pl.ds(pl.multiple_of(group * 8, 8), 8), cols] + (1.0 - BETA_TWO) * g * g
                step = (m * (1.0 / (1.0 - BETA_ONE ** OPT_STEP))) / (jnp.sqrt(v * (1.0 / (1.0 - BETA_TWO ** OPT_STEP))) + ADAM_EPS)
                ne = e - LEARN_RATE * (step + WEIGHT_DECAY * e)
                e_buf[slot, at, cols] = ne
                m_buf[slot, at, cols] = m
                v_buf[slot, at, cols] = v
                b_buf[slot, at, cols] = ne.astype(BF16)
        for cp in stores(i):
            cp.start()

    for i in range(max(0, n_tile - n_slot), n_tile):
        for cp in stores(i):
            cp.wait()


def adamw(scale, grad, second, master, exp_avg):
    vocab, dim = master.shape
    tile = next(t for t in (48, 32, 16, 8) if vocab % t == 0)
    n_slot = 14
    full = pl.BlockSpec(memory_space=VMEM)
    any_space = pl.BlockSpec(memory_space=pl.ANY)
    f32 = jax.ShapeDtypeStruct((vocab, dim), F32)
    count = vocab * dim
    ring = VMEM((n_slot, tile, dim), F32)
    return pl.pallas_call(
        functools.partial(adamw_kernel, n_slot, 8, tile),
        out_shape=(f32, f32, f32, jax.ShapeDtypeStruct((vocab, dim), BF16)),
        in_specs=[full, full, full, any_space, any_space],
        out_specs=(any_space,) * 4,
        scratch_shapes=[ring, ring, ring, VMEM((n_slot, tile, dim), BF16), DMA((2, n_slot)), DMA((4, n_slot))],
        cost_estimate=pl.CostEstimate(flops=20 * count, bytes_accessed=22 * count, transcendentals=2 * count),
        compiler_params=pltpu.CompilerParams(vmem_limit_bytes=SMALL_GRANT),
        name="adamw",
    )(scale, in_vmem(grad), in_vmem(second), master, exp_avg)


def solution(mesh):
    n_pp, n_dp, n_tp = mesh.shape["pp"], mesh.shape["dp"], mesh.shape["tp"]
    table_spec = P("tp", None)

    def device_step(master, exp_avg, exp_avg_sq, stage_ids, stage_acts):
        vocab, dim = master.shape
        tok = stage_ids.shape[1] * stage_ids.shape[2]
        acts = stage_acts.reshape(tok, dim)
        grad, scale, second = plane_gradient(master, acts, stage_ids.reshape(1, tok), exp_avg_sq, n_tp, n_dp, n_pp)
        return adamw(scale, grad, second, master, exp_avg)

    return jax.shard_map(device_step, mesh=mesh, in_specs=(table_spec, table_spec, table_spec, P("pp", "dp", None), P("pp", "dp", None, None)), out_specs=(table_spec, table_spec, table_spec, table_spec), check_vma=False)
```
